32 devices in a mesh: dp: 1 (over z), tp: 4 (over y), sp: 8 (over x, core).
Axes of the slice: x: 4, y: 4, z: 1, core: 2. Of those that a mesh axis runs over, the one named last changes fastest.
The devices are a block of a 4x4x8 slice.
Arguments:
- x_in: bfloat16 [131072, 384], P(('dp', 'sp'))
- grad_y: bfloat16 [131072, 384], P(('dp', 'sp'))
- w_qkv: bfloat16 [384, 3, 384], P(None, None, 'tp')
- w_out: bfloat16 [384, 384], P('tp')
- ln_gamma: float32 [384], replicated
- ln_beta: float32 [384], replicated
- temperature: float32 [8], replicated
Outputs:
- output 1: bfloat16 [131072, 384], P(('dp', 'sp'))
- output 2: bfloat16 [131072, 384], P(('dp', 'sp'))
- output 3: float32 [384, 3, 384], P(('dp', 'sp'), None, 'tp')
- output 4: float32 [384, 384], P(('dp', 'tp', 'sp'))
- output 5: float32 [384], P('dp')
- output 6: float32 [384], P('dp')
- output 7: float32 [8], P('dp')
All inputs are finite; a program needn't handle non-finite values.
Results may differ from the reference program's by a relative error of at most 0.001.
Values are sent between devices in bfloat16 or wider.
A program may use at most 768 MiB of HBM per device.

```python
import jax
import jax.numpy as jnp
from jax import lax

MODEL_DIM = 384
NUM_HEADS = 8
NUM_TOKENS = 131072
NUM_REGIONS = 8
HEAD_DIM = MODEL_DIM // NUM_HEADS
LN_EPS = 1e-6


def setup_inputs(seed: int = 0, part: int = 0) -> dict:
    part_key = jax.random.fold_in(jax.random.key(seed), part)
    key_noise, key_offset, key_grad, key_goffset = jax.random.split(part_key, 4)
    key_wqkv, key_wout, key_gamma, key_beta, key_temp = jax.random.split(jax.random.key(seed + 1), 5)
    rows_per_region = NUM_TOKENS // NUM_REGIONS
    w_scale = MODEL_DIM ** -0.5
    offsets = jax.random.normal(key_offset, (NUM_REGIONS, MODEL_DIM), jnp.float32)
    x_vals = jax.random.normal(key_noise, (NUM_TOKENS, MODEL_DIM), jnp.float32) + jnp.repeat(offsets, rows_per_region, axis=0)
    grad_offsets = 0.5 * jax.random.normal(key_goffset, (NUM_REGIONS, MODEL_DIM), jnp.float32)
    grad_vals = jax.random.normal(key_grad, (NUM_TOKENS, MODEL_DIM), jnp.float32) + jnp.repeat(grad_offsets, rows_per_region, axis=0)
    w_qkv = jax.random.normal(key_wqkv, (MODEL_DIM, 3, MODEL_DIM), jnp.float32) * w_scale
    w_out = jax.random.normal(key_wout, (MODEL_DIM, MODEL_DIM), jnp.float32) * w_scale
    ln_gamma = 1.0 + 0.3 * jax.random.normal(key_gamma, (MODEL_DIM,), jnp.float32)
    ln_beta = 0.3 * jax.random.normal(key_beta, (MODEL_DIM,), jnp.float32)
    temperature = jax.random.uniform(key_temp, (NUM_HEADS,), jnp.float32, 2.0, 4.0)
    return {"x_in": x_vals.astype(jnp.bfloat16), "grad_y": grad_vals.astype(jnp.bfloat16), "w_qkv": w_qkv.astype(jnp.bfloat16), "w_out": w_out.astype(jnp.bfloat16), "ln_gamma": ln_gamma, "ln_beta": ln_beta, "temperature": temperature}


def head_pass(operands):
    q_head, k_head, v_head, dout_head, temp_one = operands
    gram_mat = jnp.dot(q_head.T, k_head, preferred_element_type=jnp.float32)
    q_sq = jnp.sum(jnp.square(q_head.astype(jnp.float32)), axis=0)
    k_sq = jnp.sum(jnp.square(k_head.astype(jnp.float32)), axis=0)
    norm_prod = jnp.sqrt(q_sq)[:, None] * jnp.sqrt(k_sq)[None, :]
    gram_n = gram_mat / norm_prod
    attn_prob = jax.nn.softmax(temp_one * gram_n, axis=-1)
    attn_bf = attn_prob.astype(jnp.bfloat16)
    out_head = jnp.dot(v_head, attn_bf.T, preferred_element_type=jnp.float32).astype(jnp.bfloat16)
    d_attn = jnp.dot(dout_head.T, v_head, preferred_element_type=jnp.float32)
    dv_head = jnp.dot(dout_head, attn_bf, preferred_element_type=jnp.float32).astype(jnp.bfloat16)
    d_logit = attn_prob * (d_attn - jnp.sum(attn_prob * d_attn, axis=-1, keepdims=True))
    temp_grad = jnp.sum(d_logit * gram_n)
    grad_sn = temp_one * d_logit
    d_gram = (grad_sn / norm_prod).astype(jnp.bfloat16)
    prod_sn = grad_sn * gram_n
    q_coef = -jnp.sum(prod_sn, axis=1) / q_sq
    k_coef = -jnp.sum(prod_sn, axis=0) / k_sq
    dq_head = (jnp.dot(k_head, d_gram.T, preferred_element_type=jnp.float32) + q_head.astype(jnp.float32) * q_coef[None, :]).astype(jnp.bfloat16)
    dk_head = (jnp.dot(q_head, d_gram, preferred_element_type=jnp.float32) + k_head.astype(jnp.float32) * k_coef[None, :]).astype(jnp.bfloat16)
    return out_head, dq_head, dk_head, dv_head, temp_grad


def reference(x_in, grad_y, w_qkv, w_out, ln_gamma, ln_beta, temperature):
    x_float = x_in.astype(jnp.float32)
    centered = x_float - jnp.mean(x_float, axis=1, keepdims=True)
    inv_std = lax.rsqrt(jnp.mean(centered * centered, axis=1, keepdims=True) + LN_EPS)
    x_hat = centered * inv_std
    u_act = (x_hat * ln_gamma + ln_beta).astype(jnp.bfloat16)
    w_flat = w_qkv.reshape(MODEL_DIM, 3 * MODEL_DIM)
    qkv_act = jnp.dot(u_act, w_flat, preferred_element_type=jnp.float32).astype(jnp.bfloat16)
    qkv_heads = qkv_act.reshape(NUM_TOKENS, 3, NUM_HEADS, HEAD_DIM).transpose(1, 2, 0, 3)
    dout_act = jnp.dot(grad_y, w_out.T, preferred_element_type=jnp.float32).astype(jnp.bfloat16)
    dout_heads = dout_act.reshape(NUM_TOKENS, NUM_HEADS, HEAD_DIM).transpose(1, 0, 2)
    out_heads, dq_heads, dk_heads, dv_heads, grad_temp = lax.map(head_pass, (qkv_heads[0], qkv_heads[1], qkv_heads[2], dout_heads, temperature))
    out_act = out_heads.transpose(1, 0, 2).reshape(NUM_TOKENS, MODEL_DIM)
    y_out = (x_float + jnp.dot(out_act, w_out, preferred_element_type=jnp.float32)).astype(jnp.bfloat16)
    grad_wout = jnp.dot(out_act.T, grad_y, preferred_element_type=jnp.float32)
    dqkv_act = jnp.stack([dq_heads, dk_heads, dv_heads], axis=0).transpose(2, 0, 1, 3).reshape(NUM_TOKENS, 3 * MODEL_DIM)
    grad_wqkv = jnp.dot(u_act.T, dqkv_act, preferred_element_type=jnp.float32).reshape(MODEL_DIM, 3, MODEL_DIM)
    grad_u = jnp.dot(dqkv_act, w_flat.T, preferred_element_type=jnp.float32)
    grad_gamma = jnp.sum(grad_u * x_hat, axis=0)
    grad_beta = jnp.sum(grad_u, axis=0)
    grad_xhat = grad_u * ln_gamma
    grad_ln = inv_std * (grad_xhat - jnp.mean(grad_xhat, axis=1, keepdims=True) - x_hat * jnp.mean(grad_xhat * x_hat, axis=1, keepdims=True))
    grad_x = (grad_y.astype(jnp.float32) + grad_ln).astype(jnp.bfloat16)
    return y_out, grad_x, grad_wqkv, grad_wout, grad_gamma, grad_beta, grad_temp
```

```python
import functools

import jax
import jax.numpy as jnp
from jax import lax
from jax.experimental import pallas as pl
from jax.experimental.pallas import tpu as pltpu
from jax.sharding import PartitionSpec as P

F32, BF16 = jnp.float32, jnp.bfloat16
LN_EPS = 1e-6
NT = 256
CH = 64
MESH = pl.DeviceIdType.MESH


def dot(a, b):
    return jnp.dot(a, b, preferred_element_type=F32)


def dot_nt(a, b):
    return lax.dot_general(a, b, (((1,), (1,)), ((), ())), preferred_element_type=F32)


def fold8(v):
    return jnp.sum(v.reshape(v.shape[0] // 8, 8, v.shape[1]), axis=0)


def ln_stats(xt, cols):
    d = xt.shape[0]
    acc = jnp.zeros((8, NT), F32)
    for c in range(0, d, CH):
        acc = acc + fold8(xt[c : c + CH, cols].astype(F32))
    mean = jnp.sum(acc, axis=0, keepdims=True) * (1.0 / d)
    acc = jnp.zeros((8, NT), F32)
    for c in range(0, d, CH):
        v = xt[c : c + CH, cols].astype(F32) - mean
        acc = acc + fold8(v * v)
    inv = lax.rsqrt(jnp.sum(acc, axis=0, keepdims=True) * (1.0 / d) + LN_EPS)
    return mean, inv


def spread_columns(row_ref, out):
    d = row_ref.shape[1]
    out[...] = jnp.broadcast_to(row_ref[...], (NT, d)).T


def stats_kernel(steps, x_ref, g_ref, w_ref, gam_ref, bet_ref, out_ref, wq, gam, bet, xt, ut, qd, kv, acc, sq):
    step = pl.program_id(0)
    rows, d = x_ref.shape
    own = w_ref.shape[1]
    head = out_ref.shape[0] // 2

    @pl.when(step == 0)
    def _():
        for e in range(3):
            wq[e * own : (e + 1) * own, :] = w_ref[e]
        spread_columns(gam_ref, gam)
        spread_columns(bet_ref, bet)
        acc[...] = jnp.zeros_like(acc)
        sq[...] = jnp.zeros_like(sq)

    for n in range(rows // NT):
        cols = pl.ds(n * NT, NT)
        xt[:, cols] = x_ref[pl.ds(n * NT, NT), :].T
        mean, inv = ln_stats(xt, cols)
        for c in range(0, d, CH):
            v = (xt[c : c + CH, cols].astype(F32) - mean) * inv
            ut[c : c + CH, cols] = (v * gam[c : c + CH, :] + bet[c : c + CH, :]).astype(BF16)
    for n in range(rows // NT):
        cols = pl.ds(n * NT, NT)
        qkv = dot(wq[...], ut[:, cols]).astype(BF16)
        qd[0:own, cols] = qkv[0:own]
        kv[:, cols] = qkv[own:]
        qd[own:, cols] = dot_nt(w_ref[3], g_ref[pl.ds(n * NT, NT), :]).astype(BF16)
    for n in range(rows // NT):
        cols = pl.ds(n * NT, NT)
        for e, ref in enumerate((qd, kv)):
            v = ref[0:own, cols].astype(F32)
            v = v * v
            sq[e] += v[:, :128] + v[:, 128:]
    acc[:, 0 : 2 * own] += dot_nt(qd[...], kv[...])

    @pl.when(step == steps - 1)
    def _():
        lane = lax.broadcasted_iota(jnp.int32, (head, 128), 1)
        for h in range(own // head):
            r = h * head
            gram = pltpu.roll(acc[r : r + head, :], 256 - r, 1)[:, :128] if r else acc[r : r + head, :][:, :128]
            datt = pltpu.roll(acc[own + r : own + r + head, :], 256 - (own + r) + head, 1)[:, :128]
            q2 = jnp.sum(sq[0, r : r + head, :], axis=1, keepdims=True)
            k2 = jnp.sum(sq[1, r : r + head, :], axis=1, keepdims=True)
            v = jnp.where(lane < head, gram, datt)
            v = jnp.where(lane == 2 * head, q2, v)
            out_ref[r : r + head, :] = jnp.where(lane == 2 * head + 1, k2, v)


def stats_call(x, g, w, gam, bet, heads_loc, block=1024):
    rows, d = x.shape
    own = w.shape[1]
    steps = rows // block
    row = pl.BlockSpec((block, d), lambda i: (i, 0))
    full = lambda a: pl.BlockSpec(a.shape, lambda i: (0,) * a.ndim)
    return pl.pallas_call(
        functools.partial(stats_kernel, steps),
        grid=(steps,),
        in_specs=[row, row, full(w), full(gam), full(bet)],
        out_specs=pl.BlockSpec((own, 128), lambda i: (0, 0)),
        out_shape=jax.ShapeDtypeStruct((own, 128), F32),
        scratch_shapes=[
            pltpu.VMEM((3 * own, d), BF16),
            pltpu.VMEM((d, NT), F32),
            pltpu.VMEM((d, NT), F32),
            pltpu.VMEM((d, block), BF16),
            pltpu.VMEM((d, block), BF16),
            pltpu.VMEM((2 * own, block), BF16),
            pltpu.VMEM((2 * own, block), BF16),
            pltpu.VMEM((2 * own, 256), F32),
            pltpu.VMEM((2, own, 128), F32),
        ],
        compiler_params=pltpu.CompilerParams(dimension_semantics=("arbitrary",), vmem_limit_bytes=40 * 2**20),
        cost_estimate=pl.CostEstimate(flops=2 * rows * d * 4 * own, bytes_accessed=4 * rows * d, transcendentals=0),
        name="stats",
    )(x, g, w, gam, bet)


def greet(barrier, peers):
    for peer in peers:
        pl.semaphore_signal(barrier, inc=1, device_id=peer, device_id_type=MESH)
    pl.semaphore_wait(barrier, len(peers))


def state_kernel(tp, sp, s_ref, temp_ref, m1_ref, m2_ref, cq_ref, ck_ref, dt_ref, parts, state, big, send_a, recv_a, send_b, recv_b):
    my_sp, my_tp = lax.axis_index("sp"), lax.axis_index("tp")
    own = s_ref.shape[0]
    heads_loc = temp_ref.shape[0] // tp
    head = own // heads_loc
    d = own * tp
    sp_peers = [{"sp": lax.rem(my_sp + k, sp)} for k in range(1, sp)]
    tp_peers = [{"tp": lax.rem(my_tp + k, tp)} for k in range(1, tp)]
    greet(pltpu.get_barrier_semaphore(), sp_peers + tp_peers)

    copies = []
    for k in range(1, sp):
        copies.append(
            pltpu.make_async_remote_copy(
                src_ref=s_ref,
                dst_ref=parts.at[my_sp],
                send_sem=send_a.at[k],
                recv_sem=recv_a.at[k],
                device_id=sp_peers[k - 1],
                device_id_type=MESH,
            )
        )
        copies[-1].start()
    parts[my_sp] = s_ref[...]
    big[...] = jnp.zeros_like(big)
    for c in copies:
        c.wait()
    total = parts[0]
    for k in range(1, sp):
        total = total + parts[k]

    lane = lax.broadcasted_iota(jnp.int32, (head, 128), 1)
    row = lax.broadcasted_iota(jnp.int32, (head, 128), 0)
    valid = lane < head
    eye = lane == row
    pick = lambda t, i: jnp.sum(jnp.where(lane == i, t, 0.0), axis=1, keepdims=True)
    for h in range(heads_loc):
        t = total[h * head : (h + 1) * head, :]
        tau = temp_ref[my_tp * heads_loc + h]
        gram = t
        datt = pltpu.roll(t, 128 - head, 1)
        q2 = pick(t, 2 * head)
        k2c = pick(t, 2 * head + 1)
        k2 = jnp.sum(jnp.where(eye, k2c, 0.0), axis=0, keepdims=True)
        k2 = jnp.where(valid, k2, 1.0)
        norm = jnp.sqrt(q2) * jnp.sqrt(k2)
        gram_n = jnp.where(valid, gram / norm, 0.0)
        datt = jnp.where(valid, datt, 0.0)
        logit = jnp.where(valid, tau * gram_n, -1e30)
        ex = jnp.exp(logit - jnp.max(logit, axis=1, keepdims=True))
        ex = jnp.where(valid, ex, 0.0)
        att = ex / jnp.sum(ex, axis=1, keepdims=True)
        d_logit = att * (datt - jnp.sum(att * datt, axis=1, keepdims=True))
        d_tau = jnp.sum(jnp.sum(d_logit * gram_n, axis=1, keepdims=True), axis=0, keepdims=True)
        e_mat = tau * d_logit
        d_gram = (e_mat / norm).astype(BF16).astype(F32)
        es = e_mat * gram_n
        q_coef = -jnp.sum(es, axis=1, keepdims=True) / q2
        k_coef = -jnp.sum(es, axis=0, keepdims=True) / k2
        k_coef = jnp.sum(jnp.where(eye, k_coef, 0.0), axis=1, keepdims=True)
        v = jnp.where(valid, att.astype(BF16).astype(F32), pltpu.roll(d_gram, head, 1))
        v = jnp.where(lane == 2 * head, q_coef, v)
        v = jnp.where(lane == 2 * head + 1, k_coef, v)
        v = jnp.where(lane == 2 * head + 2, d_tau, v)
        state[0, h * head : (h + 1) * head, :] = v

    copies = []
    for k in range(1, tp):
        copies.append(
            pltpu.make_async_remote_copy(
                src_ref=state.at[0],
                dst_ref=state.at[tp - k],
                send_sem=send_b.at[k],
                recv_sem=recv_b.at[k],
                device_id=tp_peers[k - 1],
                device_id_type=MESH,
            )
        )
        copies[-1].start()
    for c in copies:
        c.wait()

    head_row = lax.broadcasted_iota(jnp.int32, dt_ref.shape, 0)
    dt = jnp.zeros(dt_ref.shape, F32)
    zero = jnp.zeros((head, d - 128), F32)
    for j in range(tp):
        for h in range(heads_loc):
            t = state[j, h * head : (h + 1) * head, :]
            r = j * own + h * head
            att = jnp.concatenate([jnp.where(valid, t, 0.0), zero], axis=1)
            d_gram = jnp.concatenate([jnp.where(valid, pltpu.roll(t, 128 - head, 1), 0.0), zero], axis=1)
            big[0, r : r + head, :] = pltpu.roll(att, r, 1) if r else att
            big[1, r : r + head, :] = pltpu.roll(d_gram, r, 1) if r else d_gram
            cq_ref[r : r + head, :] = jnp.broadcast_to(pick(t, 2 * head), (head, NT))
            ck_ref[r : r + head, :] = jnp.broadcast_to(pick(t, 2 * head + 1), (head, NT))
            which = lax.rem(my_tp + j, tp) * heads_loc + h
            dt = jnp.where(head_row == which, pick(t, 2 * head + 2)[0:1, :], dt)
    dt_ref[...] = dt
    low = m1_ref.shape[1]
    for i in range(2):
        m = big[i].astype(BF16)
        mt = m.T
        m1_ref[2 * i] = m[0:low, 0:256]
        m2_ref[2 * i] = m[low:, 128:]
        m1_ref[2 * i + 1] = mt[0:low, 0:256]
        m2_ref[2 * i + 1] = mt[low:, 128:]


def state_call(s, temps, tp, sp):
    own = s.shape[0]
    d = own * tp
    head = d // temps.shape[0]
    low = 256 // head * head
    vmem = pl.BlockSpec(memory_space=pltpu.VMEM)
    return pl.pallas_call(
        functools.partial(state_kernel, tp, sp),
        in_specs=[vmem, pl.BlockSpec(memory_space=pltpu.SMEM)],
        out_specs=[vmem] * 5,
        out_shape=[
            jax.ShapeDtypeStruct((4, low, 256), BF16),
            jax.ShapeDtypeStruct((4, d - low, 256), BF16),
            jax.ShapeDtypeStruct((d, NT), F32),
            jax.ShapeDtypeStruct((d, NT), F32),
            jax.ShapeDtypeStruct((temps.shape[0], 128), F32),
        ],
        scratch_shapes=[
            pltpu.VMEM((sp, own, 128), F32),
            pltpu.VMEM((tp, own, 128), F32),
            pltpu.VMEM((2, d, d), F32),
            pltpu.SemaphoreType.DMA((sp,)),
            pltpu.SemaphoreType.DMA((sp,)),
            pltpu.SemaphoreType.DMA((tp,)),
            pltpu.SemaphoreType.DMA((tp,)),
        ],
        compiler_params=pltpu.CompilerParams(collective_id=0, has_side_effects=True),
        name="state",
    )(s, temps)


def main_kernel(steps, x_ref, g_ref, w0, w1, w2, w3, m1, m2, gam_ref, bet_ref, cq, ck, y_ref, dx_ref, dw_ref,
                wt, wn, wo, wot, gam, bet, xt, ut, xh, qkv, do, ot, rt, gx, inv_s, acc_w, acc_o, acc_g):
    step = pl.program_id(0)
    rows, d = x_ref.shape
    pieces = (w0, w1, w2, w3)
    own = w0.shape[1]
    low = m1.shape[1]

    @pl.when(step == 0)
    def _():
        for j, piece in enumerate(pieces):
            for e in range(3):
                wt[e * d + j * own : e * d + (j + 1) * own, :] = piece[e]
            wo[j * own : (j + 1) * own, :] = piece[3]
        for e in range(3):
            wn[:, e * d : (e + 1) * d] = wt[e * d : (e + 1) * d, :].T
        wot[...] = wo[...].T
        spread_columns(gam_ref, gam)
        spread_columns(bet_ref, bet)
        acc_w[...] = jnp.zeros_like(acc_w)
        acc_o[...] = jnp.zeros_like(acc_o)
        acc_g[...] = jnp.zeros_like(acc_g)

    tiles = [(pl.ds(n * NT, NT), pl.ds(n * NT, NT)) for n in range(rows // NT)]
    for cols, _ in tiles:
        xt[:, cols] = x_ref[cols, :].T
        mean, inv = ln_stats(xt, cols)
        inv_s[:, cols] = jnp.broadcast_to(inv, (8, NT))
        for c in range(0, d, CH):
            v = (xt[c : c + CH, cols].astype(F32) - mean) * inv
            xh[c : c + CH, cols] = v
            ut[c : c + CH, cols] = (v * gam[c : c + CH, :] + bet[c : c + CH, :]).astype(BF16)
    for cols, _ in tiles:
        qkv[:, cols] = dot(wt[...], ut[:, cols]).astype(BF16)
        do[:, cols] = dot_nt(wo[...], g_ref[cols, :]).astype(BF16)
    for cols, _ in tiles:
        ot[0:low, cols] = dot(m1[0], qkv[2 * d : 2 * d + 256, cols]).astype(BF16)
        ot[low:d, cols] = dot(m2[0], qkv[2 * d + 128 : 3 * d, cols]).astype(BF16)
        rt[2 * d : 2 * d + low, cols] = dot(m1[1], do[0:256, cols]).astype(BF16)
        rt[2 * d + low : 3 * d, cols] = dot(m2[1], do[128:d, cols]).astype(BF16)
        for part, other, coef, i in ((0, d, cq, 2), (d, 0, ck, 3)):
            v = dot(m1[i], qkv[other : other + 256, cols])
            rt[part : part + low, cols] = (v + qkv[part : part + low, cols].astype(F32) * coef[0:low, :]).astype(BF16)
            v = dot(m2[i], qkv[other + 128 : other + d, cols])
            rt[part + low : part + d, cols] = (v + qkv[part + low : part + d, cols].astype(F32) * coef[low:d, :]).astype(BF16)
    for cols, _ in tiles:
        yt = dot(wot[...], ot[:, cols]) + xt[:, cols].astype(F32)
        y_ref[cols, :] = yt.astype(BF16).T
        gx[:, cols] = dot(wn[...], rt[:, cols])
    for cols, _ in tiles:
        s1 = jnp.zeros((8, NT), F32)
        s2 = jnp.zeros((8, NT), F32)
        for c in range(0, d, CH):
            du = gx[c : c + CH, cols]
            h = xh[c : c + CH, cols]
            acc_g[0, c : c + CH, :] += du * h
            acc_g[1, c : c + CH, :] += du
            a = du * gam[c : c + CH, :]
            s1 = s1 + fold8(a)
            s2 = s2 + fold8(a * h)
            gx[c : c + CH, cols] = a
        mean1 = jnp.sum(s1, axis=0, keepdims=True) * (1.0 / d)
        mean2 = jnp.sum(s2, axis=0, keepdims=True) * (1.0 / d)
        inv = inv_s[0:1, cols]
        for c in range(0, d, CH):
            gx[c : c + CH, cols] = inv * (gx[c : c + CH, cols] - mean1 - xh[c : c + CH, cols] * mean2)
        dxt = gx[:, cols] + g_ref[cols, :].T.astype(F32)
        dx_ref[cols, :] = dxt.astype(BF16).T
    r_own = jnp.concatenate([rt[e * d : e * d + own, :] for e in range(3)], axis=0)
    acc_w[...] += dot_nt(r_own, ut[...])
    acc_o[...] += dot(ot[0:own, :], g_ref[...])

    @pl.when(step == steps - 1)
    def _():
        sp, slot_rows = dw_ref.shape[0], dw_ref.shape[1]
        per = d // sp
        sub = own // sp
        wgrad = acc_w[...].T
        for s in range(sp):
            dw_ref[s, 0:per, 0 : 3 * own] = wgrad[s * per : (s + 1) * per, :]
            for q in range(d // own):
                dw_ref[s, q * sub : (q + 1) * sub, 3 * own :] = acc_o[s * sub : (s + 1) * sub, q * own : (q + 1) * own]
        zero = jnp.zeros((slot_rows - per - 2, d), F32)
        gb = jnp.concatenate([jnp.sum(acc_g[i].T, axis=0, keepdims=True) for i in range(2)] + [zero], axis=0)
        for s in range(sp):
            dw_ref[s, per:slot_rows, :] = gb


def main_call(x, g, pieces, m1, m2, gam, bet, cq, ck, sp, block=1024):
    rows, d = x.shape
    own = pieces[0].shape[1]
    steps = rows // block
    row = pl.BlockSpec((block, d), lambda i: (i, 0))
    full = lambda a: pl.BlockSpec(a.shape, lambda i: (0,) * a.ndim)
    slot = (sp, d // sp + 8, d)
    smalls = (*pieces, m1, m2, gam, bet, cq, ck)
    return pl.pallas_call(
        functools.partial(main_kernel, steps),
        grid=(steps,),
        in_specs=[row, row] + [full(a) for a in smalls],
        out_specs=[row, row, pl.BlockSpec(slot, lambda i: (0, 0, 0))],
        out_shape=[jax.ShapeDtypeStruct((rows, d), BF16), jax.ShapeDtypeStruct((rows, d), BF16), jax.ShapeDtypeStruct(slot, F32)],
        scratch_shapes=[
            pltpu.VMEM((3 * d, d), BF16),
            pltpu.VMEM((d, 3 * d), BF16),
            pltpu.VMEM((d, d), BF16),
            pltpu.VMEM((d, d), BF16),
            pltpu.VMEM((d, NT), F32),
            pltpu.VMEM((d, NT), F32),
            pltpu.VMEM((d, block), BF16),
            pltpu.VMEM((d, block), BF16),
            pltpu.VMEM((d, block), F32),
            pltpu.VMEM((3 * d, block), BF16),
            pltpu.VMEM((d, block), BF16),
            pltpu.VMEM((d, block), BF16),
            pltpu.VMEM((3 * d, block), BF16),
            pltpu.VMEM((d, block), F32),
            pltpu.VMEM((8, block), F32),
            pltpu.VMEM((3 * own, d), F32),
            pltpu.VMEM((own, d), F32),
            pltpu.VMEM((2, d, NT), F32),
        ],
        compiler_params=pltpu.CompilerParams(dimension_semantics=("arbitrary",), vmem_limit_bytes=60 * 2**20),
        cost_estimate=pl.CostEstimate(flops=2 * rows * d * d * 9, bytes_accessed=8 * rows * d, transcendentals=0),
        name="main",
    )(x, g, *smalls)


def wgrad_kernel(sp, in_ref, out_ref, pair, got, send_a, recv_a, send_b, recv_b):
    my = lax.axis_index("sp")
    chips = sp // 2
    core, chip = lax.rem(my, 2), my // 2
    other = {"sp": chip * 2 + 1 - core}
    peers = [{"sp": lax.rem(chip + k, chips) * 2 + core} for k in range(1, chips)]
    greet(pltpu.get_barrier_semaphore(), [other] + peers)
    first = []
    for c in range(chips):
        first.append(
            pltpu.make_async_remote_copy(
                src_ref=in_ref.at[2 * c + 1 - core],
                dst_ref=pair.at[c],
                send_sem=send_a.at[c],
                recv_sem=recv_a.at[c],
                device_id=other,
                device_id_type=MESH,
            )
        )
        first[-1].start()
    for c in range(chips):
        first[c].wait()
    for c in range(chips):
        got[chips + c] = in_ref[2 * c + core] + pair[c]
    second = []
    for k in range(1, chips):
        second.append(
            pltpu.make_async_remote_copy(
                src_ref=got.at[chips + lax.rem(chip + k, chips)],
                dst_ref=got.at[chip],
                send_sem=send_b.at[k],
                recv_sem=recv_b.at[k],
                device_id=peers[k - 1],
                device_id_type=MESH,
            )
        )
        second[-1].start()
    got[chip] = got[chips + chip]
    for c in second:
        c.wait()
    total = got[0]
    for c in range(1, chips):
        total = total + got[c]
    out_ref[...] = total


def wgrad_call(parts):
    sp, slot = parts.shape[0], parts.shape[1:]
    vmem = pl.BlockSpec(memory_space=pltpu.VMEM)
    return pl.pallas_call(
        functools.partial(wgrad_kernel, sp),
        in_specs=[vmem],
        out_specs=vmem,
        out_shape=jax.ShapeDtypeStruct(slot, F32),
        scratch_shapes=[
            pltpu.VMEM((sp // 2, *slot), F32),
            pltpu.VMEM((sp, *slot), F32),
            pltpu.SemaphoreType.DMA((sp // 2,)),
            pltpu.SemaphoreType.DMA((sp // 2,)),
            pltpu.SemaphoreType.DMA((sp // 2,)),
            pltpu.SemaphoreType.DMA((sp // 2,)),
        ],
        compiler_params=pltpu.CompilerParams(collective_id=1, has_side_effects=True),
        name="wgrad",
    )(parts)


def solution(mesh):
    tp, sp = mesh.shape["tp"], mesh.shape["sp"]
    row_spec = P(("dp", "sp"), None)

    def local_step(x, g, w_qkv, w_out, gamma, beta, temps):
        d = x.shape[1]
        own = w_qkv.shape[2]
        heads_loc = temps.shape[0] // tp
        gam, bet = gamma.reshape(1, d), beta.reshape(1, d)
        piece = jnp.concatenate([w_qkv.transpose(1, 2, 0), w_out[None]], axis=0)
        pieces = [piece]
        for j in range(1, tp):
            pieces.append(lax.ppermute(piece, "tp", [(i, (i - j) % tp) for i in range(tp)]))
        s = stats_call(x, g, piece, gam, bet, heads_loc)
        m1, m2, cq, ck, dt = state_call(s, temps, tp, sp)
        y, dx, parts = main_call(x, g, pieces, m1, m2, gam, bet, cq, ck, sp)
        got = wgrad_call(parts)
        per = d // sp
        sub = own // sp
        grad_wqkv = got[:per, : 3 * own].reshape(per, 3, own)
        grad_wout = got[:per, 3 * own :].reshape(tp, sub, own).transpose(1, 0, 2).reshape(sub, d)
        return y, dx, grad_wqkv, grad_wout, got[per], got[per + 1], dt[:, 0]

    in_specs = (row_spec, row_spec, P(None, None, "tp"), P("tp", None), P(None), P(None), P(None))
    out_specs = (row_spec, row_spec, P(("dp", "sp"), None, "tp"), P(("dp", "tp", "sp"), None), P("dp"), P("dp"), P("dp"))
    return jax.shard_map(local_step, mesh=mesh, in_specs=in_specs, out_specs=out_specs, check_vma=False)
```

```python
import functools

import jax
import jax.numpy as jnp
from jax import lax
from jax.experimental import pallas as pl
from jax.experimental.pallas import tpu as pltpu
from jax.sharding import PartitionSpec as P

F32, BF16 = jnp.float32, jnp.bfloat16
LN_EPS = 1e-6
NT = 256
CH = 64
LANES = 128
MESH = pl.DeviceIdType.MESH


def dot(a, b):
    return jnp.dot(a, b, preferred_element_type=F32)


def dot_nt(a, b):
    return lax.dot_general(a, b, (((1,), (1,)), ((), ())), preferred_element_type=F32)


def fold8(v):
    return jnp.sum(v.reshape(v.shape[0] // 8, 8, v.shape[1]), axis=0)


def ln_stats(xt, cols):
    d = xt.shape[0]
    shift = xt[0:16, cols].astype(F32)[0:1, :]
    s1 = jnp.zeros((8, NT), F32)
    s2 = jnp.zeros((8, NT), F32)
    for c in range(0, d, CH):
        v = xt[c : c + CH, cols].astype(F32) - shift
        s1 = s1 + fold8(v)
        s2 = s2 + fold8(v * v)
    off = jnp.sum(s1, axis=0, keepdims=True) * (1.0 / d)
    var = jnp.sum(s2, axis=0, keepdims=True) * (1.0 / d) - off * off
    return shift + off, lax.rsqrt(jnp.maximum(var, 0.0) + LN_EPS)


def spread_columns(row_ref, out):
    d = row_ref.shape[0]
    out[...] = jnp.broadcast_to(row_ref[...].reshape(1, d), (NT, d)).T


def remote(src, dst, send_sem, recv_sem, device):
    return pltpu.make_async_remote_copy(
        src_ref=src, dst_ref=dst, send_sem=send_sem, recv_sem=recv_sem, device_id=device, device_id_type=MESH
    )


def head_state(t, tau, head):
    lane = lax.broadcasted_iota(jnp.int32, (head, LANES), 1)
    row = lax.broadcasted_iota(jnp.int32, (head, LANES), 0)
    valid = lane < head
    eye = lane == row
    pick = lambda i: jnp.sum(jnp.where(lane == i, t, 0.0), axis=1, keepdims=True)
    q2 = pick(2 * head)
    k2 = jnp.sum(jnp.where(eye, pick(2 * head + 1), 0.0), axis=0, keepdims=True)
    k2 = jnp.where(valid, k2, 1.0)
    norm = jnp.sqrt(q2) * jnp.sqrt(k2)
    gram_n = jnp.where(valid, t / norm, 0.0)
    datt = jnp.where(valid, pltpu.roll(t, LANES - head, 1), 0.0)
    logit = jnp.where(valid, tau * gram_n, -1e30)
    ex = jnp.exp(logit - jnp.max(logit, axis=1, keepdims=True))
    ex = jnp.where(valid, ex, 0.0)
    att = ex / jnp.sum(ex, axis=1, keepdims=True)
    d_logit = att * (datt - jnp.sum(att * datt, axis=1, keepdims=True))
    d_tau = jnp.sum(jnp.sum(d_logit * gram_n, axis=1, keepdims=True), axis=0, keepdims=True)
    e_mat = tau * d_logit
    d_gram = (e_mat / norm).astype(BF16).astype(F32)
    es = e_mat * gram_n
    q_coef = -jnp.sum(es, axis=1, keepdims=True) / q2
    k_coef = -jnp.sum(es, axis=0, keepdims=True) / k2
    k_coef = jnp.sum(jnp.where(eye, k_coef, 0.0), axis=1, keepdims=True)
    v = jnp.where(valid, att.astype(BF16).astype(F32), pltpu.roll(d_gram, head, 1))
    v = jnp.where(lane == 2 * head, q_coef, v)
    v = jnp.where(lane == 2 * head + 1, k_coef, v)
    return jnp.where(lane == 2 * head + 2, d_tau, v)


def front_kernel(tp, sp, steps, x_ref, g_ref, w_ref, w4_ref, gam_ref, bet_ref, temp_ref,
                 save_ref, wt_ref, wn_ref, wo_ref, wot_ref, m1_ref, m2_ref, cq_ref, ck_ref, dt_ref,
                 wq, gam, bet, xt, gt, ut, qd, kv, acc, sq, wall, sums, pair, parts, state, big,
                 send_w, recv_w, send_p, recv_p, send_a, recv_a, send_b, recv_b):
    step = pl.program_id(0)
    my_sp, my_tp = lax.axis_index("sp"), lax.axis_index("tp")
    chips = sp // 2
    core, chip = lax.rem(my_sp, 2), my_sp // 2
    rows, d = x_ref.shape
    own = w4_ref.shape[0]
    head = own // 2
    rest = d - own
    other = {"sp": chip * 2 + 1 - core}
    chip_peers = [{"sp": lax.rem(chip + k, chips) * 2 + core} for k in range(1, chips)]
    tp_peers = [[{"tp": lax.rem(my_tp + k, tp), "sp": chip * 2 + t} for t in range(2)] for k in range(1, tp)]
    barrier = pltpu.get_barrier_semaphore()
    peers = [other] + chip_peers + [p for ps in tp_peers for p in ps]

    @pl.when(step == 0)
    def _():
        for peer in peers:
            pl.semaphore_signal(barrier, inc=1, device_id=peer, device_id_type=MESH)
        for e in range(3):
            wq[e * own : (e + 1) * own, :] = w_ref[e]
        spread_columns(gam_ref, gam)
        spread_columns(bet_ref, bet)
        acc[...] = jnp.zeros_like(acc)
        sq[...] = jnp.zeros_like(sq)
        big[...] = jnp.zeros_like(big)

    def weight_copies():
        out = []
        for k in range(1, tp):
            for i, (src, dst) in enumerate(((w_ref, wall.at[tp - k, 0:3]), (w4_ref, wall.at[tp - k, 3]))):
                peer = {"tp": lax.rem(my_tp + k, tp), "sp": my_sp}
                out.append(remote(src, dst, send_w.at[k, i], recv_w.at[k, i], peer))
        return out

    @pl.when(step == 1)
    def _():
        pl.semaphore_wait(barrier, len(peers))
        for c in weight_copies():
            c.start()

    tiles = rows // NT
    at = lambda n: pl.ds(n * NT, NT)

    def norm(n):
        xt[:, at(n)] = x_ref[at(n), :].T
        gt[:, at(n)] = g_ref[at(n), :].T
        mean, inv = ln_stats(xt, at(n))
        mean = mean * inv
        for c in range(0, d, CH):
            v = xt[c : c + CH, at(n)].astype(F32) * inv - mean
            ut[c : c + CH, at(n)] = (v * gam[c : c + CH, :] + bet[c : c + CH, :]).astype(BF16)

    def project(n):
        qkv = dot(wq[...], ut[:, at(n)])
        for e, ref in enumerate((qd, kv)):
            v = qkv[e * own : (e + 1) * own].astype(BF16)
            ref[0:own, at(n)] = v
            save_ref[e * own : (e + 1) * own, at(n)] = v
            v = v.astype(F32)
            v = v * v
            sq[e] += v[:, :128] + v[:, 128:]
        v = qkv[2 * own :].astype(BF16)
        kv[own:, at(n)] = v
        save_ref[2 * own : 3 * own, at(n)] = v
        v = dot(w4_ref[...], gt[:, at(n)]).astype(BF16)
        qd[own:, at(n)] = v
        save_ref[3 * own :, at(n)] = v

    norm(0)
    for n in range(tiles):
        if n + 1 < tiles:
            norm(n + 1)
        project(n)
    acc[:, 0 : 2 * own] += dot_nt(qd[...], kv[...])

    @pl.when(step == steps - 1)
    def _():
        lane = lax.broadcasted_iota(jnp.int32, (head, LANES), 1)
        valid = lane < head
        for h in range(2):
            r = h * head
            gram = pltpu.roll(acc[r : r + head, :], 256 - r, 1)[:, :128] if r else acc[r : r + head, :][:, :128]
            datt = pltpu.roll(acc[own + r : own + r + head, :], 256 - (own + r) + head, 1)[:, :128]
            q2 = jnp.sum(sq[0, r : r + head, :], axis=1, keepdims=True)
            k2 = jnp.sum(sq[1, r : r + head, :], axis=1, keepdims=True)
            v = jnp.where(valid, gram, datt)
            v = jnp.where(lane == 2 * head, q2, v)
            sums[r : r + head, :] = jnp.where(lane == 2 * head + 1, k2, v)

        mine = pl.ds(pl.multiple_of(core * head, 8), head)
        theirs = pl.ds(pl.multiple_of((1 - core) * head, 8), head)
        first = remote(sums.at[theirs], pair, send_p.at[0], recv_p.at[0], other)
        first.start()
        for c in weight_copies():
            c.wait()
        first.wait()
        parts[chip] = sums[mine, :] + pair[...]
        copies = [
            remote(parts.at[chip], parts.at[chip], send_a.at[k], recv_a.at[k], chip_peers[k - 1]) for k in range(1, chips)
        ]
        for c in copies:
            c.start()
        pieces = [(w_ref, w4_ref)] + [(wall.at[j, 0:3], wall.at[j, 3]) for j in range(1, tp)]
        for j, (piece, piece4) in enumerate(pieces):
            for e in range(3):
                wn_ref[:, e * d + j * own : e * d + (j + 1) * own] = piece[e].T
                if j:
                    wt_ref[e * rest + (j - 1) * own : e * rest + j * own, :] = piece[e]
            wot_ref[:, j * own : (j + 1) * own] = piece4[...].T
            if j:
                wo_ref[(j - 1) * own : j * own, :] = piece4[...]
        for c in copies:
            c.wait()
        total = parts[0]
        for k in range(1, chips):
            total = total + parts[k]
        state[0, core] = head_state(total, temp_ref[my_tp * 2 + core], head)

        copies = [remote(state.at[0, core], state.at[0, core], send_b.at[0, 0], recv_b.at[0, core], other)]
        for k in range(1, tp):
            for t in range(2):
                copies.append(
                    remote(state.at[0, core], state.at[tp - k, core], send_b.at[k, t], recv_b.at[k, core], tp_peers[k - 1][t])
                )
        for c in copies:
            c.start()
        for c in copies:
            c.wait_send()
        remote(state.at[0, core], state.at[0, 1 - core], send_b.at[0, 0], recv_b.at[0, 1 - core], other).wait_recv()
        for k in range(1, tp):
            for t in range(2):
                remote(state.at[0, core], state.at[tp - k, t], send_b.at[k, t], recv_b.at[k, t], tp_peers[k - 1][t]).wait_recv()

        lane1 = lax.broadcasted_iota(jnp.int32, dt_ref.shape, 1)
        dt = jnp.zeros(dt_ref.shape, F32)
        zero = jnp.zeros((head, d - LANES), F32)
        for j in range(tp):
            for h in range(2):
                t = state[j, h]
                pick = lambda i: jnp.sum(jnp.where(lane == i, t, 0.0), axis=1, keepdims=True)
                r = j * own + h * head
                att = jnp.concatenate([jnp.where(valid, t, 0.0), zero], axis=1)
                d_gram = jnp.concatenate([jnp.where(valid, pltpu.roll(t, LANES - head, 1), 0.0), zero], axis=1)
                big[0, r : r + head, :] = pltpu.roll(att, r, 1) if r else att
                big[1, r : r + head, :] = pltpu.roll(d_gram, r, 1) if r else d_gram
                cq_ref[r : r + head, :] = jnp.broadcast_to(pick(2 * head), (head, NT))
                ck_ref[r : r + head, :] = jnp.broadcast_to(pick(2 * head + 1), (head, NT))
                which = lax.rem(my_tp + j, tp) * 2 + h
                dt = jnp.where(lane1 == which, pick(2 * head + 2)[0:1, :], dt)
        dt_ref[...] = dt
        low = m1_ref.shape[1]
        for i in range(2):
            m = big[i].astype(BF16)
            mt = m.T
            m1_ref[2 * i] = m[0:low, 0:256]
            m2_ref[2 * i] = m[low:, 128:]
            m1_ref[2 * i + 1] = mt[0:low, 0:256]
            m2_ref[2 * i + 1] = mt[low:, 128:]


def front_call(x, g, w, w4, gam, bet, temps, tp, sp, block=2048):
    rows, d = x.shape
    own = w4.shape[0]
    head = d // temps.shape[0]
    low = 256 // head * head
    steps = rows // block
    row = pl.BlockSpec((block, d), lambda i: (i, 0))
    full = lambda shape: pl.BlockSpec(shape, lambda i: (0,) * len(shape))
    smalls = [
        ((3 * (d - own), d), BF16),
        ((d, 3 * d), BF16),
        ((d - own, d), BF16),
        ((d, d), BF16),
        ((4, low, 256), BF16),
        ((4, d - low, 256), BF16),
        ((d, NT), F32),
        ((d, NT), F32),
        ((1, LANES), F32),
    ]
    dma = pltpu.SemaphoreType.DMA
    return pl.pallas_call(
        functools.partial(front_kernel, tp, sp, steps),
        grid=(steps,),
        in_specs=[row, row, full(w.shape), full(w4.shape), full(gam.shape), full(bet.shape), pl.BlockSpec(memory_space=pltpu.SMEM)],
        out_specs=[pl.BlockSpec((4 * own, block), lambda i: (0, i))] + [full(s) for s, _ in smalls],
        out_shape=[jax.ShapeDtypeStruct((4 * own, rows), BF16)] + [jax.ShapeDtypeStruct(s, t) for s, t in smalls],
        scratch_shapes=[
            pltpu.VMEM((3 * own, d), BF16),
            pltpu.VMEM((d, NT), F32),
            pltpu.VMEM((d, NT), F32),
            pltpu.VMEM((d, block), BF16),
            pltpu.VMEM((d, block), BF16),
            pltpu.VMEM((d, block), BF16),
            pltpu.VMEM((2 * own, block), BF16),
            pltpu.VMEM((2 * own, block), BF16),
            pltpu.VMEM((2 * own, 256), F32),
            pltpu.VMEM((2, own, 128), F32),
            pltpu.VMEM((tp, 4, own, d), BF16),
            pltpu.VMEM((own, LANES), F32),
            pltpu.VMEM((head, LANES), F32),
            pltpu.VMEM((sp // 2, head, LANES), F32),
            pltpu.VMEM((tp, 2, head, LANES), F32),
            pltpu.VMEM((2, d, d), F32),
            dma((tp, 2)),
            dma((tp, 2)),
            dma((1,)),
            dma((1,)),
            dma((sp // 2,)),
            dma((sp // 2,)),
            dma((tp, 2)),
            dma((tp, 2)),
        ],
        compiler_params=pltpu.CompilerParams(
            dimension_semantics=("arbitrary",), vmem_limit_bytes=60 * 2**20, collective_id=0, has_side_effects=True
        ),
        cost_estimate=pl.CostEstimate(flops=2 * rows * d * 4 * own, bytes_accessed=4 * rows * d, transcendentals=0),
        name="front",
    )(x, g, w, w4, gam, bet, temps)


def main_kernel(steps, x_ref, g_ref, save_ref, wt, wn, wo, wot, m1, m2, gam_ref, bet_ref, cq, ck, y_ref, dx_ref, dw_ref,
                gam, bet, xt, ut, xh, qkv, do, ot, rt, gx, inv_s, acc_w, acc_o, acc_g):
    step = pl.program_id(0)
    rows, d = x_ref.shape
    rest = wo.shape[0]
    own = d - rest
    low = m1.shape[1]

    @pl.when(step == 0)
    def _():
        spread_columns(gam_ref, gam)
        spread_columns(bet_ref, bet)
        acc_w[...] = jnp.zeros_like(acc_w)
        acc_o[...] = jnp.zeros_like(acc_o)
        acc_g[...] = jnp.zeros_like(acc_g)

    tiles = rows // NT
    at = lambda n: pl.ds(n * NT, NT)

    def norm(n):
        xt[:, at(n)] = x_ref[at(n), :].T
        mean, inv = ln_stats(xt, at(n))
        inv_s[:, at(n)] = jnp.broadcast_to(inv, (8, NT))
        mean = mean * inv
        for c in range(0, d, CH):
            v = xt[c : c + CH, at(n)].astype(F32) * inv - mean
            xh[c : c + CH, at(n)] = v
            ut[c : c + CH, at(n)] = (v * gam[c : c + CH, :] + bet[c : c + CH, :]).astype(BF16)

    def project(n):
        for e in range(3):
            qkv[e * d : e * d + own, at(n)] = save_ref[e * own : (e + 1) * own, at(n)]
            qkv[e * d + own : (e + 1) * d, at(n)] = dot(wt[e * rest : (e + 1) * rest, :], ut[:, at(n)]).astype(BF16)
        do[0:own, at(n)] = save_ref[3 * own :, at(n)]
        do[own:, at(n)] = dot_nt(wo[...], g_ref[at(n), :]).astype(BF16)

    def mix(n):
        ot[0:low, at(n)] = dot(m1[0], qkv[2 * d : 2 * d + 256, at(n)]).astype(BF16)
        ot[low:d, at(n)] = dot(m2[0], qkv[2 * d + 128 : 3 * d, at(n)]).astype(BF16)
        rt[2 * d : 2 * d + low, at(n)] = dot(m1[1], do[0:256, at(n)]).astype(BF16)
        rt[2 * d + low : 3 * d, at(n)] = dot(m2[1], do[128:d, at(n)]).astype(BF16)
        for part, other, coef, i in ((0, d, cq, 2), (d, 0, ck, 3)):
            v = dot(m1[i], qkv[other : other + 256, at(n)])
            rt[part : part + low, at(n)] = (v + qkv[part : part + low, at(n)].astype(F32) * coef[0:low, :]).astype(BF16)
            v = dot(m2[i], qkv[other + 128 : other + d, at(n)])
            rt[part + low : part + d, at(n)] = (v + qkv[part + low : part + d, at(n)].astype(F32) * coef[low:d, :]).astype(BF16)

    def out(n):
        for c, m in ((0, 128), (128, 256)):
            yt = dot(wot[c : c + m, :], ot[:, at(n)]) + xt[c : c + m, at(n)].astype(F32)
            y_ref[at(n), c : c + m] = yt.astype(BF16).T
        gx[:, at(n)] = dot(wn[...], rt[:, at(n)])

    def norm_bwd(n):
        s1 = jnp.zeros((8, NT), F32)
        s2 = jnp.zeros((8, NT), F32)
        for c in range(0, d, CH):
            du = gx[c : c + CH, at(n)]
            h = xh[c : c + CH, at(n)]
            acc_g[0, c : c + CH, :] += du * h
            acc_g[1, c : c + CH, :] += du
            a = du * gam[c : c + CH, :]
            s1 = s1 + fold8(a)
            s2 = s2 + fold8(a * h)
            gx[c : c + CH, at(n)] = a
        mean1 = jnp.sum(s1, axis=0, keepdims=True) * (1.0 / d)
        mean2 = jnp.sum(s2, axis=0, keepdims=True) * (1.0 / d)
        inv = inv_s[0:1, at(n)]
        for c in range(0, d, CH):
            v = inv * (gx[c : c + CH, at(n)] - mean1 - xh[c : c + CH, at(n)] * mean2)
            gx[c : c + CH, at(n)] = v
        dxt = gx[:, at(n)] + g_ref[at(n), :].T.astype(F32)
        dx_ref[at(n), :] = dxt.astype(BF16).T

    stages = (norm, project, mix, out, norm_bwd)
    for n in range(tiles + len(stages) - 1):
        for k in reversed(range(len(stages))):
            if 0 <= n - k < tiles:
                stages[k](n - k)
    r_own = jnp.concatenate([rt[e * d : e * d + own, :] for e in range(3)], axis=0)
    acc_w[...] += dot_nt(r_own, ut[...])
    acc_o[...] += dot(ot[0:own, :], g_ref[...])

    @pl.when(step == steps - 1)
    def _():
        sp, slot_rows = dw_ref.shape[0], dw_ref.shape[1]
        per = d // sp
        sub = own // sp
        wgrad = acc_w[...].T
        for s in range(sp):
            dw_ref[s, 0:per, 0 : 3 * own] = wgrad[s * per : (s + 1) * per, :]
            for q in range(d // own):
                dw_ref[s, q * sub : (q + 1) * sub, 3 * own :] = acc_o[s * sub : (s + 1) * sub, q * own : (q + 1) * own]
        zero = jnp.zeros((slot_rows - per - 2, d), F32)
        gb = jnp.concatenate([jnp.sum(acc_g[i].T, axis=0, keepdims=True) for i in range(2)] + [zero], axis=0)
        for s in range(sp):
            dw_ref[s, per:slot_rows, :] = gb


def main_call(x, g, save, wt, wn, wo, wot, m1, m2, gam, bet, cq, ck, sp, block=2048):
    rows, d = x.shape
    own = d - wo.shape[0]
    steps = rows // block
    row = pl.BlockSpec((block, d), lambda i: (i, 0))
    full = lambda a: pl.BlockSpec(a.shape, lambda i: (0,) * a.ndim)
    slot = (sp, d // sp + 8, d)
    smalls = (wt, wn, wo, wot, m1, m2, gam, bet, cq, ck)
    return pl.pallas_call(
        functools.partial(main_kernel, steps),
        grid=(steps,),
        in_specs=[row, row, pl.BlockSpec((4 * own, block), lambda i: (0, i))] + [full(a) for a in smalls],
        out_specs=[row, row, pl.BlockSpec(slot, lambda i: (0, 0, 0))],
        out_shape=[jax.ShapeDtypeStruct((rows, d), BF16), jax.ShapeDtypeStruct((rows, d), BF16), jax.ShapeDtypeStruct(slot, F32)],
        scratch_shapes=[
            pltpu.VMEM((d, NT), F32),
            pltpu.VMEM((d, NT), F32),
            pltpu.VMEM((d, block), BF16),
            pltpu.VMEM((d, block), BF16),
            pltpu.VMEM((d, block), F32),
            pltpu.VMEM((3 * d, block), BF16),
            pltpu.VMEM((d, block), BF16),
            pltpu.VMEM((d, block), BF16),
            pltpu.VMEM((3 * d, block), BF16),
            pltpu.VMEM((d, block), F32),
            pltpu.VMEM((8, block), F32),
            pltpu.VMEM((3 * own, d), F32),
            pltpu.VMEM((own, d), F32),
            pltpu.VMEM((2, d, NT), F32),
        ],
        compiler_params=pltpu.CompilerParams(dimension_semantics=("arbitrary",), vmem_limit_bytes=60 * 2**20),
        cost_estimate=pl.CostEstimate(flops=2 * rows * d * d * 9, bytes_accessed=8 * rows * d, transcendentals=0),
        name="main",
    )(x, g, save, *smalls)


def wgrad_kernel(sp, in_ref, w_ref, o_ref, gam_ref, bet_ref, pair, got, send_a, recv_a, send_b, recv_b):
    my = lax.axis_index("sp")
    chips = sp // 2
    core, chip = lax.rem(my, 2), my // 2
    other = {"sp": chip * 2 + 1 - core}
    peers = [{"sp": lax.rem(chip + k, chips) * 2 + core} for k in range(1, chips)]
    barrier = pltpu.get_barrier_semaphore()
    for peer in [other] + peers:
        pl.semaphore_signal(barrier, inc=1, device_id=peer, device_id_type=MESH)
    pl.semaphore_wait(barrier, chips)
    first = [remote(in_ref.at[2 * c + 1 - core], pair.at[c], send_a.at[c], recv_a.at[c], other) for c in range(chips)]
    for c in first:
        c.start()
    for c in range(chips):
        first[c].wait()
    for c in range(chips):
        got[chips + c] = in_ref[2 * c + core] + pair[c]
    second = [
        remote(got.at[chips + lax.rem(chip + k, chips)], got.at[chip], send_b.at[k], recv_b.at[k], peers[k - 1])
        for k in range(1, chips)
    ]
    for c in second:
        c.start()
    got[chip] = got[chips + chip]
    for c in second:
        c.wait()
    total = got[0]
    for c in range(1, chips):
        total = total + got[c]
    per, own = w_ref.shape[1:]
    sub = o_ref.shape[0]
    for e in range(3):
        w_ref[e] = total[0:per, e * own : (e + 1) * own]
    for q in range(o_ref.shape[1] // own):
        o_ref[:, q * own : (q + 1) * own] = total[q * sub : (q + 1) * sub, 3 * own :]
    gam_ref[...] = total[per]
    bet_ref[...] = total[per + 1]


def wgrad_call(parts, own):
    sp, rows, d = parts.shape
    vmem = pl.BlockSpec(memory_space=pltpu.VMEM)
    return pl.pallas_call(
        functools.partial(wgrad_kernel, sp),
        in_specs=[vmem],
        out_specs=[vmem] * 4,
        out_shape=[
            jax.ShapeDtypeStruct((3, d // sp, own), F32),
            jax.ShapeDtypeStruct((own // sp, d), F32),
            jax.ShapeDtypeStruct((d,), F32),
            jax.ShapeDtypeStruct((d,), F32),
        ],
        scratch_shapes=[
            pltpu.VMEM((sp // 2, rows, d), F32),
            pltpu.VMEM((sp, rows, d), F32),
            pltpu.SemaphoreType.DMA((sp // 2,)),
            pltpu.SemaphoreType.DMA((sp // 2,)),
            pltpu.SemaphoreType.DMA((sp // 2,)),
            pltpu.SemaphoreType.DMA((sp // 2,)),
        ],
        compiler_params=pltpu.CompilerParams(collective_id=1, has_side_effects=True),
        name="wgrad",
    )(parts)


def solution(mesh):
    tp, sp = mesh.shape["tp"], mesh.shape["sp"]
    row_spec = P(("dp", "sp"), None)

    def local_step(x, g, w_qkv, w_out, gamma, beta, temps):
        save, wt, wn, wo, wot, m1, m2, cq, ck, dt = front_call(
            x, g, w_qkv.transpose(1, 2, 0), w_out, gamma, beta, temps, tp, sp
        )
        y, dx, parts = main_call(x, g, save, wt, wn, wo, wot, m1, m2, gamma, beta, cq, ck, sp)
        grad_w, grad_o, grad_gamma, grad_beta = wgrad_call(parts, w_out.shape[0])
        return y, dx, grad_w.transpose(1, 0, 2), grad_o, grad_gamma, grad_beta, dt[0, : temps.shape[0]]

    in_specs = (row_spec, row_spec, P(None, None, "tp"), P("tp", None), P(None), P(None), P(None))
    out_specs = (row_spec, row_spec, P(("dp", "sp"), None, "tp"), P(("dp", "tp", "sp"), None), P("dp"), P("dp"), P("dp"))
    return jax.shard_map(local_step, mesh=mesh, in_specs=in_specs, out_specs=out_specs, check_vma=False)
```

```python
import functools

import jax
import jax.numpy as jnp
from jax import lax
from jax.experimental import pallas as pl
from jax.experimental.pallas import tpu as pltpu
from jax.sharding import PartitionSpec as P

F32, BF16 = jnp.float32, jnp.bfloat16
LN_EPS = 1e-6
NT = 256
CH = 64
LANES = 128
MESH = pl.DeviceIdType.MESH


def dot(a, b):
    return jnp.dot(a, b, preferred_element_type=F32)


def dot_nt(a, b):
    return lax.dot_general(a, b, (((1,), (1,)), ((), ())), preferred_element_type=F32)


def fold8(v):
    return jnp.sum(v.reshape(v.shape[0] // 8, 8, v.shape[1]), axis=0)


def ln_stats(xt, cols):
    d = xt.shape[0]
    shift = xt[0:16, cols].astype(F32)[0:1, :]
    s1 = jnp.zeros((8, NT), F32)
    s2 = jnp.zeros((8, NT), F32)
    for c in range(0, d, CH):
        v = xt[c : c + CH, cols].astype(F32) - shift
        s1 = s1 + fold8(v)
        s2 = s2 + fold8(v * v)
    off = jnp.sum(s1, axis=0, keepdims=True) * (1.0 / d)
    var = jnp.sum(s2, axis=0, keepdims=True) * (1.0 / d) - off * off
    return shift + off, lax.rsqrt(jnp.maximum(var, 0.0) + LN_EPS)


def spread_columns(row_ref, out):
    d = row_ref.shape[0]
    out[...] = jnp.broadcast_to(row_ref[...].reshape(1, d), (NT, d)).T


def remote(src, dst, send_sem, recv_sem, device):
    return pltpu.make_async_remote_copy(
        src_ref=src, dst_ref=dst, send_sem=send_sem, recv_sem=recv_sem, device_id=device, device_id_type=MESH
    )


def head_state(t, tau, head):
    lane = lax.broadcasted_iota(jnp.int32, (head, LANES), 1)
    row = lax.broadcasted_iota(jnp.int32, (head, LANES), 0)
    valid = lane < head
    eye = lane == row
    pick = lambda i: jnp.sum(jnp.where(lane == i, t, 0.0), axis=1, keepdims=True)
    q2 = pick(2 * head)
    k2 = jnp.sum(jnp.where(eye, pick(2 * head + 1), 0.0), axis=0, keepdims=True)
    k2 = jnp.where(valid, k2, 1.0)
    norm = jnp.sqrt(q2) * jnp.sqrt(k2)
    gram_n = jnp.where(valid, t / norm, 0.0)
    datt = jnp.where(valid, pltpu.roll(t, LANES - head, 1), 0.0)
    logit = jnp.where(valid, tau * gram_n, -1e30)
    ex = jnp.exp(logit - jnp.max(logit, axis=1, keepdims=True))
    ex = jnp.where(valid, ex, 0.0)
    att = ex / jnp.sum(ex, axis=1, keepdims=True)
    d_logit = att * (datt - jnp.sum(att * datt, axis=1, keepdims=True))
    d_tau = jnp.sum(jnp.sum(d_logit * gram_n, axis=1, keepdims=True), axis=0, keepdims=True)
    e_mat = tau * d_logit
    d_gram = (e_mat / norm).astype(BF16).astype(F32)
    es = e_mat * gram_n
    q_coef = -jnp.sum(es, axis=1, keepdims=True) / q2
    k_coef = -jnp.sum(es, axis=0, keepdims=True) / k2
    k_coef = jnp.sum(jnp.where(eye, k_coef, 0.0), axis=1, keepdims=True)
    v = jnp.where(valid, att.astype(BF16).astype(F32), pltpu.roll(d_gram, head, 1))
    v = jnp.where(lane == 2 * head, q_coef, v)
    v = jnp.where(lane == 2 * head + 1, k_coef, v)
    return jnp.where(lane == 2 * head + 2, d_tau, v)


def front_kernel(tp, sp, steps, x_ref, g_ref, w_ref, w4_ref, gam_ref, bet_ref, temp_ref,
                 save_ref, u_ref, st_ref, wt_ref, wn_ref, wo_ref, wot_ref, m1_ref, m2_ref, cq_ref, ck_ref, dt_ref,
                 wq, gam, bet, xt, gt, ut, save_s, u_s, qd, kv, acc, sq, wall, sums, pair, parts, state, big,
                 out_sem, send_w, recv_w, send_p, recv_p, send_a, recv_a, send_b, recv_b):
    step = pl.program_id(0)
    my_sp, my_tp = lax.axis_index("sp"), lax.axis_index("tp")
    chips = sp // 2
    core, chip = lax.rem(my_sp, 2), my_sp // 2
    rows, d = x_ref.shape
    own = w4_ref.shape[0]
    head = own // 2
    rest = d - own
    other = {"sp": chip * 2 + 1 - core}
    chip_peers = [{"sp": lax.rem(chip + k, chips) * 2 + core} for k in range(1, chips)]
    tp_peers = [[{"tp": lax.rem(my_tp + k, tp), "sp": chip * 2 + t} for t in range(2)] for k in range(1, tp)]
    barrier = pltpu.get_barrier_semaphore()
    peers = [other] + chip_peers + [p for ps in tp_peers for p in ps]

    @pl.when(step == 0)
    def _():
        for peer in peers:
            pl.semaphore_signal(barrier, inc=1, device_id=peer, device_id_type=MESH)
        for e in range(3):
            wq[e * own : (e + 1) * own, :] = w_ref[e]
        spread_columns(gam_ref, gam)
        spread_columns(bet_ref, bet)
        acc[...] = jnp.zeros_like(acc)
        sq[...] = jnp.zeros_like(sq)
        big[...] = jnp.zeros_like(big)

    def weight_copies():
        out = []
        for k in range(1, tp):
            for i, (src, dst) in enumerate(((w_ref, wall.at[tp - k, 0:3]), (w4_ref, wall.at[tp - k, 3]))):
                peer = {"tp": lax.rem(my_tp + k, tp), "sp": my_sp}
                out.append(remote(src, dst, send_w.at[k, i], recv_w.at[k, i], peer))
        return out

    @pl.when(step == 1)
    def _():
        pl.semaphore_wait(barrier, len(peers))
        for c in weight_copies():
            c.start()

    slot = lax.rem(step, 2)

    def save_copies(to, at_slot):
        cols = pl.ds(pl.multiple_of(to * rows, LANES), rows)
        return [
            pltpu.make_async_copy(save_s.at[at_slot], save_ref.at[:, cols], out_sem.at[at_slot, 0]),
            pltpu.make_async_copy(u_s.at[at_slot], u_ref.at[:, cols], out_sem.at[at_slot, 1]),
        ]

    @pl.when(step >= 2)
    def _():
        for c in save_copies(step - 2, slot):
            c.wait()

    tiles = rows // NT
    at = lambda n: pl.ds(n * NT, NT)

    def norm(n):
        xt[:, at(n)] = x_ref[at(n), :].T
        gt[:, at(n)] = g_ref[at(n), :].T
        mean, inv = ln_stats(xt, at(n))
        mean = mean * inv
        st_ref[0:1, at(n)] = mean
        st_ref[1:2, at(n)] = inv
        for c in range(0, d, CH):
            v = xt[c : c + CH, at(n)].astype(F32) * inv - mean
            v = (v * gam[c : c + CH, :] + bet[c : c + CH, :]).astype(BF16)
            ut[c : c + CH, at(n)] = v
            u_s[slot, c : c + CH, at(n)] = v

    def project(n):
        qkv = dot(wq[...], ut[:, at(n)])
        for e, (ref, r) in enumerate(((qd, 0), (kv, 0), (kv, own))):
            v = qkv[e * own : (e + 1) * own].astype(BF16)
            ref[r : r + own, at(n)] = v
            save_s[slot, e * own : (e + 1) * own, at(n)] = v
            if e == 0:
                v = v.astype(F32)
                v = v * v
                sq[...] += v[:, :LANES] + v[:, LANES:]
        v = dot(w4_ref[...], gt[:, at(n)]).astype(BF16)
        qd[own:, at(n)] = v
        save_s[slot, 3 * own :, at(n)] = v

    def gram(n):
        cols = pl.ds(n * NT, 2 * NT)
        left = jnp.concatenate([qd[:, cols], kv[0:own, cols]], axis=0)
        acc[:, 0 : 2 * own] += dot_nt(left, kv[:, cols])

    norm(0)
    for n in range(tiles):
        if n + 1 < tiles:
            norm(n + 1)
        if n >= 2 and n % 2 == 0:
            gram(n - 2)
        project(n)
    gram(tiles - 2)
    for c in save_copies(step, slot):
        c.start()

    @pl.when(step == steps - 1)
    def _():
        lane = lax.broadcasted_iota(jnp.int32, (head, LANES), 1)
        row = lax.broadcasted_iota(jnp.int32, (head, LANES), 0)
        valid = lane < head

        def block(r, c, to):
            shift = (to - c) % 256
            v = acc[r : r + head, :]
            return (pltpu.roll(v, shift, 1) if shift else v)[:, :LANES]

        for h in range(2):
            r = h * head
            q2 = jnp.sum(sq[r : r + head, :], axis=1, keepdims=True)
            k2 = jnp.sum(jnp.where(lane == row, block(2 * own + r, r, 0), 0.0), axis=1, keepdims=True)
            v = jnp.where(valid, block(r, r, 0), block(own + r, own + r, head))
            v = jnp.where(lane == 2 * head, q2, v)
            sums[r : r + head, :] = jnp.where(lane == 2 * head + 1, k2, v)

        mine = pl.ds(pl.multiple_of(core * head, 8), head)
        theirs = pl.ds(pl.multiple_of((1 - core) * head, 8), head)
        first = remote(sums.at[theirs], pair, send_p.at[0], recv_p.at[0], other)
        first.start()
        for c in weight_copies():
            c.wait()
        first.wait()
        parts[chip] = sums[mine, :] + pair[...]
        copies = [
            remote(parts.at[chip], parts.at[chip], send_a.at[k], recv_a.at[k], chip_peers[k - 1]) for k in range(1, chips)
        ]
        for c in copies:
            c.start()
        pieces = [(w_ref, w4_ref)] + [(wall.at[j, 0:3], wall.at[j, 3]) for j in range(1, tp)]
        for j, (piece, piece4) in enumerate(pieces):
            for e in range(3):
                wn_ref[:, e * d + j * own : e * d + (j + 1) * own] = piece[e].T
                if j:
                    wt_ref[e * rest + (j - 1) * own : e * rest + j * own, :] = piece[e]
            wot_ref[:, j * own : (j + 1) * own] = piece4[...].T
            if j:
                wo_ref[(j - 1) * own : j * own, :] = piece4[...]
        for c in copies:
            c.wait()
        total = parts[0]
        for k in range(1, chips):
            total = total + parts[k]
        state[0, core] = head_state(total, temp_ref[my_tp * 2 + core], head)

        copies = [remote(state.at[0, core], state.at[0, core], send_b.at[0, 0], recv_b.at[0, core], other)]
        for k in range(1, tp):
            for t in range(2):
                copies.append(
                    remote(state.at[0, core], state.at[tp - k, core], send_b.at[k, t], recv_b.at[k, core], tp_peers[k - 1][t])
                )
        for c in copies:
            c.start()
        for c in copies:
            c.wait_send()
        remote(state.at[0, core], state.at[0, 1 - core], send_b.at[0, 0], recv_b.at[0, 1 - core], other).wait_recv()
        for k in range(1, tp):
            for t in range(2):
                remote(state.at[0, core], state.at[tp - k, t], send_b.at[k, t], recv_b.at[k, t], tp_peers[k - 1][t]).wait_recv()

        lane1 = lax.broadcasted_iota(jnp.int32, dt_ref.shape, 1)
        dt = jnp.zeros(dt_ref.shape, F32)
        zero = jnp.zeros((head, d - LANES), F32)
        for j in range(tp):
            for h in range(2):
                t = state[j, h]
                pick = lambda i: jnp.sum(jnp.where(lane == i, t, 0.0), axis=1, keepdims=True)
                r = j * own + h * head
                att = jnp.concatenate([jnp.where(valid, t, 0.0), zero], axis=1)
                d_gram = jnp.concatenate([jnp.where(valid, pltpu.roll(t, LANES - head, 1), 0.0), zero], axis=1)
                big[0, r : r + head, :] = pltpu.roll(att, r, 1) if r else att
                big[1, r : r + head, :] = pltpu.roll(d_gram, r, 1) if r else d_gram
                cq_ref[r : r + head, :] = jnp.broadcast_to(pick(2 * head), (head, NT))
                ck_ref[r : r + head, :] = jnp.broadcast_to(pick(2 * head + 1), (head, NT))
                which = lax.rem(my_tp + j, tp) * 2 + h
                dt = jnp.where(lane1 == which, pick(2 * head + 2)[0:1, :], dt)
        dt_ref[...] = dt
        low = m1_ref.shape[1]
        for i in range(2):
            m = big[i].astype(BF16)
            mt = m.T
            m1_ref[2 * i] = m[0:low, 0:256]
            m2_ref[2 * i] = m[low:, 128:]
            m1_ref[2 * i + 1] = mt[0:low, 0:256]
            m2_ref[2 * i + 1] = mt[low:, 128:]
        for c in save_copies(step - 1, 1 - slot) + save_copies(step, slot):
            c.wait()


def front_call(x, g, w, w4, gam, bet, temps, tp, sp, block=2048):
    rows, d = x.shape
    own = w4.shape[0]
    head = d // temps.shape[0]
    low = 256 // head * head
    steps = rows // block
    row = pl.BlockSpec((block, d), lambda i: (i, 0))
    full = lambda shape: pl.BlockSpec(shape, lambda i: (0,) * len(shape))
    smalls = [
        ((3 * (d - own), d), BF16),
        ((d, 3 * d), BF16),
        ((d - own, d), BF16),
        ((d, d), BF16),
        ((4, low, 256), BF16),
        ((4, d - low, 256), BF16),
        ((d, NT), F32),
        ((d, NT), F32),
        ((1, LANES), F32),
    ]
    dma = pltpu.SemaphoreType.DMA
    return pl.pallas_call(
        functools.partial(front_kernel, tp, sp, steps),
        grid=(steps,),
        in_specs=[row, row, full(w.shape), full(w4.shape), full(gam.shape), full(bet.shape), pl.BlockSpec(memory_space=pltpu.SMEM)],
        out_specs=[pl.BlockSpec(memory_space=pl.ANY)] * 2
        + [pl.BlockSpec((8, block), lambda i: (0, i))]
        + [full(s) for s, _ in smalls],
        out_shape=[jax.ShapeDtypeStruct((r, rows), t) for r, t in ((4 * own, BF16), (d, BF16), (8, F32))] + [jax.ShapeDtypeStruct(s, t) for s, t in smalls],
        scratch_shapes=[
            pltpu.VMEM((3 * own, d), BF16),
            pltpu.VMEM((d, NT), F32),
            pltpu.VMEM((d, NT), F32),
            pltpu.VMEM((d, block), BF16),
            pltpu.VMEM((d, block), BF16),
            pltpu.VMEM((d, block), BF16),
            pltpu.VMEM((2, 4 * own, block), BF16),
            pltpu.VMEM((2, d, block), BF16),
            pltpu.VMEM((2 * own, block), BF16),
            pltpu.VMEM((2 * own, block), BF16),
            pltpu.VMEM((3 * own, 256), F32),
            pltpu.VMEM((own, LANES), F32),
            pltpu.VMEM((tp, 4, own, d), BF16),
            pltpu.VMEM((own, LANES), F32),
            pltpu.VMEM((head, LANES), F32),
            pltpu.VMEM((sp // 2, head, LANES), F32),
            pltpu.VMEM((tp, 2, head, LANES), F32),
            pltpu.VMEM((2, d, d), F32),
            dma((2, 2)),
            dma((tp, 2)),
            dma((tp, 2)),
            dma((1,)),
            dma((1,)),
            dma((sp // 2,)),
            dma((sp // 2,)),
            dma((tp, 2)),
            dma((tp, 2)),
        ],
        compiler_params=pltpu.CompilerParams(
            dimension_semantics=("arbitrary",), vmem_limit_bytes=60 * 2**20, collective_id=0, has_side_effects=True
        ),
        cost_estimate=pl.CostEstimate(flops=2 * rows * d * 4 * own, bytes_accessed=4 * rows * d, transcendentals=0),
        name="front",
    )(x, g, w, w4, gam, bet, temps)


def main_kernel(steps, x_ref, g_ref, save_ref, u_ref, st_ref, wt, wn, wo, wot, m1, m2, gam_ref, cq, ck, y_ref, dx_ref, dw_ref,
                gam, xt, gt, qkv, do, ot, rt, gx, acc_w, acc_o, acc_g):
    step = pl.program_id(0)
    rows, d = x_ref.shape
    rest = wo.shape[0]
    own = d - rest
    low = m1.shape[1]

    @pl.when(step == 0)
    def _():
        spread_columns(gam_ref, gam)
        acc_w[...] = jnp.zeros_like(acc_w)
        acc_o[...] = jnp.zeros_like(acc_o)
        acc_g[...] = jnp.zeros_like(acc_g)

    tiles = rows // NT
    at = lambda n: pl.ds(n * NT, NT)

    def project(n):
        for e in range(3):
            qkv[e * d : e * d + own, at(n)] = save_ref[e * own : (e + 1) * own, at(n)]
            qkv[e * d + own : (e + 1) * d, at(n)] = dot(wt[e * rest : (e + 1) * rest, :], u_ref[:, at(n)]).astype(BF16)
        do[0:own, at(n)] = save_ref[3 * own :, at(n)]
        do[own:, at(n)] = dot_nt(wo[...], g_ref[at(n), :]).astype(BF16)

    def mix(n):
        ot[0:low, at(n)] = dot(m1[0], qkv[2 * d : 2 * d + 256, at(n)]).astype(BF16)
        ot[low:d, at(n)] = dot(m2[0], qkv[2 * d + 128 : 3 * d, at(n)]).astype(BF16)
        rt[2 * d : 2 * d + low, at(n)] = dot(m1[1], do[0:256, at(n)]).astype(BF16)
        rt[2 * d + low : 3 * d, at(n)] = dot(m2[1], do[128:d, at(n)]).astype(BF16)
        for part, other, coef, i in ((0, d, cq, 2), (d, 0, ck, 3)):
            v = dot(m1[i], qkv[other : other + 256, at(n)])
            rt[part : part + low, at(n)] = (v + qkv[part : part + low, at(n)].astype(F32) * coef[0:low, :]).astype(BF16)
            v = dot(m2[i], qkv[other + 128 : other + d, at(n)])
            rt[part + low : part + d, at(n)] = (v + qkv[part + low : part + d, at(n)].astype(F32) * coef[low:d, :]).astype(BF16)

    def out(n):
        xt[:, at(n)] = x_ref[at(n), :].T
        for c, m in ((0, 128), (128, 256)):
            yt = dot(wot[c : c + m, :], ot[:, at(n)]) + xt[c : c + m, at(n)].astype(F32)
            y_ref[at(n), c : c + m] = yt.astype(BF16).T
        gx[:, at(n)] = dot(wn[...], rt[:, at(n)])

    def norm_bwd(first):
        pair = (first, first + 1)
        mean = {n: st_ref[0:1, at(n)] for n in pair}
        inv = {n: st_ref[1:2, at(n)] for n in pair}
        s1 = {n: jnp.zeros((8, NT), F32) for n in pair}
        s2 = {n: jnp.zeros((8, NT), F32) for n in pair}
        for c in range(0, d, CH):
            gm = gam[c : c + CH, :]
            sum_h, sum_u = [], []
            for n in pair:
                du = gx[c : c + CH, at(n)]
                duh = du * (xt[c : c + CH, at(n)].astype(F32) * inv[n] - mean[n])
                s1[n] = s1[n] + fold8(du * gm)
                s2[n] = s2[n] + fold8(duh * gm)
                sum_h.append(duh)
                sum_u.append(du)
            v = sum_h[0] + sum_h[1]
            acc_g[0, c : c + CH, :] += v[:, :LANES] + v[:, LANES:]
            v = sum_u[0] + sum_u[1]
            acc_g[1, c : c + CH, :] += v[:, :LANES] + v[:, LANES:]
        for n in pair:
            m1_ = jnp.sum(s1[n], axis=0, keepdims=True) * (1.0 / d)
            m2_ = jnp.sum(s2[n], axis=0, keepdims=True) * (1.0 / d)
            slope = m2_ * inv[n] * inv[n]
            base = inv[n] * (mean[n] * m2_ - m1_)
            gt[:, at(n)] = g_ref[at(n), :].T
            for c in range(0, d, CH):
                v = gx[c : c + CH, at(n)] * gam[c : c + CH, :] * inv[n] + base - xt[c : c + CH, at(n)].astype(F32) * slope
                gt[c : c + CH, at(n)] = (v + gt[c : c + CH, at(n)].astype(F32)).astype(BF16)
            dx_ref[at(n), :] = gt[:, at(n)].T

    stages = (project, mix, out)
    for n in range(tiles + len(stages) + 1):
        if n >= 4 and n % 2 == 0:
            norm_bwd(n - 4)
        for k in reversed(range(len(stages))):
            if 0 <= n - k < tiles:
                stages[k](n - k)
    r_own = jnp.concatenate([rt[e * d : e * d + own, :] for e in range(3)], axis=0)
    acc_w[...] += dot_nt(r_own, u_ref[...])
    acc_o[...] += dot(ot[0:own, :], g_ref[...])

    @pl.when(step == steps - 1)
    def _():
        sp, slot_rows = dw_ref.shape[0], dw_ref.shape[1]
        per = d // sp
        sub = own // sp
        wgrad = acc_w[...].T
        for s in range(sp):
            dw_ref[s, 0:per, 0 : 3 * own] = wgrad[s * per : (s + 1) * per, :]
            for q in range(d // own):
                dw_ref[s, q * sub : (q + 1) * sub, 3 * own :] = acc_o[s * sub : (s + 1) * sub, q * own : (q + 1) * own]
        zero = jnp.zeros((slot_rows - per - 2, d), F32)
        gb = jnp.concatenate([jnp.sum(acc_g[i].T, axis=0, keepdims=True) for i in range(2)] + [zero], axis=0)
        for s in range(sp):
            dw_ref[s, per:slot_rows, :] = gb


def main_call(x, g, save, u, st, wt, wn, wo, wot, m1, m2, gam, cq, ck, sp, block=2048):
    rows, d = x.shape
    own = d - wo.shape[0]
    steps = rows // block
    row = pl.BlockSpec((block, d), lambda i: (i, 0))
    col = lambda a: pl.BlockSpec((a.shape[0], block), lambda i: (0, i))
    full = lambda a: pl.BlockSpec(a.shape, lambda i: (0,) * a.ndim)
    slot = (sp, d // sp + 8, d)
    smalls = (wt, wn, wo, wot, m1, m2, gam, cq, ck)
    return pl.pallas_call(
        functools.partial(main_kernel, steps),
        grid=(steps,),
        in_specs=[row, row, col(save), col(u), col(st)] + [full(a) for a in smalls],
        out_specs=[row, row, pl.BlockSpec(slot, lambda i: (0, 0, 0))],
        out_shape=[jax.ShapeDtypeStruct((rows, d), BF16), jax.ShapeDtypeStruct((rows, d), BF16), jax.ShapeDtypeStruct(slot, F32)],
        scratch_shapes=[
            pltpu.VMEM((d, NT), F32),
            pltpu.VMEM((d, block), BF16),
            pltpu.VMEM((d, block), BF16),
            pltpu.VMEM((3 * d, block), BF16),
            pltpu.VMEM((d, block), BF16),
            pltpu.VMEM((d, block), BF16),
            pltpu.VMEM((3 * d, block), BF16),
            pltpu.VMEM((d, block), F32),
            pltpu.VMEM((3 * own, d), F32),
            pltpu.VMEM((own, d), F32),
            pltpu.VMEM((2, d, LANES), F32),
        ],
        compiler_params=pltpu.CompilerParams(dimension_semantics=("arbitrary",), vmem_limit_bytes=60 * 2**20),
        cost_estimate=pl.CostEstimate(flops=2 * rows * d * d * 9, bytes_accessed=8 * rows * d, transcendentals=0),
        name="main",
    )(x, g, save, u, st, *smalls)


def wgrad_kernel(sp, in_ref, out_ref, mine, pair, got, sem, send_a, recv_a, send_b, recv_b):
    my = lax.axis_index("sp")
    chips = sp // 2
    core, chip = lax.rem(my, 2), my // 2
    other = {"sp": chip * 2 + 1 - core}
    peers = [{"sp": lax.rem(chip + k, chips) * 2 + core} for k in range(1, chips)]
    barrier = pltpu.get_barrier_semaphore()
    for peer in [other] + peers:
        pl.semaphore_signal(barrier, inc=1, device_id=peer, device_id_type=MESH)
    load = pltpu.make_async_copy(in_ref, mine, sem)
    load.start()
    load.wait()
    pl.semaphore_wait(barrier, chips)
    first = [remote(mine.at[2 * c + 1 - core], pair.at[c], send_a.at[c], recv_a.at[c], other) for c in range(chips)]
    for c in first:
        c.start()
    for c in range(chips):
        first[c].wait()
    for c in range(chips):
        got[chips + c] = mine[2 * c + core] + pair[c]
    second = [
        remote(got.at[chips + lax.rem(chip + k, chips)], got.at[chip], send_b.at[k], recv_b.at[k], peers[k - 1])
        for k in range(1, chips)
    ]
    for c in second:
        c.start()
    got[chip] = got[chips + chip]
    for c in second:
        c.wait()
    total = got[0]
    for c in range(1, chips):
        total = total + got[c]
    out_ref[...] = total


def wgrad_call(parts):
    sp, slot = parts.shape[0], parts.shape[1:]
    dma = pltpu.SemaphoreType.DMA
    return pl.pallas_call(
        functools.partial(wgrad_kernel, sp),
        in_specs=[pl.BlockSpec(memory_space=pl.ANY)],
        out_specs=pl.BlockSpec(memory_space=pltpu.VMEM),
        out_shape=jax.ShapeDtypeStruct(slot, F32),
        scratch_shapes=[
            pltpu.VMEM((sp, *slot), F32),
            pltpu.VMEM((sp // 2, *slot), F32),
            pltpu.VMEM((sp, *slot), F32),
            dma,
            dma((sp // 2,)),
            dma((sp // 2,)),
            dma((sp // 2,)),
            dma((sp // 2,)),
        ],
        compiler_params=pltpu.CompilerParams(collective_id=1, has_side_effects=True),
        name="wgrad",
    )(parts)


def finish_kernel(sum_ref, dt_ref, w_ref, o_ref, gam_ref, bet_ref, tau_ref):
    per, own = w_ref.shape[1:]
    sub = o_ref.shape[0]
    for e in range(3):
        w_ref[e] = sum_ref[0:per, e * own : (e + 1) * own]
    for q in range(o_ref.shape[1] // own):
        o_ref[:, q * own : (q + 1) * own] = sum_ref[q * sub : (q + 1) * sub, 3 * own :]
    gam_ref[...] = sum_ref[per]
    bet_ref[...] = sum_ref[per + 1]
    tau_ref[...] = dt_ref[0, 0 : tau_ref.shape[0]]


def finish_call(total, dt, own, sp, heads):
    d = total.shape[1]
    vmem = pl.BlockSpec(memory_space=pltpu.VMEM)
    shapes = [(3, d // sp, own), (own // sp, d), (d,), (d,), (heads,)]
    return pl.pallas_call(
        finish_kernel,
        in_specs=[vmem, vmem],
        out_specs=[vmem] * 5,
        out_shape=[jax.ShapeDtypeStruct(s, F32) for s in shapes],
        name="finish",
    )(total, dt)


def solution(mesh):
    tp, sp = mesh.shape["tp"], mesh.shape["sp"]
    row_spec = P(("dp", "sp"), None)

    def local_step(x, g, w_qkv, w_out, gamma, beta, temps):
        save, u, st, wt, wn, wo, wot, m1, m2, cq, ck, dt = front_call(
            x, g, w_qkv.transpose(1, 2, 0), w_out, gamma, beta, temps, tp, sp
        )
        y, dx, parts = main_call(x, g, save, u, st, wt, wn, wo, wot, m1, m2, gamma, cq, ck, sp)
        grad_w, grad_o, grad_gamma, grad_beta, grad_temp = finish_call(
            wgrad_call(parts), dt, w_out.shape[0], sp, temps.shape[0]
        )
        return y, dx, grad_w.transpose(1, 0, 2), grad_o, grad_gamma, grad_beta, grad_temp

    in_specs = (row_spec, row_spec, P(None, None, "tp"), P("tp", None), P(None), P(None), P(None))
    out_specs = (row_spec, row_spec, P(("dp", "sp"), None, "tp"), P(("dp", "tp", "sp"), None), P("dp"), P("dp"), P("dp"))
    return jax.shard_map(local_step, mesh=mesh, in_specs=in_specs, out_specs=out_specs, check_vma=False)
```

```python
import functools

import jax
import jax.numpy as jnp
from jax import lax
from jax.experimental import pallas as pl
from jax.experimental.pallas import tpu as pltpu
from jax.sharding import PartitionSpec as P

F32, BF16 = jnp.float32, jnp.bfloat16
LN_EPS = 1e-6
NT = 256
CH = 64
LANES = 128
MESH = pl.DeviceIdType.MESH


def dot(a, b):
    return jnp.dot(a, b, preferred_element_type=F32)


def dot_nt(a, b):
    return lax.dot_general(a, b, (((1,), (1,)), ((), ())), preferred_element_type=F32)


def fold8(v):
    return jnp.sum(v.reshape(v.shape[0] // 8, 8, v.shape[1]), axis=0)


def ln_stats(xt, cols):
    d = xt.shape[0]
    shift = xt[0:16, cols].astype(F32)[0:1, :]
    s1 = jnp.zeros((8, NT), F32)
    s2 = jnp.zeros((8, NT), F32)
    for c in range(0, d, CH):
        v = xt[c : c + CH, cols].astype(F32) - shift
        s1 = s1 + fold8(v)
        s2 = s2 + fold8(v * v)
    off = jnp.sum(s1, axis=0, keepdims=True) * (1.0 / d)
    var = jnp.sum(s2, axis=0, keepdims=True) * (1.0 / d) - off * off
    return shift + off, lax.rsqrt(jnp.maximum(var, 0.0) + LN_EPS)


def spread_columns(row_ref, out):
    d = row_ref.shape[0]
    out[...] = jnp.broadcast_to(row_ref[...].reshape(1, d), (NT, d)).T


def remote(src, dst, send_sem, recv_sem, device):
    return pltpu.make_async_remote_copy(
        src_ref=src, dst_ref=dst, send_sem=send_sem, recv_sem=recv_sem, device_id=device, device_id_type=MESH
    )


def head_state(t, tau, head):
    lane = lax.broadcasted_iota(jnp.int32, (head, LANES), 1)
    row = lax.broadcasted_iota(jnp.int32, (head, LANES), 0)
    valid = lane < head
    eye = lane == row
    pick = lambda i: jnp.sum(jnp.where(lane == i, t, 0.0), axis=1, keepdims=True)
    q2 = pick(2 * head)
    k2 = jnp.sum(jnp.where(eye, pick(2 * head + 1), 0.0), axis=0, keepdims=True)
    k2 = jnp.where(valid, k2, 1.0)
    norm = jnp.sqrt(q2) * jnp.sqrt(k2)
    gram_n = jnp.where(valid, t / norm, 0.0)
    datt = jnp.where(valid, pltpu.roll(t, LANES - head, 1), 0.0)
    logit = jnp.where(valid, tau * gram_n, -1e30)
    ex = jnp.exp(logit - jnp.max(logit, axis=1, keepdims=True))
    ex = jnp.where(valid, ex, 0.0)
    att = ex / jnp.sum(ex, axis=1, keepdims=True)
    d_logit = att * (datt - jnp.sum(att * datt, axis=1, keepdims=True))
    d_tau = jnp.sum(jnp.sum(d_logit * gram_n, axis=1, keepdims=True), axis=0, keepdims=True)
    e_mat = tau * d_logit
    d_gram = (e_mat / norm).astype(BF16).astype(F32)
    es = e_mat * gram_n
    q_coef = -jnp.sum(es, axis=1, keepdims=True) / q2
    k_coef = -jnp.sum(es, axis=0, keepdims=True) / k2
    k_coef = jnp.sum(jnp.where(eye, k_coef, 0.0), axis=1, keepdims=True)
    v = jnp.where(valid, att.astype(BF16).astype(F32), pltpu.roll(d_gram, head, 1))
    v = jnp.where(lane == 2 * head, q_coef, v)
    v = jnp.where(lane == 2 * head + 1, k_coef, v)
    return jnp.where(lane == 2 * head + 2, d_tau, v)


def front_kernel(tp, sp, steps, x_ref, g_ref, w_ref, w4_ref, gam_ref, bet_ref, temp_ref,
                 save_ref, u_ref, st_ref, wt_ref, wn_ref, wo_ref, wot_ref, m1_ref, m2_ref, cq_ref, ck_ref, dt_ref,
                 wq, gam, bet, xt, gt, ut, save_s, u_s, qd, kv, acc, sq, wall, sums, pair, parts, state, big,
                 out_sem, send_w, recv_w, send_p, recv_p, send_a, recv_a, send_b, recv_b):
    step = pl.program_id(0)
    my_sp, my_tp = lax.axis_index("sp"), lax.axis_index("tp")
    chips = sp // 2
    core, chip = lax.rem(my_sp, 2), my_sp // 2
    rows, d = x_ref.shape
    own = w4_ref.shape[0]
    head = own // 2
    rest = d - own
    other = {"sp": chip * 2 + 1 - core}
    chip_peers = [{"sp": lax.rem(chip + k, chips) * 2 + core} for k in range(1, chips)]
    tp_peers = [[{"tp": lax.rem(my_tp + k, tp), "sp": chip * 2 + t} for t in range(2)] for k in range(1, tp)]
    barrier = pltpu.get_barrier_semaphore()
    peers = [other] + chip_peers + [p for ps in tp_peers for p in ps]

    @pl.when(step == 0)
    def _():
        for peer in peers:
            pl.semaphore_signal(barrier, inc=1, device_id=peer, device_id_type=MESH)
        for e in range(3):
            wq[e * own : (e + 1) * own, :] = w_ref[e]
        spread_columns(gam_ref, gam)
        spread_columns(bet_ref, bet)
        acc[...] = jnp.zeros_like(acc)
        sq[...] = jnp.zeros_like(sq)
        big[...] = jnp.zeros_like(big)

    def weight_copies():
        out = []
        for k in range(1, tp):
            for i, (src, dst) in enumerate(((w_ref, wall.at[tp - k, 0:3]), (w4_ref, wall.at[tp - k, 3]))):
                peer = {"tp": lax.rem(my_tp + k, tp), "sp": my_sp}
                out.append(remote(src, dst, send_w.at[k, i], recv_w.at[k, i], peer))
        return out

    @pl.when(step == 1)
    def _():
        pl.semaphore_wait(barrier, len(peers))
        for c in weight_copies():
            c.start()

    slot = lax.rem(step, 2)

    def save_copies(to, at_slot):
        cols = pl.ds(pl.multiple_of(to * rows, LANES), rows)
        return [
            pltpu.make_async_copy(save_s.at[at_slot], save_ref.at[:, cols], out_sem.at[at_slot, 0]),
            pltpu.make_async_copy(u_s.at[at_slot], u_ref.at[:, cols], out_sem.at[at_slot, 1]),
        ]

    @pl.when(step >= 2)
    def _():
        for c in save_copies(step - 2, slot):
            c.wait()

    tiles = rows // NT
    at = lambda n: pl.ds(n * NT, NT)

    def norm(n):
        xt[:, at(n)] = x_ref[at(n), :].T
        gt[:, at(n)] = g_ref[at(n), :].T
        mean, inv = ln_stats(xt, at(n))
        mean = mean * inv
        st_ref[0:1, at(n)] = mean
        st_ref[1:2, at(n)] = inv
        for c in range(0, d, CH):
            v = xt[c : c + CH, at(n)].astype(F32) * inv - mean
            v = (v * gam[c : c + CH, :] + bet[c : c + CH, :]).astype(BF16)
            ut[c : c + CH, at(n)] = v
            u_s[slot, c : c + CH, at(n)] = v

    def project(n):
        qkv = dot(wq[...], ut[:, at(n)])
        for e, (ref, r) in enumerate(((qd, 0), (kv, 0), (kv, own))):
            v = qkv[e * own : (e + 1) * own].astype(BF16)
            ref[r : r + own, at(n)] = v
            save_s[slot, e * own : (e + 1) * own, at(n)] = v
            if e == 0:
                v = v.astype(F32)
                v = v * v
                sq[...] += v[:, :LANES] + v[:, LANES:]
        v = dot(w4_ref[...], gt[:, at(n)]).astype(BF16)
        qd[own:, at(n)] = v
        save_s[slot, 3 * own :, at(n)] = v

    def gram(n):
        cols = pl.ds(n * NT, 2 * NT)
        left = jnp.concatenate([qd[:, cols], kv[0:own, cols]], axis=0)
        acc[:, 0 : 2 * own] += dot_nt(left, kv[:, cols])

    norm(0)
    for n in range(tiles):
        if n + 1 < tiles:
            norm(n + 1)
        if n >= 2 and n % 2 == 0:
            gram(n - 2)
        project(n)
    gram(tiles - 2)
    for c in save_copies(step, slot):
        c.start()

    @pl.when(step == steps - 1)
    def _():
        lane = lax.broadcasted_iota(jnp.int32, (head, LANES), 1)
        row = lax.broadcasted_iota(jnp.int32, (head, LANES), 0)
        valid = lane < head

        def block(r, c, to):
            shift = (to - c) % 256
            v = acc[r : r + head, :]
            return (pltpu.roll(v, shift, 1) if shift else v)[:, :LANES]

        for h in range(2):
            r = h * head
            q2 = jnp.sum(sq[r : r + head, :], axis=1, keepdims=True)
            k2 = jnp.sum(jnp.where(lane == row, block(2 * own + r, r, 0), 0.0), axis=1, keepdims=True)
            v = jnp.where(valid, block(r, r, 0), block(own + r, own + r, head))
            v = jnp.where(lane == 2 * head, q2, v)
            sums[r : r + head, :] = jnp.where(lane == 2 * head + 1, k2, v)

        mine = pl.ds(pl.multiple_of(core * head, 8), head)
        theirs = pl.ds(pl.multiple_of((1 - core) * head, 8), head)
        first = remote(sums.at[theirs], pair, send_p.at[0], recv_p.at[0], other)
        first.start()
        for c in weight_copies():
            c.wait()
        first.wait()
        parts[chip] = sums[mine, :] + pair[...]
        copies = [
            remote(parts.at[chip], parts.at[chip], send_a.at[k], recv_a.at[k], chip_peers[k - 1]) for k in range(1, chips)
        ]
        for c in copies:
            c.start()
        pieces = [(w_ref, w4_ref)] + [(wall.at[j, 0:3], wall.at[j, 3]) for j in range(1, tp)]
        for j, (piece, piece4) in enumerate(pieces):
            for e in range(3):
                wn_ref[:, e * d + j * own : e * d + (j + 1) * own] = piece[e].T
                if j:
                    wt_ref[e * rest + (j - 1) * own : e * rest + j * own, :] = piece[e]
            wot_ref[:, j * own : (j + 1) * own] = piece4[...].T
            if j:
                wo_ref[(j - 1) * own : j * own, :] = piece4[...]
        for c in copies:
            c.wait()
        total = parts[0]
        for k in range(1, chips):
            total = total + parts[k]
        state[0, core] = head_state(total, temp_ref[my_tp * 2 + core], head)

        copies = [remote(state.at[0, core], state.at[0, core], send_b.at[0, 0], recv_b.at[0, core], other)]
        for k in range(1, tp):
            for t in range(2):
                copies.append(
                    remote(state.at[0, core], state.at[tp - k, core], send_b.at[k, t], recv_b.at[k, core], tp_peers[k - 1][t])
                )
        for c in copies:
            c.start()
        for c in copies:
            c.wait_send()
        remote(state.at[0, core], state.at[0, 1 - core], send_b.at[0, 0], recv_b.at[0, 1 - core], other).wait_recv()
        for k in range(1, tp):
            for t in range(2):
                remote(state.at[0, core], state.at[tp - k, t], send_b.at[k, t], recv_b.at[k, t], tp_peers[k - 1][t]).wait_recv()

        lane1 = lax.broadcasted_iota(jnp.int32, dt_ref.shape, 1)
        dt = jnp.zeros(dt_ref.shape, F32)
        zero = jnp.zeros((head, d - LANES), F32)
        for j in range(tp):
            for h in range(2):
                t = state[j, h]
                pick = lambda i: jnp.sum(jnp.where(lane == i, t, 0.0), axis=1, keepdims=True)
                r = j * own + h * head
                att = jnp.concatenate([jnp.where(valid, t, 0.0), zero], axis=1)
                d_gram = jnp.concatenate([jnp.where(valid, pltpu.roll(t, LANES - head, 1), 0.0), zero], axis=1)
                big[0, r : r + head, :] = pltpu.roll(att, r, 1) if r else att
                big[1, r : r + head, :] = pltpu.roll(d_gram, r, 1) if r else d_gram
                cq_ref[r : r + head, :] = jnp.broadcast_to(pick(2 * head), (head, NT))
                ck_ref[r : r + head, :] = jnp.broadcast_to(pick(2 * head + 1), (head, NT))
                which = lax.rem(my_tp + j, tp) * 2 + h
                dt = jnp.where(lane1 == which, pick(2 * head + 2)[0:1, :], dt)
        dt_ref[...] = dt
        low = m1_ref.shape[1]
        for i in range(2):
            m = big[i].astype(BF16)
            mt = m.T
            m1_ref[2 * i] = m[0:low, 0:256]
            m2_ref[2 * i] = m[low:, 128:]
            m1_ref[2 * i + 1] = mt[0:low, 0:256]
            m2_ref[2 * i + 1] = mt[low:, 128:]
        for c in save_copies(step - 1, 1 - slot) + save_copies(step, slot):
            c.wait()


def front_call(x, g, w, w4, gam, bet, temps, tp, sp, block=4096):
    rows, d = x.shape
    own = w4.shape[0]
    head = d // temps.shape[0]
    low = 256 // head * head
    steps = rows // block
    row = pl.BlockSpec((block, d), lambda i: (i, 0))
    full = lambda shape: pl.BlockSpec(shape, lambda i: (0,) * len(shape))
    smalls = [
        ((3 * (d - own), d), BF16),
        ((d, 3 * d), BF16),
        ((d - own, d), BF16),
        ((d, d), BF16),
        ((4, low, 256), BF16),
        ((4, d - low, 256), BF16),
        ((d, NT), F32),
        ((d, NT), F32),
        ((1, LANES), F32),
    ]
    dma = pltpu.SemaphoreType.DMA
    return pl.pallas_call(
        functools.partial(front_kernel, tp, sp, steps),
        grid=(steps,),
        in_specs=[row, row, full(w.shape), full(w4.shape), full(gam.shape), full(bet.shape), pl.BlockSpec(memory_space=pltpu.SMEM)],
        out_specs=[pl.BlockSpec(memory_space=pl.ANY)] * 2
        + [pl.BlockSpec((8, block), lambda i: (0, i))]
        + [full(s) for s, _ in smalls],
        out_shape=[jax.ShapeDtypeStruct((r, rows), t) for r, t in ((4 * own, BF16), (d, BF16), (8, F32))] + [jax.ShapeDtypeStruct(s, t) for s, t in smalls],
        scratch_shapes=[
            pltpu.VMEM((3 * own, d), BF16),
            pltpu.VMEM((d, NT), F32),
            pltpu.VMEM((d, NT), F32),
            pltpu.VMEM((d, block), BF16),
            pltpu.VMEM((d, block), BF16),
            pltpu.VMEM((d, block), BF16),
            pltpu.VMEM((2, 4 * own, block), BF16),
            pltpu.VMEM((2, d, block), BF16),
            pltpu.VMEM((2 * own, block), BF16),
            pltpu.VMEM((2 * own, block), BF16),
            pltpu.VMEM((3 * own, 256), F32),
            pltpu.VMEM((own, LANES), F32),
            pltpu.VMEM((tp, 4, own, d), BF16),
            pltpu.VMEM((own, LANES), F32),
            pltpu.VMEM((head, LANES), F32),
            pltpu.VMEM((sp // 2, head, LANES), F32),
            pltpu.VMEM((tp, 2, head, LANES), F32),
            pltpu.VMEM((2, d, d), F32),
            dma((2, 2)),
            dma((tp, 2)),
            dma((tp, 2)),
            dma((1,)),
            dma((1,)),
            dma((sp // 2,)),
            dma((sp // 2,)),
            dma((tp, 2)),
            dma((tp, 2)),
        ],
        compiler_params=pltpu.CompilerParams(
            dimension_semantics=("arbitrary",), vmem_limit_bytes=60 * 2**20, collective_id=0, has_side_effects=True
        ),
        cost_estimate=pl.CostEstimate(flops=2 * rows * d * 4 * own, bytes_accessed=4 * rows * d, transcendentals=0),
        name="front",
    )(x, g, w, w4, gam, bet, temps)


def main_kernel(steps, x_ref, g_ref, save_ref, u_ref, st_ref, wt, wn, wo, wot, m1, m2, gam_ref, cq, ck, y_ref, dx_ref, dw_ref,
                gam, xt, gt, qkv, do, ot, rt, gx, acc_w, acc_o, acc_g):
    step = pl.program_id(0)
    rows, d = x_ref.shape
    rest = wo.shape[0]
    own = d - rest
    low = m1.shape[1]

    @pl.when(step == 0)
    def _():
        spread_columns(gam_ref, gam)
        acc_w[...] = jnp.zeros_like(acc_w)
        acc_o[...] = jnp.zeros_like(acc_o)
        acc_g[...] = jnp.zeros_like(acc_g)

    tiles = rows // NT
    at = lambda n: pl.ds(n * NT, NT)

    def project(n):
        for e in range(3):
            qkv[e * d : e * d + own, at(n)] = save_ref[e * own : (e + 1) * own, at(n)]
            qkv[e * d + own : (e + 1) * d, at(n)] = dot(wt[e * rest : (e + 1) * rest, :], u_ref[:, at(n)]).astype(BF16)
        do[0:own, at(n)] = save_ref[3 * own :, at(n)]
        do[own:, at(n)] = dot_nt(wo[...], g_ref[at(n), :]).astype(BF16)

    def mix(n):
        ot[0:low, at(n)] = dot(m1[0], qkv[2 * d : 2 * d + 256, at(n)]).astype(BF16)
        ot[low:d, at(n)] = dot(m2[0], qkv[2 * d + 128 : 3 * d, at(n)]).astype(BF16)
        rt[2 * d : 2 * d + low, at(n)] = dot(m1[1], do[0:256, at(n)]).astype(BF16)
        rt[2 * d + low : 3 * d, at(n)] = dot(m2[1], do[128:d, at(n)]).astype(BF16)
        for part, other, coef, i in ((0, d, cq, 2), (d, 0, ck, 3)):
            v = dot(m1[i], qkv[other : other + 256, at(n)])
            rt[part : part + low, at(n)] = (v + qkv[part : part + low, at(n)].astype(F32) * coef[0:low, :]).astype(BF16)
            v = dot(m2[i], qkv[other + 128 : other + d, at(n)])
            rt[part + low : part + d, at(n)] = (v + qkv[part + low : part + d, at(n)].astype(F32) * coef[low:d, :]).astype(BF16)

    def out(n):
        xt[:, at(n)] = x_ref[at(n), :].T
        for c, m in ((0, 128), (128, 256)):
            yt = dot(wot[c : c + m, :], ot[:, at(n)]) + xt[c : c + m, at(n)].astype(F32)
            y_ref[at(n), c : c + m] = yt.astype(BF16).T
        gx[:, at(n)] = dot(wn[...], rt[:, at(n)])

    def norm_bwd(first):
        pair = (first, first + 1)
        mean = {n: st_ref[0:1, at(n)] for n in pair}
        inv = {n: st_ref[1:2, at(n)] for n in pair}
        s1 = {n: jnp.zeros((8, NT), F32) for n in pair}
        s2 = {n: jnp.zeros((8, NT), F32) for n in pair}
        for c in range(0, d, CH):
            gm = gam[c : c + CH, :]
            sum_h, sum_u = [], []
            for n in pair:
                du = gx[c : c + CH, at(n)]
                duh = du * (xt[c : c + CH, at(n)].astype(F32) * inv[n] - mean[n])
                s1[n] = s1[n] + fold8(du * gm)
                s2[n] = s2[n] + fold8(duh * gm)
                sum_h.append(duh)
                sum_u.append(du)
            v = sum_h[0] + sum_h[1]
            acc_g[0, c : c + CH, :] += v[:, :LANES] + v[:, LANES:]
            v = sum_u[0] + sum_u[1]
            acc_g[1, c : c + CH, :] += v[:, :LANES] + v[:, LANES:]
        for n in pair:
            m1_ = jnp.sum(s1[n], axis=0, keepdims=True) * (1.0 / d)
            m2_ = jnp.sum(s2[n], axis=0, keepdims=True) * (1.0 / d)
            slope = m2_ * inv[n] * inv[n]
            base = inv[n] * (mean[n] * m2_ - m1_)
            gt[:, at(n)] = g_ref[at(n), :].T
            for c in range(0, d, CH):
                v = gx[c : c + CH, at(n)] * gam[c : c + CH, :] * inv[n] + base - xt[c : c + CH, at(n)].astype(F32) * slope
                gt[c : c + CH, at(n)] = (v + gt[c : c + CH, at(n)].astype(F32)).astype(BF16)
            dx_ref[at(n), :] = gt[:, at(n)].T

    stages = (project, mix, out)
    for n in range(tiles + len(stages) + 1):
        if n >= 4 and n % 2 == 0:
            norm_bwd(n - 4)
        for k in reversed(range(len(stages))):
            if 0 <= n - k < tiles:
                stages[k](n - k)
    r_own = jnp.concatenate([rt[e * d : e * d + own, :] for e in range(3)], axis=0)
    acc_w[...] += dot_nt(r_own, u_ref[...])
    acc_o[...] += dot(ot[0:own, :], g_ref[...])

    @pl.when(step == steps - 1)
    def _():
        sp, slot_rows = dw_ref.shape[0], dw_ref.shape[1]
        per = d // sp
        sub = own // sp
        wgrad = acc_w[...].T
        for s in range(sp):
            dw_ref[s, 0:per, 0 : 3 * own] = wgrad[s * per : (s + 1) * per, :]
            for q in range(d // own):
                dw_ref[s, q * sub : (q + 1) * sub, 3 * own :] = acc_o[s * sub : (s + 1) * sub, q * own : (q + 1) * own]
        zero = jnp.zeros((slot_rows - per - 2, d), F32)
        gb = jnp.concatenate([jnp.sum(acc_g[i].T, axis=0, keepdims=True) for i in range(2)] + [zero], axis=0)
        for s in range(sp):
            dw_ref[s, per:slot_rows, :] = gb


def main_call(x, g, save, u, st, wt, wn, wo, wot, m1, m2, gam, cq, ck, sp, block=2048):
    rows, d = x.shape
    own = d - wo.shape[0]
    steps = rows // block
    row = pl.BlockSpec((block, d), lambda i: (i, 0))
    col = lambda a: pl.BlockSpec((a.shape[0], block), lambda i: (0, i))
    full = lambda a: pl.BlockSpec(a.shape, lambda i: (0,) * a.ndim)
    slot = (sp, d // sp + 8, d)
    smalls = (wt, wn, wo, wot, m1, m2, gam, cq, ck)
    return pl.pallas_call(
        functools.partial(main_kernel, steps),
        grid=(steps,),
        in_specs=[row, row, col(save), col(u), col(st)] + [full(a) for a in smalls],
        out_specs=[row, row, pl.BlockSpec(slot, lambda i: (0, 0, 0))],
        out_shape=[jax.ShapeDtypeStruct((rows, d), BF16), jax.ShapeDtypeStruct((rows, d), BF16), jax.ShapeDtypeStruct(slot, F32)],
        scratch_shapes=[
            pltpu.VMEM((d, NT), F32),
            pltpu.VMEM((d, block), BF16),
            pltpu.VMEM((d, block), BF16),
            pltpu.VMEM((3 * d, block), BF16),
            pltpu.VMEM((d, block), BF16),
            pltpu.VMEM((d, block), BF16),
            pltpu.VMEM((3 * d, block), BF16),
            pltpu.VMEM((d, block), F32),
            pltpu.VMEM((3 * own, d), F32),
            pltpu.VMEM((own, d), F32),
            pltpu.VMEM((2, d, LANES), F32),
        ],
        compiler_params=pltpu.CompilerParams(dimension_semantics=("arbitrary",), vmem_limit_bytes=60 * 2**20),
        cost_estimate=pl.CostEstimate(flops=2 * rows * d * d * 9, bytes_accessed=8 * rows * d, transcendentals=0),
        name="main",
    )(x, g, save, u, st, *smalls)


def wgrad_kernel(sp, in_ref, out_ref, mine, pair, got, sem, send_a, recv_a, send_b, recv_b):
    my = lax.axis_index("sp")
    chips = sp // 2
    core, chip = lax.rem(my, 2), my // 2
    other = {"sp": chip * 2 + 1 - core}
    peers = [{"sp": lax.rem(chip + k, chips) * 2 + core} for k in range(1, chips)]
    barrier = pltpu.get_barrier_semaphore()
    for peer in [other] + peers:
        pl.semaphore_signal(barrier, inc=1, device_id=peer, device_id_type=MESH)
    load = pltpu.make_async_copy(in_ref, mine, sem)
    load.start()
    load.wait()
    pl.semaphore_wait(barrier, chips)
    first = [remote(mine.at[2 * c + 1 - core], pair.at[c], send_a.at[c], recv_a.at[c], other) for c in range(chips)]
    for c in first:
        c.start()
    for c in range(chips):
        first[c].wait()
    for c in range(chips):
        got[chips + c] = mine[2 * c + core] + pair[c]
    second = [
        remote(got.at[chips + lax.rem(chip + k, chips)], got.at[chip], send_b.at[k], recv_b.at[k], peers[k - 1])
        for k in range(1, chips)
    ]
    for c in second:
        c.start()
    got[chip] = got[chips + chip]
    for c in second:
        c.wait()
    total = got[0]
    for c in range(1, chips):
        total = total + got[c]
    out_ref[...] = total


def wgrad_call(parts):
    sp, slot = parts.shape[0], parts.shape[1:]
    dma = pltpu.SemaphoreType.DMA
    return pl.pallas_call(
        functools.partial(wgrad_kernel, sp),
        in_specs=[pl.BlockSpec(memory_space=pl.ANY)],
        out_specs=pl.BlockSpec(memory_space=pltpu.VMEM),
        out_shape=jax.ShapeDtypeStruct(slot, F32),
        scratch_shapes=[
            pltpu.VMEM((sp, *slot), F32),
            pltpu.VMEM((sp // 2, *slot), F32),
            pltpu.VMEM((sp, *slot), F32),
            dma,
            dma((sp // 2,)),
            dma((sp // 2,)),
            dma((sp // 2,)),
            dma((sp // 2,)),
        ],
        compiler_params=pltpu.CompilerParams(collective_id=1, has_side_effects=True),
        name="wgrad",
    )(parts)


def finish_kernel(sum_ref, dt_ref, w_ref, o_ref, gam_ref, bet_ref, tau_ref):
    per, own = w_ref.shape[1:]
    sub = o_ref.shape[0]
    for e in range(3):
        w_ref[e] = sum_ref[0:per, e * own : (e + 1) * own]
    for q in range(o_ref.shape[1] // own):
        o_ref[:, q * own : (q + 1) * own] = sum_ref[q * sub : (q + 1) * sub, 3 * own :]
    gam_ref[...] = sum_ref[per]
    bet_ref[...] = sum_ref[per + 1]
    tau_ref[...] = dt_ref[0, 0 : tau_ref.shape[0]]


def finish_call(total, dt, own, sp, heads):
    d = total.shape[1]
    vmem = pl.BlockSpec(memory_space=pltpu.VMEM)
    shapes = [(3, d // sp, own), (own // sp, d), (d,), (d,), (heads,)]
    return pl.pallas_call(
        finish_kernel,
        in_specs=[vmem, vmem],
        out_specs=[vmem] * 5,
        out_shape=[jax.ShapeDtypeStruct(s, F32) for s in shapes],
        name="finish",
    )(total, dt)


def solution(mesh):
    tp, sp = mesh.shape["tp"], mesh.shape["sp"]
    row_spec = P(("dp", "sp"), None)

    def local_step(x, g, w_qkv, w_out, gamma, beta, temps):
        save, u, st, wt, wn, wo, wot, m1, m2, cq, ck, dt = front_call(
            x, g, w_qkv.transpose(1, 2, 0), w_out, gamma, beta, temps, tp, sp
        )
        y, dx, parts = main_call(x, g, save, u, st, wt, wn, wo, wot, m1, m2, gamma, cq, ck, sp)
        grad_w, grad_o, grad_gamma, grad_beta, grad_temp = finish_call(
            wgrad_call(parts), dt, w_out.shape[0], sp, temps.shape[0]
        )
        return y, dx, grad_w.transpose(1, 0, 2), grad_o, grad_gamma, grad_beta, grad_temp

    in_specs = (row_spec, row_spec, P(None, None, "tp"), P("tp", None), P(None), P(None), P(None))
    out_specs = (row_spec, row_spec, P(("dp", "sp"), None, "tp"), P(("dp", "tp", "sp"), None), P("dp"), P("dp"), P("dp"))
    return jax.shard_map(local_step, mesh=mesh, in_specs=in_specs, out_specs=out_specs, check_vma=False)
```

```python
import functools

import jax
import jax.numpy as jnp
from jax import lax
from jax.experimental import pallas as pl
from jax.experimental.pallas import tpu as pltpu
from jax.sharding import PartitionSpec as P

F32, BF16 = jnp.float32, jnp.bfloat16
LN_EPS = 1e-6
NT = 256
CH = 64
LANES = 128
MESH = pl.DeviceIdType.MESH


def dot(a, b):
    return jnp.dot(a, b, preferred_element_type=F32)


def dot_nt(a, b):
    return lax.dot_general(a, b, (((1,), (1,)), ((), ())), preferred_element_type=F32)


def fold8(v):
    return jnp.sum(v.reshape(v.shape[0] // 8, 8, v.shape[1]), axis=0)


def ln_stats(xt, cols):
    d = xt.shape[0]
    shift = xt[0:16, cols].astype(F32)[0:1, :]
    s1 = jnp.zeros((8, NT), F32)
    s2 = jnp.zeros((8, NT), F32)
    for c in range(0, d, CH):
        v = xt[c : c + CH, cols].astype(F32) - shift
        s1 = s1 + fold8(v)
        s2 = s2 + fold8(v * v)
    off = jnp.sum(s1, axis=0, keepdims=True) * (1.0 / d)
    var = jnp.sum(s2, axis=0, keepdims=True) * (1.0 / d) - off * off
    return shift + off, lax.rsqrt(jnp.maximum(var, 0.0) + LN_EPS)


def spread_columns(row_ref, out):
    d = row_ref.shape[0]
    out[...] = jnp.broadcast_to(row_ref[...].reshape(1, d), (NT, d)).T


def remote(src, dst, send_sem, recv_sem, device):
    return pltpu.make_async_remote_copy(
        src_ref=src, dst_ref=dst, send_sem=send_sem, recv_sem=recv_sem, device_id=device, device_id_type=MESH
    )


def head_state(t, tau, head):
    lane = lax.broadcasted_iota(jnp.int32, (head, LANES), 1)
    row = lax.broadcasted_iota(jnp.int32, (head, LANES), 0)
    valid = lane < head
    eye = lane == row
    pick = lambda i: t[:, i : i + 1]
    q2 = pick(2 * head)
    k2 = jnp.sum(jnp.where(eye, pick(2 * head + 1), 0.0), axis=0, keepdims=True)
    k2 = jnp.where(valid, k2, 1.0)
    norm = jnp.sqrt(q2) * jnp.sqrt(k2)
    gram_n = jnp.where(valid, t / norm, 0.0)
    datt = jnp.where(valid, pltpu.roll(t, LANES - head, 1), 0.0)
    logit = jnp.where(valid, tau * gram_n, -1e30)
    ex = jnp.exp(logit - jnp.max(logit, axis=1, keepdims=True))
    ex = jnp.where(valid, ex, 0.0)
    att = ex / jnp.sum(ex, axis=1, keepdims=True)
    d_logit = att * (datt - jnp.sum(att * datt, axis=1, keepdims=True))
    d_tau = jnp.sum(jnp.sum(d_logit * gram_n, axis=1, keepdims=True), axis=0, keepdims=True)
    e_mat = tau * d_logit
    d_gram = (e_mat / norm).astype(BF16).astype(F32)
    es = e_mat * gram_n
    q_coef = -jnp.sum(es, axis=1, keepdims=True) / q2
    k_coef = -jnp.sum(es, axis=0, keepdims=True) / k2
    k_coef = jnp.sum(jnp.where(eye, k_coef, 0.0), axis=1, keepdims=True)
    v = jnp.where(valid, att.astype(BF16).astype(F32), pltpu.roll(d_gram, head, 1))
    v = jnp.where(lane == 2 * head, q_coef, v)
    v = jnp.where(lane == 2 * head + 1, k_coef, v)
    return jnp.where(lane == 2 * head + 2, d_tau, v)


def front_kernel(tp, sp, steps, x_ref, g_ref, w_ref, w4_ref, gam_ref, bet_ref, temp_ref,
                 save_ref, u_ref, st_ref, wt_ref, wn_ref, wo_ref, wot_ref, m1_ref, m2_ref, cq_ref, ck_ref, dt_ref,
                 wq, gam, bet, xt, gt, ut, save_s, u_s, qd, kv, acc, sq, wall, sums, pair, parts, state, big,
                 out_sem, send_w, recv_w, send_p, recv_p, send_a, recv_a, send_b, recv_b):
    step = pl.program_id(0)
    my_sp, my_tp = lax.axis_index("sp"), lax.axis_index("tp")
    chips = sp // 2
    core, chip = lax.rem(my_sp, 2), my_sp // 2
    rows, d = x_ref.shape
    own = w4_ref.shape[0]
    head = own // 2
    rest = d - own
    other = {"sp": chip * 2 + 1 - core}
    chip_peers = [{"sp": lax.rem(chip + k, chips) * 2 + core} for k in range(1, chips)]
    tp_peers = [[{"tp": lax.rem(my_tp + k, tp), "sp": chip * 2 + t} for t in range(2)] for k in range(1, tp)]
    barrier = pltpu.get_barrier_semaphore()
    peers = [other] + chip_peers + [p for ps in tp_peers for p in ps]

    @pl.when(step == 0)
    def _():
        for peer in peers:
            pl.semaphore_signal(barrier, inc=1, device_id=peer, device_id_type=MESH)
        for e in range(3):
            wq[e * own : (e + 1) * own, :] = w_ref[e]
        spread_columns(gam_ref, gam)
        spread_columns(bet_ref, bet)
        acc[...] = jnp.zeros_like(acc)
        sq[...] = jnp.zeros_like(sq)
        big[...] = jnp.zeros_like(big)

    def weight_copies():
        out = []
        for k in range(1, tp):
            for i, (src, dst) in enumerate(((w_ref, wall.at[tp - k, 0:3]), (w4_ref, wall.at[tp - k, 3]))):
                peer = {"tp": lax.rem(my_tp + k, tp), "sp": my_sp}
                out.append(remote(src, dst, send_w.at[k, i], recv_w.at[k, i], peer))
        return out

    @pl.when(step == 1)
    def _():
        pl.semaphore_wait(barrier, len(peers))
        for c in weight_copies():
            c.start()

    slot = lax.rem(step, 2)

    def save_copies(to, at_slot):
        cols = pl.ds(pl.multiple_of(to * rows, LANES), rows)
        return [
            pltpu.make_async_copy(save_s.at[at_slot], save_ref.at[:, cols], out_sem.at[at_slot, 0]),
            pltpu.make_async_copy(u_s.at[at_slot], u_ref.at[:, cols], out_sem.at[at_slot, 1]),
        ]

    @pl.when(step >= 2)
    def _():
        for c in save_copies(step - 2, slot):
            c.wait()

    tiles = rows // NT
    at = lambda n: pl.ds(n * NT, NT)

    def norm(n):
        xt[:, at(n)] = x_ref[at(n), :].T
        gt[:, at(n)] = g_ref[at(n), :].T
        mean, inv = ln_stats(xt, at(n))
        mean = mean * inv
        st_ref[0:1, at(n)] = mean
        st_ref[1:2, at(n)] = inv
        for c in range(0, d, CH):
            v = xt[c : c + CH, at(n)].astype(F32) * inv - mean
            v = (v * gam[c : c + CH, :] + bet[c : c + CH, :]).astype(BF16)
            ut[c : c + CH, at(n)] = v
            u_s[slot, c : c + CH, at(n)] = v

    def project(n):
        qkv = dot(wq[...], ut[:, at(n)])
        for e, (ref, r) in enumerate(((qd, 0), (kv, 0), (kv, own))):
            v = qkv[e * own : (e + 1) * own].astype(BF16)
            ref[r : r + own, at(n)] = v
            save_s[slot, e * own : (e + 1) * own, at(n)] = v
            if e < 2:
                v = v.astype(F32)
                v = v * v
                sq[e * own : (e + 1) * own] += v[:, :LANES] + v[:, LANES:]
        v = dot(w4_ref[...], gt[:, at(n)]).astype(BF16)
        qd[own:, at(n)] = v
        save_s[slot, 3 * own :, at(n)] = v

    def gram(n):
        cols = pl.ds(n * NT, 4 * NT)
        acc[:, 0 : 2 * own] += dot_nt(qd[:, cols], kv[:, cols])

    norm(0)
    for n in range(tiles):
        if n + 1 < tiles:
            norm(n + 1)
        if n >= 4 and n % 4 == 0:
            gram(n - 4)
        project(n)
    gram(tiles - 4)
    for c in save_copies(step, slot):
        c.start()

    @pl.when(step == steps - 1)
    def _():
        lane = lax.broadcasted_iota(jnp.int32, (head, LANES), 1)
        row = lax.broadcasted_iota(jnp.int32, (head, LANES), 0)
        valid = lane < head

        def block(r, c, to):
            shift = (to - c) % 256
            v = acc[r : r + head, :]
            return (pltpu.roll(v, shift, 1) if shift else v)[:, :LANES]

        for h in range(2):
            r = h * head
            q2 = jnp.sum(sq[r : r + head, :], axis=1, keepdims=True)
            k2 = jnp.sum(sq[own + r : own + r + head, :], axis=1, keepdims=True)
            v = jnp.where(valid, block(r, r, 0), block(own + r, own + r, head))
            v = jnp.where(lane == 2 * head, q2, v)
            sums[r : r + head, :] = jnp.where(lane == 2 * head + 1, k2, v)

        mine = pl.ds(pl.multiple_of(core * head, 8), head)
        theirs = pl.ds(pl.multiple_of((1 - core) * head, 8), head)
        first = remote(sums.at[theirs], pair, send_p.at[0], recv_p.at[0], other)
        first.start()
        for c in weight_copies():
            c.wait()
        first.wait()
        parts[chip] = sums[mine, :] + pair[...]
        copies = [
            remote(parts.at[chip], parts.at[chip], send_a.at[k], recv_a.at[k], chip_peers[k - 1]) for k in range(1, chips)
        ]
        for c in copies:
            c.start()
        pieces = [(w_ref, w4_ref)] + [(wall.at[j, 0:3], wall.at[j, 3]) for j in range(1, tp)]
        for j, (piece, piece4) in enumerate(pieces):
            for e in range(3):
                wn_ref[:, e * d + j * own : e * d + (j + 1) * own] = piece[e].T
                if j:
                    wt_ref[e * rest + (j - 1) * own : e * rest + j * own, :] = piece[e]
            wot_ref[:, j * own : (j + 1) * own] = piece4[...].T
            if j:
                wo_ref[(j - 1) * own : j * own, :] = piece4[...]
        for c in copies:
            c.wait()
        total = parts[0]
        for k in range(1, chips):
            total = total + parts[k]
        state[0, core] = head_state(total, temp_ref[my_tp * 2 + core], head)

        copies = [remote(state.at[0, core], state.at[0, core], send_b.at[0, 0], recv_b.at[0, core], other)]
        for k in range(1, tp):
            for t in range(2):
                copies.append(
                    remote(state.at[0, core], state.at[tp - k, core], send_b.at[k, t], recv_b.at[k, core], tp_peers[k - 1][t])
                )
        for c in copies:
            c.start()
        lane1 = lax.broadcasted_iota(jnp.int32, dt_ref.shape, 1)
        dt = jnp.zeros(dt_ref.shape, F32)
        zero = jnp.zeros((head, d - LANES), F32)
        for j in (0, tp - 1, 1, *range(2, tp - 1)):
            k = tp - j
            if j == 0:
                remote(state.at[0, core], state.at[0, 1 - core], send_b.at[0, 0], recv_b.at[0, 1 - core], other).wait_recv()
            for h in range(2):
                if j:
                    remote(state.at[0, core], state.at[j, h], send_b.at[k, h], recv_b.at[k, h], tp_peers[k - 1][h]).wait_recv()
                t = state[j, h]
                pick = lambda i: t[:, i : i + 1]
                r = j * own + h * head
                att = jnp.concatenate([jnp.where(valid, t, 0.0), zero], axis=1)
                d_gram = jnp.concatenate([jnp.where(valid, pltpu.roll(t, LANES - head, 1), 0.0), zero], axis=1)
                big[0, r : r + head, :] = pltpu.roll(att, r, 1) if r else att
                big[1, r : r + head, :] = pltpu.roll(d_gram, r, 1) if r else d_gram
                cq_ref[r : r + head, :] = jnp.broadcast_to(pick(2 * head), (head, NT))
                ck_ref[r : r + head, :] = jnp.broadcast_to(pick(2 * head + 1), (head, NT))
                which = lax.rem(my_tp + j, tp) * 2 + h
                dt = jnp.where(lane1 == which, pick(2 * head + 2)[0:1, :], dt)
        for c in copies:
            c.wait_send()
        dt_ref[...] = dt
        low = m1_ref.shape[1]
        for i in range(2):
            m = big[i].astype(BF16)
            mt = m.T
            m1_ref[2 * i] = m[0:low, 0:256]
            m2_ref[2 * i] = m[low:, 128:]
            m1_ref[2 * i + 1] = mt[0:low, 0:256]
            m2_ref[2 * i + 1] = mt[low:, 128:]
        for c in save_copies(step - 1, 1 - slot) + save_copies(step, slot):
            c.wait()


def front_call(x, g, w, w4, gam, bet, temps, tp, sp, block=4096):
    rows, d = x.shape
    own = w4.shape[0]
    head = d // temps.shape[0]
    low = 256 // head * head
    steps = rows // block
    row = pl.BlockSpec((block, d), lambda i: (i, 0))
    full = lambda shape: pl.BlockSpec(shape, lambda i: (0,) * len(shape))
    smalls = [
        ((3 * (d - own), d), BF16),
        ((d, 3 * d), BF16),
        ((d - own, d), BF16),
        ((d, d), BF16),
        ((4, low, 256), BF16),
        ((4, d - low, 256), BF16),
        ((d, NT), F32),
        ((d, NT), F32),
        ((1, LANES), F32),
    ]
    dma = pltpu.SemaphoreType.DMA
    return pl.pallas_call(
        functools.partial(front_kernel, tp, sp, steps),
        grid=(steps,),
        in_specs=[row, row, full(w.shape), full(w4.shape), full(gam.shape), full(bet.shape), pl.BlockSpec(memory_space=pltpu.SMEM)],
        out_specs=[pl.BlockSpec(memory_space=pl.ANY)] * 2
        + [pl.BlockSpec((8, block), lambda i: (0, i))]
        + [full(s) for s, _ in smalls],
        out_shape=[jax.ShapeDtypeStruct((r, rows), t) for r, t in ((4 * own, BF16), (d, BF16), (8, F32))] + [jax.ShapeDtypeStruct(s, t) for s, t in smalls],
        scratch_shapes=[
            pltpu.VMEM((3 * own, d), BF16),
            pltpu.VMEM((d, NT), F32),
            pltpu.VMEM((d, NT), F32),
            pltpu.VMEM((d, block), BF16),
            pltpu.VMEM((d, block), BF16),
            pltpu.VMEM((d, block), BF16),
            pltpu.VMEM((2, 4 * own, block), BF16),
            pltpu.VMEM((2, d, block), BF16),
            pltpu.VMEM((2 * own, block), BF16),
            pltpu.VMEM((2 * own, block), BF16),
            pltpu.VMEM((2 * own, 256), F32),
            pltpu.VMEM((2 * own, LANES), F32),
            pltpu.VMEM((tp, 4, own, d), BF16),
            pltpu.VMEM((own, LANES), F32),
            pltpu.VMEM((head, LANES), F32),
            pltpu.VMEM((sp // 2, head, LANES), F32),
            pltpu.VMEM((tp, 2, head, LANES), F32),
            pltpu.VMEM((2, d, d), F32),
            dma((2, 2)),
            dma((tp, 2)),
            dma((tp, 2)),
            dma((1,)),
            dma((1,)),
            dma((sp // 2,)),
            dma((sp // 2,)),
            dma((tp, 2)),
            dma((tp, 2)),
        ],
        compiler_params=pltpu.CompilerParams(
            dimension_semantics=("arbitrary",), vmem_limit_bytes=60 * 2**20, collective_id=0, has_side_effects=True
        ),
        cost_estimate=pl.CostEstimate(flops=2 * rows * d * 4 * own, bytes_accessed=4 * rows * d, transcendentals=0),
        name="front",
    )(x, g, w, w4, gam, bet, temps)


def main_kernel(steps, x_ref, g_ref, save_ref, u_ref, st_ref, wt, wn, wo, wot, m1, m2, gam_ref, cq, ck, y_ref, dx_ref, dw_ref,
                gam, xt, gt, qkv, do, ot, rt, gx, acc_w, acc_o, acc_g):
    step = pl.program_id(0)
    rows, d = x_ref.shape
    rest = wo.shape[0]
    own = d - rest
    low = m1.shape[1]

    @pl.when(step == 0)
    def _():
        spread_columns(gam_ref, gam)
        acc_w[...] = jnp.zeros_like(acc_w)
        acc_o[...] = jnp.zeros_like(acc_o)
        acc_g[...] = jnp.zeros_like(acc_g)

    tiles = rows // NT
    at = lambda n: pl.ds(n * NT, NT)

    def project(n):
        for e in range(3):
            qkv[e * d : e * d + own, at(n)] = save_ref[e * own : (e + 1) * own, at(n)]
            qkv[e * d + own : (e + 1) * d, at(n)] = dot(wt[e * rest : (e + 1) * rest, :], u_ref[:, at(n)]).astype(BF16)
        do[0:own, at(n)] = save_ref[3 * own :, at(n)]
        do[own:, at(n)] = dot_nt(wo[...], g_ref[at(n), :]).astype(BF16)

    def mix(n):
        ot[0:low, at(n)] = dot(m1[0], qkv[2 * d : 2 * d + 256, at(n)]).astype(BF16)
        ot[low:d, at(n)] = dot(m2[0], qkv[2 * d + 128 : 3 * d, at(n)]).astype(BF16)
        rt[2 * d : 2 * d + low, at(n)] = dot(m1[1], do[0:256, at(n)]).astype(BF16)
        rt[2 * d + low : 3 * d, at(n)] = dot(m2[1], do[128:d, at(n)]).astype(BF16)
        for part, other, coef, i in ((0, d, cq, 2), (d, 0, ck, 3)):
            v = dot(m1[i], qkv[other : other + 256, at(n)])
            rt[part : part + low, at(n)] = (v + qkv[part : part + low, at(n)].astype(F32) * coef[0:low, :]).astype(BF16)
            v = dot(m2[i], qkv[other + 128 : other + d, at(n)])
            rt[part + low : part + d, at(n)] = (v + qkv[part + low : part + d, at(n)].astype(F32) * coef[low:d, :]).astype(BF16)

    def out(n):
        xt[:, at(n)] = x_ref[at(n), :].T
        for c, m in ((0, 128), (128, 256)):
            yt = dot(wot[c : c + m, :], ot[:, at(n)]) + xt[c : c + m, at(n)].astype(F32)
            y_ref[at(n), c : c + m] = yt.astype(BF16).T
        gx[:, at(n)] = dot(wn[...], rt[:, at(n)])

    def norm_bwd(*pair):
        mean = {n: st_ref[0:1, at(n)] for n in pair}
        inv = {n: st_ref[1:2, at(n)] for n in pair}
        s1 = {n: jnp.zeros((8, NT), F32) for n in pair}
        s2 = {n: jnp.zeros((8, NT), F32) for n in pair}
        for c in range(0, d, CH):
            gm = gam[c : c + CH, :]
            sum_h, sum_u = [], []
            for n in pair:
                du = gx[c : c + CH, at(n)]
                duh = du * (xt[c : c + CH, at(n)].astype(F32) * inv[n] - mean[n])
                s1[n] = s1[n] + fold8(du * gm)
                s2[n] = s2[n] + fold8(duh * gm)
                sum_h.append(duh)
                sum_u.append(du)
            v = sum(sum_h[1:], sum_h[0])
            acc_g[0, c : c + CH, :] += v[:, :LANES] + v[:, LANES:]
            v = sum(sum_u[1:], sum_u[0])
            acc_g[1, c : c + CH, :] += v[:, :LANES] + v[:, LANES:]
        for n in pair:
            m1_ = jnp.sum(s1[n], axis=0, keepdims=True) * (1.0 / d)
            m2_ = jnp.sum(s2[n], axis=0, keepdims=True) * (1.0 / d)
            slope = m2_ * inv[n] * inv[n]
            base = inv[n] * (mean[n] * m2_ - m1_)
            gt[:, at(n)] = g_ref[at(n), :].T
            for c in range(0, d, CH):
                v = gx[c : c + CH, at(n)] * gam[c : c + CH, :] * inv[n] + base - xt[c : c + CH, at(n)].astype(F32) * slope
                gt[c : c + CH, at(n)] = (v + gt[c : c + CH, at(n)].astype(F32)).astype(BF16)
            dx_ref[at(n), :] = gt[:, at(n)].T

    for n in range(tiles + 3):
        if n >= 3:
            norm_bwd(n - 3)
        if n < tiles:
            project(n)
        if 2 <= n < tiles + 2:
            out(n - 2)
        if 1 <= n < tiles + 1:
            mix(n - 1)
    r_own = jnp.concatenate([rt[e * d : e * d + own, :] for e in range(3)], axis=0)
    acc_w[...] += dot_nt(r_own, u_ref[...])
    acc_o[...] += dot(ot[0:own, :], g_ref[...])

    @pl.when(step == steps - 1)
    def _():
        sp, slot_rows = dw_ref.shape[0], dw_ref.shape[1]
        per = d // sp
        sub = own // sp
        wgrad = acc_w[...].T
        for s in range(sp):
            dw_ref[s, 0:per, 0 : 3 * own] = wgrad[s * per : (s + 1) * per, :]
            for q in range(d // own):
                dw_ref[s, q * sub : (q + 1) * sub, 3 * own :] = acc_o[s * sub : (s + 1) * sub, q * own : (q + 1) * own]
        zero = jnp.zeros((slot_rows - per - 2, d), F32)
        gb = jnp.concatenate([jnp.sum(acc_g[i].T, axis=0, keepdims=True) for i in range(2)] + [zero], axis=0)
        for s in range(sp):
            dw_ref[s, per:slot_rows, :] = gb


def main_call(x, g, save, u, st, wt, wn, wo, wot, m1, m2, gam, cq, ck, sp, block=2048):
    rows, d = x.shape
    own = d - wo.shape[0]
    steps = rows // block
    row = pl.BlockSpec((block, d), lambda i: (i, 0))
    col = lambda a: pl.BlockSpec((a.shape[0], block), lambda i: (0, i))
    full = lambda a: pl.BlockSpec(a.shape, lambda i: (0,) * a.ndim)
    slot = (sp, d // sp + 8, d)
    smalls = (wt, wn, wo, wot, m1, m2, gam, cq, ck)
    return pl.pallas_call(
        functools.partial(main_kernel, steps),
        grid=(steps,),
        in_specs=[row, row, col(save), col(u), col(st)] + [full(a) for a in smalls],
        out_specs=[row, row, pl.BlockSpec(slot, lambda i: (0, 0, 0))],
        out_shape=[jax.ShapeDtypeStruct((rows, d), BF16), jax.ShapeDtypeStruct((rows, d), BF16), jax.ShapeDtypeStruct(slot, F32)],
        scratch_shapes=[
            pltpu.VMEM((d, NT), F32),
            pltpu.VMEM((d, block), BF16),
            pltpu.VMEM((d, block), BF16),
            pltpu.VMEM((3 * d, block), BF16),
            pltpu.VMEM((d, block), BF16),
            pltpu.VMEM((d, block), BF16),
            pltpu.VMEM((3 * d, block), BF16),
            pltpu.VMEM((d, block), F32),
            pltpu.VMEM((3 * own, d), F32),
            pltpu.VMEM((own, d), F32),
            pltpu.VMEM((2, d, LANES), F32),
        ],
        compiler_params=pltpu.CompilerParams(dimension_semantics=("arbitrary",), vmem_limit_bytes=60 * 2**20),
        cost_estimate=pl.CostEstimate(flops=2 * rows * d * d * 9, bytes_accessed=8 * rows * d, transcendentals=0),
        name="main",
    )(x, g, save, u, st, *smalls)


def wgrad_kernel(sp, in_ref, out_ref, mine, pair, got, sem, send_a, recv_a, send_b, recv_b):
    my = lax.axis_index("sp")
    chips = sp // 2
    core, chip = lax.rem(my, 2), my // 2
    other = {"sp": chip * 2 + 1 - core}
    peers = [{"sp": lax.rem(chip + k, chips) * 2 + core} for k in range(1, chips)]
    barrier = pltpu.get_barrier_semaphore()
    for peer in [other] + peers:
        pl.semaphore_signal(barrier, inc=1, device_id=peer, device_id_type=MESH)
    load = pltpu.make_async_copy(in_ref, mine, sem)
    load.start()
    load.wait()
    pl.semaphore_wait(barrier, chips)
    first = [remote(mine.at[2 * c + 1 - core], pair.at[c], send_a.at[c], recv_a.at[c], other) for c in range(chips)]
    for c in first:
        c.start()
    for c in range(chips):
        first[c].wait()
    for c in range(chips):
        got[chips + c] = mine[2 * c + core] + pair[c]
    second = [
        remote(got.at[chips + lax.rem(chip + k, chips)], got.at[chip], send_b.at[k], recv_b.at[k], peers[k - 1])
        for k in range(1, chips)
    ]
    for c in second:
        c.start()
    got[chip] = got[chips + chip]
    for c in second:
        c.wait()
    total = got[0]
    for c in range(1, chips):
        total = total + got[c]
    out_ref[...] = total


def wgrad_call(parts):
    sp, slot = parts.shape[0], parts.shape[1:]
    dma = pltpu.SemaphoreType.DMA
    return pl.pallas_call(
        functools.partial(wgrad_kernel, sp),
        in_specs=[pl.BlockSpec(memory_space=pl.ANY)],
        out_specs=pl.BlockSpec(memory_space=pltpu.VMEM),
        out_shape=jax.ShapeDtypeStruct(slot, F32),
        scratch_shapes=[
            pltpu.VMEM((sp, *slot), F32),
            pltpu.VMEM((sp // 2, *slot), F32),
            pltpu.VMEM((sp, *slot), F32),
            dma,
            dma((sp // 2,)),
            dma((sp // 2,)),
            dma((sp // 2,)),
            dma((sp // 2,)),
        ],
        compiler_params=pltpu.CompilerParams(collective_id=1, has_side_effects=True),
        name="wgrad",
    )(parts)


def finish_kernel(sum_ref, dt_ref, w_ref, o_ref, gam_ref, bet_ref, tau_ref):
    per, own = w_ref.shape[1:]
    sub = o_ref.shape[0]
    for e in range(3):
        w_ref[e] = sum_ref[0:per, e * own : (e + 1) * own]
    for q in range(o_ref.shape[1] // own):
        o_ref[:, q * own : (q + 1) * own] = sum_ref[q * sub : (q + 1) * sub, 3 * own :]
    gam_ref[...] = sum_ref[per]
    bet_ref[...] = sum_ref[per + 1]
    tau_ref[...] = dt_ref[0, 0 : tau_ref.shape[0]]


def finish_call(total, dt, own, sp, heads):
    d = total.shape[1]
    vmem = pl.BlockSpec(memory_space=pltpu.VMEM)
    shapes = [(3, d // sp, own), (own // sp, d), (d,), (d,), (heads,)]
    return pl.pallas_call(
        finish_kernel,
        in_specs=[vmem, vmem],
        out_specs=[vmem] * 5,
        out_shape=[jax.ShapeDtypeStruct(s, F32) for s in shapes],
        name="finish",
    )(total, dt)


def solution(mesh):
    tp, sp = mesh.shape["tp"], mesh.shape["sp"]
    row_spec = P(("dp", "sp"), None)

    def local_step(x, g, w_qkv, w_out, gamma, beta, temps):
        save, u, st, wt, wn, wo, wot, m1, m2, cq, ck, dt = front_call(
            x, g, w_qkv.transpose(1, 2, 0), w_out, gamma, beta, temps, tp, sp
        )
        y, dx, parts = main_call(x, g, save, u, st, wt, wn, wo, wot, m1, m2, gamma, cq, ck, sp)
        grad_w, grad_o, grad_gamma, grad_beta, grad_temp = finish_call(
            wgrad_call(parts), dt, w_out.shape[0], sp, temps.shape[0]
        )
        return y, dx, grad_w.transpose(1, 0, 2), grad_o, grad_gamma, grad_beta, grad_temp

    in_specs = (row_spec, row_spec, P(None, None, "tp"), P("tp", None), P(None), P(None), P(None))
    out_specs = (row_spec, row_spec, P(("dp", "sp"), None, "tp"), P(("dp", "tp", "sp"), None), P("dp"), P("dp"), P("dp"))
    return jax.shard_map(local_step, mesh=mesh, in_specs=in_specs, out_specs=out_specs, check_vma=False)
```

```python
import functools

import jax
import jax.numpy as jnp
from jax import lax
from jax.experimental import pallas as pl
from jax.experimental.pallas import tpu as pltpu
from jax.sharding import PartitionSpec as P

F32, BF16 = jnp.float32, jnp.bfloat16
LN_EPS = 1e-6
NT = 256
CH = 64
LANES = 128
MESH = pl.DeviceIdType.MESH


def dot(a, b):
    return jnp.dot(a, b, preferred_element_type=F32)


def dot_nt(a, b):
    return lax.dot_general(a, b, (((1,), (1,)), ((), ())), preferred_element_type=F32)


def fold8(v):
    return jnp.sum(v.reshape(v.shape[0] // 8, 8, v.shape[1]), axis=0)


def ln_stats(xt, cols):
    d = xt.shape[0]
    shift = xt[0:16, cols].astype(F32)[0:1, :]
    s1 = jnp.zeros((8, NT), F32)
    s2 = jnp.zeros((8, NT), F32)
    for c in range(0, d, CH):
        v = xt[c : c + CH, cols].astype(F32) - shift
        s1 = s1 + fold8(v)
        s2 = s2 + fold8(v * v)
    off = jnp.sum(s1, axis=0, keepdims=True) * (1.0 / d)
    var = jnp.sum(s2, axis=0, keepdims=True) * (1.0 / d) - off * off
    return shift + off, lax.rsqrt(jnp.maximum(var, 0.0) + LN_EPS)


def spread_columns(row_ref, out):
    d = row_ref.shape[0]
    out[...] = jnp.broadcast_to(row_ref[...].reshape(1, d), (NT, d)).T


def remote(src, dst, send_sem, recv_sem, device):
    return pltpu.make_async_remote_copy(
        src_ref=src, dst_ref=dst, send_sem=send_sem, recv_sem=recv_sem, device_id=device, device_id_type=MESH
    )


def head_state(t, tau, head):
    lane = lax.broadcasted_iota(jnp.int32, (head, LANES), 1)
    row = lax.broadcasted_iota(jnp.int32, (head, LANES), 0)
    valid = lane < head
    eye = lane == row
    pick = lambda i: t[:, i : i + 1]
    q2 = pick(2 * head)
    k2 = jnp.sum(jnp.where(eye, pick(2 * head + 1), 0.0), axis=0, keepdims=True)
    k2 = jnp.where(valid, k2, 1.0)
    norm = jnp.sqrt(q2) * jnp.sqrt(k2)
    gram_n = jnp.where(valid, t / norm, 0.0)
    datt = jnp.where(valid, pltpu.roll(t, LANES - head, 1), 0.0)
    logit = jnp.where(valid, tau * gram_n, -1e30)
    ex = jnp.exp(logit - jnp.max(logit, axis=1, keepdims=True))
    ex = jnp.where(valid, ex, 0.0)
    att = ex / jnp.sum(ex, axis=1, keepdims=True)
    d_logit = att * (datt - jnp.sum(att * datt, axis=1, keepdims=True))
    d_tau = jnp.sum(jnp.sum(d_logit * gram_n, axis=1, keepdims=True), axis=0, keepdims=True)
    e_mat = tau * d_logit
    d_gram = (e_mat / norm).astype(BF16).astype(F32)
    es = e_mat * gram_n
    q_coef = -jnp.sum(es, axis=1, keepdims=True) / q2
    k_coef = -jnp.sum(es, axis=0, keepdims=True) / k2
    k_coef = jnp.sum(jnp.where(eye, k_coef, 0.0), axis=1, keepdims=True)
    v = jnp.where(valid, att.astype(BF16).astype(F32), pltpu.roll(d_gram, head, 1))
    v = jnp.where(lane == 2 * head, q_coef, v)
    v = jnp.where(lane == 2 * head + 1, k_coef, v)
    return jnp.where(lane == 2 * head + 2, d_tau, v)


def front_kernel(tp, sp, steps, x_ref, g_ref, w_ref, w4_ref, gam_ref, bet_ref, temp_ref,
                 save_ref, u_ref, st_ref, wt_ref, wn_ref, wo_ref, wot_ref, m1_ref, m2_ref, cq_ref, ck_ref, dt_ref,
                 wq, gam, bet, xt, gt, ut, save_s, u_s, qd, kv, acc, sq, wall, sums, pair, parts, state, big,
                 out_sem, send_w, recv_w, send_p, recv_p, send_a, recv_a, send_b, recv_b):
    step = pl.program_id(0)
    my_sp, my_tp = lax.axis_index("sp"), lax.axis_index("tp")
    chips = sp // 2
    core, chip = lax.rem(my_sp, 2), my_sp // 2
    rows, d = x_ref.shape
    own = w4_ref.shape[0]
    head = own // 2
    rest = d - own
    other = {"sp": chip * 2 + 1 - core}
    chip_peers = [{"sp": lax.rem(chip + k, chips) * 2 + core} for k in range(1, chips)]
    tp_peers = [[{"tp": lax.rem(my_tp + k, tp), "sp": chip * 2 + t} for t in range(2)] for k in range(1, tp)]
    barrier = pltpu.get_barrier_semaphore()
    peers = [other] + chip_peers + [p for ps in tp_peers for p in ps]

    @pl.when(step == 0)
    def _():
        for peer in peers:
            pl.semaphore_signal(barrier, inc=1, device_id=peer, device_id_type=MESH)
        for e in range(3):
            wq[e * own : (e + 1) * own, :] = w_ref[e]
        spread_columns(gam_ref, gam)
        spread_columns(bet_ref, bet)
        acc[...] = jnp.zeros_like(acc)
        sq[...] = jnp.zeros_like(sq)

    def weight_copies():
        out = []
        for k in range(1, tp):
            for i, (src, dst) in enumerate(((w_ref, wall.at[tp - k, 0:3]), (w4_ref, wall.at[tp - k, 3]))):
                peer = {"tp": lax.rem(my_tp + k, tp), "sp": my_sp}
                out.append(remote(src, dst, send_w.at[k, i], recv_w.at[k, i], peer))
        return out

    @pl.when(step == 1)
    def _():
        pl.semaphore_wait(barrier, len(peers))
        for c in weight_copies():
            c.start()

    slot = lax.rem(step, 2)

    def save_copies(to, at_slot):
        cols = pl.ds(pl.multiple_of(to * rows, LANES), rows)
        return [
            pltpu.make_async_copy(save_s.at[at_slot], save_ref.at[:, cols], out_sem.at[at_slot, 0]),
            pltpu.make_async_copy(u_s.at[at_slot], u_ref.at[:, cols], out_sem.at[at_slot, 1]),
        ]

    @pl.when(step >= 2)
    def _():
        for c in save_copies(step - 2, slot):
            c.wait()

    tiles = rows // NT
    at = lambda n: pl.ds(n * NT, NT)

    def norm(n):
        xt[:, at(n)] = x_ref[at(n), :].T
        gt[:, at(n)] = g_ref[at(n), :].T
        mean, inv = ln_stats(xt, at(n))
        mean = mean * inv
        st_ref[0:1, at(n)] = mean
        st_ref[1:2, at(n)] = inv
        for c in range(0, d, CH):
            v = xt[c : c + CH, at(n)].astype(F32) * inv - mean
            v = (v * gam[c : c + CH, :] + bet[c : c + CH, :]).astype(BF16)
            ut[c : c + CH, at(n)] = v
            u_s[slot, c : c + CH, at(n)] = v

    def project(n):
        qkv = dot(wq[...], ut[:, at(n)])
        for e, (ref, r) in enumerate(((qd, 0), (kv, 0), (kv, own))):
            v = qkv[e * own : (e + 1) * own].astype(BF16)
            ref[r : r + own, at(n)] = v
            save_s[slot, e * own : (e + 1) * own, at(n)] = v
            if e < 2:
                v = v.astype(F32)
                v = v * v
                sq[e * own : (e + 1) * own] += v[:, :LANES] + v[:, LANES:]
        v = dot(w4_ref[...], gt[:, at(n)]).astype(BF16)
        qd[own:, at(n)] = v
        save_s[slot, 3 * own :, at(n)] = v

    def gram(n):
        cols = pl.ds(n * NT, 4 * NT)
        acc[:, 0 : 2 * own] += dot_nt(qd[:, cols], kv[:, cols])

    norm(0)
    for n in range(tiles):
        if n + 1 < tiles:
            norm(n + 1)
        if n >= 4 and n % 4 == 0:
            gram(n - 4)
        project(n)
    gram(tiles - 4)
    for c in save_copies(step, slot):
        c.start()

    @pl.when(step == steps - 1)
    def _():
        lane = lax.broadcasted_iota(jnp.int32, (head, LANES), 1)
        row = lax.broadcasted_iota(jnp.int32, (head, LANES), 0)
        valid = lane < head

        def block(r, c, to):
            shift = (to - c) % 256
            v = acc[r : r + head, :]
            return (pltpu.roll(v, shift, 1) if shift else v)[:, :LANES]

        for h in range(2):
            r = h * head
            q2 = jnp.sum(sq[r : r + head, :], axis=1, keepdims=True)
            k2 = jnp.sum(sq[own + r : own + r + head, :], axis=1, keepdims=True)
            v = jnp.where(valid, block(r, r, 0), block(own + r, own + r, head))
            v = jnp.where(lane == 2 * head, q2, v)
            sums[r : r + head, :] = jnp.where(lane == 2 * head + 1, k2, v)

        mine = pl.ds(pl.multiple_of(core * head, 8), head)
        theirs = pl.ds(pl.multiple_of((1 - core) * head, 8), head)
        first = remote(sums.at[theirs], pair, send_p.at[0], recv_p.at[0], other)
        first.start()
        for c in weight_copies():
            c.wait()
        first.wait()
        parts[chip] = sums[mine, :] + pair[...]
        copies = [
            remote(parts.at[chip], parts.at[chip], send_a.at[k], recv_a.at[k], chip_peers[k - 1]) for k in range(1, chips)
        ]
        for c in copies:
            c.start()
        big[...] = jnp.zeros_like(big)
        pieces = [(w_ref, w4_ref)] + [(wall.at[j, 0:3], wall.at[j, 3]) for j in range(1, tp)]
        for j, (piece, piece4) in enumerate(pieces):
            for e in range(3):
                wn_ref[:, e * d + j * own : e * d + (j + 1) * own] = piece[e].T
                if j:
                    wt_ref[e * rest + (j - 1) * own : e * rest + j * own, :] = piece[e]
            wot_ref[:, j * own : (j + 1) * own] = piece4[...].T
            if j:
                wo_ref[(j - 1) * own : j * own, :] = piece4[...]
        for c in copies:
            c.wait()
        total = parts[0]
        for k in range(1, chips):
            total = total + parts[k]
        state[0, core] = head_state(total, temp_ref[my_tp * 2 + core], head)

        copies = [remote(state.at[0, core], state.at[0, core], send_b.at[0, 0], recv_b.at[0, core], other)]
        for k in range(1, tp):
            for t in range(2):
                copies.append(
                    remote(state.at[0, core], state.at[tp - k, core], send_b.at[k, t], recv_b.at[k, core], tp_peers[k - 1][t])
                )
        for c in copies:
            c.start()
        lane1 = lax.broadcasted_iota(jnp.int32, dt_ref.shape, 1)
        dt = jnp.zeros(dt_ref.shape, F32)
        zero = jnp.zeros((head, d - LANES), F32)
        for j in (0, tp - 1, 1, *range(2, tp - 1)):
            k = tp - j
            if j == 0:
                remote(state.at[0, core], state.at[0, 1 - core], send_b.at[0, 0], recv_b.at[0, 1 - core], other).wait_recv()
            for h in range(2):
                if j:
                    remote(state.at[0, core], state.at[j, h], send_b.at[k, h], recv_b.at[k, h], tp_peers[k - 1][h]).wait_recv()
                t = state[j, h]
                pick = lambda i: t[:, i : i + 1]
                r = j * own + h * head
                att = jnp.concatenate([jnp.where(valid, t, 0.0), zero], axis=1)
                d_gram = jnp.concatenate([jnp.where(valid, pltpu.roll(t, LANES - head, 1), 0.0), zero], axis=1)
                big[0, r : r + head, :] = pltpu.roll(att, r, 1) if r else att
                big[1, r : r + head, :] = pltpu.roll(d_gram, r, 1) if r else d_gram
                cq_ref[r : r + head, :] = jnp.broadcast_to(pick(2 * head), (head, NT))
                ck_ref[r : r + head, :] = jnp.broadcast_to(pick(2 * head + 1), (head, NT))
                which = lax.rem(my_tp + j, tp) * 2 + h
                dt = jnp.where(lane1 == which, pick(2 * head + 2)[0:1, :], dt)
        for c in copies:
            c.wait_send()
        dt_ref[...] = dt
        low = m1_ref.shape[1]
        for i in range(2):
            m = big[i].astype(BF16)
            mt = m.T
            m1_ref[2 * i] = m[0:low, 0:256]
            m2_ref[2 * i] = m[low:, 128:]
            m1_ref[2 * i + 1] = mt[0:low, 0:256]
            m2_ref[2 * i + 1] = mt[low:, 128:]
        for c in save_copies(step - 1, 1 - slot) + save_copies(step, slot):
            c.wait()


def front_call(x, g, w, w4, gam, bet, temps, tp, sp, block=4096):
    rows, d = x.shape
    own = w4.shape[0]
    head = d // temps.shape[0]
    low = 256 // head * head
    steps = rows // block
    row = pl.BlockSpec((block, d), lambda i: (i, 0))
    full = lambda shape: pl.BlockSpec(shape, lambda i: (0,) * len(shape))
    smalls = [
        ((3 * (d - own), d), BF16),
        ((d, 3 * d), BF16),
        ((d - own, d), BF16),
        ((d, d), BF16),
        ((4, low, 256), BF16),
        ((4, d - low, 256), BF16),
        ((d, NT), F32),
        ((d, NT), F32),
        ((1, LANES), F32),
    ]
    dma = pltpu.SemaphoreType.DMA
    return pl.pallas_call(
        functools.partial(front_kernel, tp, sp, steps),
        grid=(steps,),
        in_specs=[row, row, full(w.shape), full(w4.shape), full(gam.shape), full(bet.shape), pl.BlockSpec(memory_space=pltpu.SMEM)],
        out_specs=[pl.BlockSpec(memory_space=pl.ANY)] * 2
        + [pl.BlockSpec((8, block), lambda i: (0, i))]
        + [full(s) for s, _ in smalls],
        out_shape=[jax.ShapeDtypeStruct((r, rows), t) for r, t in ((4 * own, BF16), (d, BF16), (8, F32))] + [jax.ShapeDtypeStruct(s, t) for s, t in smalls],
        scratch_shapes=[
            pltpu.VMEM((3 * own, d), BF16),
            pltpu.VMEM((d, NT), F32),
            pltpu.VMEM((d, NT), F32),
            pltpu.VMEM((d, block), BF16),
            pltpu.VMEM((d, block), BF16),
            pltpu.VMEM((d, block), BF16),
            pltpu.VMEM((2, 4 * own, block), BF16),
            pltpu.VMEM((2, d, block), BF16),
            pltpu.VMEM((2 * own, block), BF16),
            pltpu.VMEM((2 * own, block), BF16),
            pltpu.VMEM((2 * own, 256), F32),
            pltpu.VMEM((2 * own, LANES), F32),
            pltpu.VMEM((tp, 4, own, d), BF16),
            pltpu.VMEM((own, LANES), F32),
            pltpu.VMEM((head, LANES), F32),
            pltpu.VMEM((sp // 2, head, LANES), F32),
            pltpu.VMEM((tp, 2, head, LANES), F32),
            pltpu.VMEM((2, d, d), F32),
            dma((2, 2)),
            dma((tp, 2)),
            dma((tp, 2)),
            dma((1,)),
            dma((1,)),
            dma((sp // 2,)),
            dma((sp // 2,)),
            dma((tp, 2)),
            dma((tp, 2)),
        ],
        compiler_params=pltpu.CompilerParams(
            dimension_semantics=("arbitrary",), vmem_limit_bytes=60 * 2**20, collective_id=0, has_side_effects=True
        ),
        cost_estimate=pl.CostEstimate(flops=2 * rows * d * 4 * own, bytes_accessed=4 * rows * d, transcendentals=0),
        name="front",
    )(x, g, w, w4, gam, bet, temps)


def main_kernel(steps, x_ref, g_ref, save_ref, u_ref, st_ref, wt, wn, wo, wot, m1, m2, gam_ref, cq, ck, y_ref, dx_ref, dw_ref, gb_ref,
                gam, xt, gt, qkv, do, ot, rt, gx, acc_w, acc_o, acc_g):
    step = pl.program_id(0)
    rows, d = x_ref.shape
    rest = wo.shape[0]
    own = d - rest
    low = m1.shape[1]

    @pl.when(step == 0)
    def _():
        spread_columns(gam_ref, gam)
        acc_w[...] = jnp.zeros_like(acc_w)
        acc_o[...] = jnp.zeros_like(acc_o)
        acc_g[...] = jnp.zeros_like(acc_g)

    tiles = rows // NT
    at = lambda n: pl.ds(n * NT, NT)

    def project(n):
        for e in range(3):
            qkv[e * d : e * d + own, at(n)] = save_ref[e * own : (e + 1) * own, at(n)]
            qkv[e * d + own : (e + 1) * d, at(n)] = dot(wt[e * rest : (e + 1) * rest, :], u_ref[:, at(n)]).astype(BF16)
        do[0:own, at(n)] = save_ref[3 * own :, at(n)]
        do[own:, at(n)] = dot_nt(wo[...], g_ref[at(n), :]).astype(BF16)

    def mix(n):
        ot[0:low, at(n)] = dot(m1[0], qkv[2 * d : 2 * d + 256, at(n)]).astype(BF16)
        ot[low:d, at(n)] = dot(m2[0], qkv[2 * d + 128 : 3 * d, at(n)]).astype(BF16)
        rt[2 * d : 2 * d + low, at(n)] = dot(m1[1], do[0:256, at(n)]).astype(BF16)
        rt[2 * d + low : 3 * d, at(n)] = dot(m2[1], do[128:d, at(n)]).astype(BF16)
        for part, other, coef, i in ((0, d, cq, 2), (d, 0, ck, 3)):
            v = dot(m1[i], qkv[other : other + 256, at(n)])
            rt[part : part + low, at(n)] = (v + qkv[part : part + low, at(n)].astype(F32) * coef[0:low, :]).astype(BF16)
            v = dot(m2[i], qkv[other + 128 : other + d, at(n)])
            rt[part + low : part + d, at(n)] = (v + qkv[part + low : part + d, at(n)].astype(F32) * coef[low:d, :]).astype(BF16)

    def out(n):
        xt[:, at(n)] = x_ref[at(n), :].T
        for c, m in ((0, 128), (128, 256)):
            yt = dot(wot[c : c + m, :], ot[:, at(n)]) + xt[c : c + m, at(n)].astype(F32)
            y_ref[at(n), c : c + m] = yt.astype(BF16).T
        gx[:, at(n)] = dot(wn[...], rt[:, at(n)])

    def norm_bwd(*pair):
        mean = {n: st_ref[0:1, at(n)] for n in pair}
        inv = {n: st_ref[1:2, at(n)] for n in pair}
        s1 = {n: jnp.zeros((8, NT), F32) for n in pair}
        s2 = {n: jnp.zeros((8, NT), F32) for n in pair}
        for c in range(0, d, CH):
            gm = gam[c : c + CH, :]
            sum_h, sum_u = [], []
            for n in pair:
                du = gx[c : c + CH, at(n)]
                duh = du * (xt[c : c + CH, at(n)].astype(F32) * inv[n] - mean[n])
                s1[n] = s1[n] + fold8(du * gm)
                s2[n] = s2[n] + fold8(duh * gm)
                sum_h.append(duh)
                sum_u.append(du)
            v = sum(sum_h[1:], sum_h[0])
            acc_g[0, c : c + CH, :] += v[:, :LANES] + v[:, LANES:]
            v = sum(sum_u[1:], sum_u[0])
            acc_g[1, c : c + CH, :] += v[:, :LANES] + v[:, LANES:]
        for n in pair:
            m1_ = jnp.sum(s1[n], axis=0, keepdims=True) * (1.0 / d)
            m2_ = jnp.sum(s2[n], axis=0, keepdims=True) * (1.0 / d)
            slope = m2_ * inv[n] * inv[n]
            base = inv[n] * (mean[n] * m2_ - m1_)
            gt[:, at(n)] = g_ref[at(n), :].T
            for c in range(0, d, CH):
                v = gx[c : c + CH, at(n)] * gam[c : c + CH, :] * inv[n] + base - xt[c : c + CH, at(n)].astype(F32) * slope
                gt[c : c + CH, at(n)] = (v + gt[c : c + CH, at(n)].astype(F32)).astype(BF16)
            dx_ref[at(n), :] = gt[:, at(n)].T

    for n in range(tiles + 3):
        if n >= 3:
            norm_bwd(n - 3)
        if n < tiles:
            project(n)
        if 2 <= n < tiles + 2:
            out(n - 2)
        if 1 <= n < tiles + 1:
            mix(n - 1)
    r_own = jnp.concatenate([rt[e * d : e * d + own, :] for e in range(3)], axis=0)
    acc_w[...] += dot_nt(r_own, u_ref[...])
    acc_o[...] += dot(ot[0:own, :], g_ref[...])

    @pl.when(step == steps - 1)
    def _():
        sp = dw_ref.shape[0]
        per = d // sp
        sub = own // sp
        wgrad = acc_w[...].T
        for s in range(sp):
            dw_ref[s, 0:per, 0 : 3 * own] = wgrad[s * per : (s + 1) * per, :]
            for q in range(d // own):
                dw_ref[s, q * sub : (q + 1) * sub, 3 * own :] = acc_o[s * sub : (s + 1) * sub, q * own : (q + 1) * own]
        for i in range(2):
            row = jnp.sum(acc_g[i].T, axis=0, keepdims=True)
            for q in range(d // own):
                gb_ref[i * (d // own) + q : i * (d // own) + q + 1, 0:own] = row[:, q * own : (q + 1) * own]


def main_call(x, g, save, u, st, wt, wn, wo, wot, m1, m2, gam, cq, ck, sp, block=2048):
    rows, d = x.shape
    own = d - wo.shape[0]
    steps = rows // block
    row = pl.BlockSpec((block, d), lambda i: (i, 0))
    col = lambda a: pl.BlockSpec((a.shape[0], block), lambda i: (0, i))
    full = lambda a: pl.BlockSpec(a.shape, lambda i: (0,) * a.ndim)
    slot = (sp, d // sp, d)
    sums = (2 * d // own, LANES)
    smalls = (wt, wn, wo, wot, m1, m2, gam, cq, ck)
    return pl.pallas_call(
        functools.partial(main_kernel, steps),
        grid=(steps,),
        in_specs=[row, row, col(save), col(u), col(st)] + [full(a) for a in smalls],
        out_specs=[row, row, pl.BlockSpec(slot, lambda i: (0, 0, 0)), pl.BlockSpec(sums, lambda i: (0, 0))],
        out_shape=[jax.ShapeDtypeStruct((rows, d), BF16), jax.ShapeDtypeStruct((rows, d), BF16), jax.ShapeDtypeStruct(slot, F32), jax.ShapeDtypeStruct(sums, F32)],
        scratch_shapes=[
            pltpu.VMEM((d, NT), F32),
            pltpu.VMEM((d, block), BF16),
            pltpu.VMEM((d, block), BF16),
            pltpu.VMEM((3 * d, block), BF16),
            pltpu.VMEM((d, block), BF16),
            pltpu.VMEM((d, block), BF16),
            pltpu.VMEM((3 * d, block), BF16),
            pltpu.VMEM((d, block), F32),
            pltpu.VMEM((3 * own, d), F32),
            pltpu.VMEM((own, d), F32),
            pltpu.VMEM((2, d, LANES), F32),
        ],
        compiler_params=pltpu.CompilerParams(dimension_semantics=("arbitrary",), vmem_limit_bytes=60 * 2**20),
        cost_estimate=pl.CostEstimate(flops=2 * rows * d * d * 9, bytes_accessed=8 * rows * d, transcendentals=0),
        name="main",
    )(x, g, save, u, st, *smalls)


def wgrad_kernel(sp, in_ref, gb_in, out_ref, gb_out, mine, pair, got, gb_mine, gb_pair, gb_got, sem, send_a, recv_a, send_b, recv_b):
    my = lax.axis_index("sp")
    chips = sp // 2
    core, chip = lax.rem(my, 2), my // 2
    other = {"sp": chip * 2 + 1 - core}
    there = [lax.rem(chip + k, chips) for k in range(chips)]
    peers = [{"sp": c * 2 + core} for c in there]
    barrier = pltpu.get_barrier_semaphore()
    for peer in [other] + peers[1:]:
        pl.semaphore_signal(barrier, inc=1, device_id=peer, device_id_type=MESH)
    loads = [pltpu.make_async_copy(in_ref, mine, sem.at[0]), pltpu.make_async_copy(gb_in, gb_mine, sem.at[1])]
    for c in loads:
        c.start()
    for c in loads:
        c.wait()
    pl.semaphore_wait(barrier, chips)
    order = sorted(range(1, chips), key=lambda k: -min(k, chips - k)) + [0]
    first = [remote(mine.at[2 * c + 1 - core], pair.at[c], send_a.at[k], recv_a.at[k], other) for k, c in enumerate(there)]
    gb_first = remote(gb_mine, gb_pair, send_a.at[chips], recv_a.at[chips], other)
    for k in order:
        first[k].start()
    gb_first.start()
    second = {
        k: remote(got.at[chips + there[k]], got.at[chip], send_b.at[k], recv_b.at[k], peers[k]) for k in range(1, chips)
    }
    for k in order:
        first[k].wait()
        v = mine[2 * there[k] + core] + pair[there[k]]
        if k:
            got[chips + there[k]] = v
            second[k].start()
        else:
            got[chip] = v
    gb_first.wait()
    gb_got[chips] = gb_mine[...] + gb_pair[...]
    gb_second = [
        remote(gb_got.at[chips], gb_got.at[chip], send_b.at[chips + k], recv_b.at[chips + k], peers[k]) for k in range(1, chips)
    ]
    for c in gb_second:
        c.start()
    gb_got[chip] = gb_mine[...] + gb_pair[...]
    for k in order[:-1]:
        second[k].wait()
    total = got[0]
    for c in range(1, chips):
        total = total + got[c]
    out_ref[...] = total
    for c in gb_second:
        c.wait()
    total = gb_got[0]
    for c in range(1, chips):
        total = total + gb_got[c]
    gb_out[...] = total


def wgrad_call(parts, gb):
    sp, slot = parts.shape[0], parts.shape[1:]
    chips = sp // 2
    dma = pltpu.SemaphoreType.DMA
    hbm, vmem = pl.BlockSpec(memory_space=pl.ANY), pl.BlockSpec(memory_space=pltpu.VMEM)
    return pl.pallas_call(
        functools.partial(wgrad_kernel, sp),
        in_specs=[hbm, hbm],
        out_specs=[vmem, vmem],
        out_shape=[jax.ShapeDtypeStruct(slot, F32), jax.ShapeDtypeStruct(gb.shape, F32)],
        scratch_shapes=[
            pltpu.VMEM((sp, *slot), F32),
            pltpu.VMEM((chips, *slot), F32),
            pltpu.VMEM((sp, *slot), F32),
            pltpu.VMEM(gb.shape, F32),
            pltpu.VMEM(gb.shape, F32),
            pltpu.VMEM((chips + 1, *gb.shape), F32),
            dma((2,)),
            dma((chips + 1,)),
            dma((chips + 1,)),
            dma((sp,)),
            dma((sp,)),
        ],
        compiler_params=pltpu.CompilerParams(collective_id=1, has_side_effects=True),
        name="wgrad",
    )(parts, gb)


def finish_kernel(sum_ref, gb_ref, dt_ref, w_ref, o_ref, gam_ref, bet_ref, tau_ref):
    own = w_ref.shape[2]
    sub = o_ref.shape[0]
    split = o_ref.shape[1] // own
    for e in range(3):
        w_ref[e] = sum_ref[:, e * own : (e + 1) * own]
    for q in range(split):
        o_ref[:, q * own : (q + 1) * own] = sum_ref[q * sub : (q + 1) * sub, 3 * own :]
    for i, ref in enumerate((gam_ref, bet_ref)):
        row = [gb_ref[i * split + q : i * split + q + 1, 0:own] for q in range(split)]
        ref[...] = jnp.concatenate(row, axis=1)[0]
    tau_ref[...] = dt_ref[0, 0 : tau_ref.shape[0]]


def finish_call(total, gb, dt, own, sp, heads):
    d = total.shape[1]
    vmem = pl.BlockSpec(memory_space=pltpu.VMEM)
    shapes = [(3, d // sp, own), (own // sp, d), (d,), (d,), (heads,)]
    return pl.pallas_call(
        finish_kernel,
        in_specs=[vmem] * 3,
        out_specs=[vmem] * 5,
        out_shape=[jax.ShapeDtypeStruct(s, F32) for s in shapes],
        name="finish",
    )(total, gb, dt)


def solution(mesh):
    tp, sp = mesh.shape["tp"], mesh.shape["sp"]
    row_spec = P(("dp", "sp"), None)

    def local_step(x, g, w_qkv, w_out, gamma, beta, temps):
        save, u, st, wt, wn, wo, wot, m1, m2, cq, ck, dt = front_call(
            x, g, w_qkv.transpose(1, 2, 0), w_out, gamma, beta, temps, tp, sp
        )
        y, dx, parts, gb = main_call(x, g, save, u, st, wt, wn, wo, wot, m1, m2, gamma, cq, ck, sp)
        grad_w, grad_o, grad_gamma, grad_beta, grad_temp = finish_call(
            *wgrad_call(parts, gb), dt, w_out.shape[0], sp, temps.shape[0]
        )
        return y, dx, grad_w.transpose(1, 0, 2), grad_o, grad_gamma, grad_beta, grad_temp

    in_specs = (row_spec, row_spec, P(None, None, "tp"), P("tp", None), P(None), P(None), P(None))
    out_specs = (row_spec, row_spec, P(("dp", "sp"), None, "tp"), P(("dp", "tp", "sp"), None), P("dp"), P("dp"), P("dp"))
    return jax.shard_map(local_step, mesh=mesh, in_specs=in_specs, out_specs=out_specs, check_vma=False)
```

```python
import functools

import jax
import jax.numpy as jnp
from jax import lax
from jax.experimental import pallas as pl
from jax.experimental.pallas import tpu as pltpu
from jax.sharding import PartitionSpec as P

F32, BF16 = jnp.float32, jnp.bfloat16
LN_EPS = 1e-6
NT = 256
CH = 64
LANES = 128
MESH = pl.DeviceIdType.MESH


def dot(a, b):
    return jnp.dot(a, b, preferred_element_type=F32)


def dot_nt(a, b):
    return lax.dot_general(a, b, (((1,), (1,)), ((), ())), preferred_element_type=F32)


def fold8(v):
    return jnp.sum(v.reshape(v.shape[0] // 8, 8, v.shape[1]), axis=0)


def ln_stats(xt, cols):
    d = xt.shape[0]
    acc = jnp.zeros((8, NT), F32)
    for c in range(0, d, CH):
        acc = acc + fold8(xt[c : c + CH, cols].astype(F32))
    mean = jnp.sum(acc, axis=0, keepdims=True) * (1.0 / d)
    acc = jnp.zeros((8, NT), F32)
    for c in range(0, d, CH):
        v = xt[c : c + CH, cols].astype(F32) - mean
        acc = acc + fold8(v * v)
    return mean, lax.rsqrt(jnp.sum(acc, axis=0, keepdims=True) * (1.0 / d) + LN_EPS)


def spread_columns(row_ref, out):
    d = row_ref.shape[0]
    out[...] = jnp.broadcast_to(row_ref[...].reshape(1, d), (NT, d)).T


def remote(src, dst, send_sem, recv_sem, device):
    return pltpu.make_async_remote_copy(
        src_ref=src, dst_ref=dst, send_sem=send_sem, recv_sem=recv_sem, device_id=device, device_id_type=MESH
    )


def head_state(t, tau, head):
    lane = lax.broadcasted_iota(jnp.int32, (head, LANES), 1)
    row = lax.broadcasted_iota(jnp.int32, (head, LANES), 0)
    valid = lane < head
    eye = lane == row
    pick = lambda i: t[:, i : i + 1]
    q2 = pick(2 * head)
    k2 = jnp.sum(jnp.where(eye, pick(2 * head + 1), 0.0), axis=0, keepdims=True)
    k2 = jnp.where(valid, k2, 1.0)
    norm = jnp.sqrt(q2) * jnp.sqrt(k2)
    gram_n = jnp.where(valid, t / norm, 0.0)
    datt = jnp.where(valid, pltpu.roll(t, LANES - head, 1), 0.0)
    logit = jnp.where(valid, tau * gram_n, -1e30)
    ex = jnp.exp(logit - jnp.max(logit, axis=1, keepdims=True))
    ex = jnp.where(valid, ex, 0.0)
    att = ex / jnp.sum(ex, axis=1, keepdims=True)
    d_logit = att * (datt - jnp.sum(att * datt, axis=1, keepdims=True))
    d_tau = jnp.sum(jnp.sum(d_logit * gram_n, axis=1, keepdims=True), axis=0, keepdims=True)
    e_mat = tau * d_logit
    d_gram = (e_mat / norm).astype(BF16).astype(F32)
    es = e_mat * gram_n
    q_coef = -jnp.sum(es, axis=1, keepdims=True) / q2
    k_coef = -jnp.sum(es, axis=0, keepdims=True) / k2
    k_coef = jnp.sum(jnp.where(eye, k_coef, 0.0), axis=1, keepdims=True)
    v = jnp.where(valid, att.astype(BF16).astype(F32), pltpu.roll(d_gram, head, 1))
    v = jnp.where(lane == 2 * head, q_coef, v)
    v = jnp.where(lane == 2 * head + 1, k_coef, v)
    return jnp.where(lane == 2 * head + 2, d_tau, v)


def front_kernel(tp, sp, steps, x_ref, g_ref, w_ref, w4_ref, gam_ref, bet_ref, temp_ref,
                 save_ref, u_ref, st_ref, wt_ref, wn_ref, wo_ref, wot_ref, m1_ref, m2_ref, cq_ref, ck_ref, dt_ref,
                 wq, gam, bet, xt, gt, ut, save_s, u_s, qd, kv, acc, sq, wall, sums, pair, parts, state, big,
                 out_sem, send_w, recv_w, send_p, recv_p, send_a, recv_a, send_b, recv_b):
    step = pl.program_id(0)
    my_sp, my_tp = lax.axis_index("sp"), lax.axis_index("tp")
    chips = sp // 2
    core, chip = lax.rem(my_sp, 2), my_sp // 2
    rows, d = x_ref.shape
    own = w4_ref.shape[0]
    head = own // 2
    rest = d - own
    other = {"sp": chip * 2 + 1 - core}
    chip_peers = [{"sp": lax.rem(chip + k, chips) * 2 + core} for k in range(1, chips)]
    tp_peers = [[{"tp": lax.rem(my_tp + k, tp), "sp": chip * 2 + t} for t in range(2)] for k in range(1, tp)]
    barrier = pltpu.get_barrier_semaphore()
    peers = [other] + chip_peers + [p for ps in tp_peers for p in ps]

    @pl.when(step == 0)
    def _():
        for peer in peers:
            pl.semaphore_signal(barrier, inc=1, device_id=peer, device_id_type=MESH)
        for e in range(3):
            wq[e * own : (e + 1) * own, :] = w_ref[e]
        spread_columns(gam_ref, gam)
        spread_columns(bet_ref, bet)
        acc[...] = jnp.zeros_like(acc)
        sq[...] = jnp.zeros_like(sq)

    def weight_copies():
        out = []
        for k in range(1, tp):
            for i, (src, dst) in enumerate(((w_ref, wall.at[tp - k, 0:3]), (w4_ref, wall.at[tp - k, 3]))):
                peer = {"tp": lax.rem(my_tp + k, tp), "sp": my_sp}
                out.append(remote(src, dst, send_w.at[k, i], recv_w.at[k, i], peer))
        return out

    @pl.when(step == 1)
    def _():
        pl.semaphore_wait(barrier, len(peers))
        for c in weight_copies():
            c.start()

    slot = lax.rem(step, 2)

    def save_copies(to, at_slot):
        cols = pl.ds(pl.multiple_of(to * rows, LANES), rows)
        return [
            pltpu.make_async_copy(save_s.at[at_slot], save_ref.at[:, cols], out_sem.at[at_slot, 0]),
            pltpu.make_async_copy(u_s.at[at_slot], u_ref.at[:, cols], out_sem.at[at_slot, 1]),
        ]

    @pl.when(step >= 2)
    def _():
        for c in save_copies(step - 2, slot):
            c.wait()

    tiles = rows // NT
    at = lambda n: pl.ds(n * NT, NT)

    def norm(n):
        xt[:, at(n)] = x_ref[at(n), :].T
        gt[:, at(n)] = g_ref[at(n), :].T
        mean, inv = ln_stats(xt, at(n))
        st_ref[0:1, at(n)] = mean
        st_ref[1:2, at(n)] = inv
        for c in range(0, d, CH):
            v = (xt[c : c + CH, at(n)].astype(F32) - mean) * inv
            v = (v * gam[c : c + CH, :] + bet[c : c + CH, :]).astype(BF16)
            ut[c : c + CH, at(n)] = v
            u_s[slot, c : c + CH, at(n)] = v

    def project(n):
        qkv = dot(wq[...], ut[:, at(n)])
        for e, (ref, r) in enumerate(((qd, 0), (kv, 0), (kv, own))):
            v = qkv[e * own : (e + 1) * own].astype(BF16)
            ref[r : r + own, at(n)] = v
            save_s[slot, e * own : (e + 1) * own, at(n)] = v
            if e < 2:
                v = v.astype(F32)
                v = v * v
                sq[e * own : (e + 1) * own] += v[:, :LANES] + v[:, LANES:]
        v = dot(w4_ref[...], gt[:, at(n)]).astype(BF16)
        qd[own:, at(n)] = v
        save_s[slot, 3 * own :, at(n)] = v

    def gram(n):
        cols = pl.ds(n * NT, 4 * NT)
        acc[:, 0 : 2 * own] += dot_nt(qd[:, cols], kv[:, cols])

    norm(0)
    for n in range(tiles):
        if n + 1 < tiles:
            norm(n + 1)
        if n >= 4 and n % 4 == 0:
            gram(n - 4)
        project(n)
    gram(tiles - 4)
    for c in save_copies(step, slot):
        c.start()

    @pl.when(step == steps - 1)
    def _():
        lane = lax.broadcasted_iota(jnp.int32, (head, LANES), 1)
        row = lax.broadcasted_iota(jnp.int32, (head, LANES), 0)
        valid = lane < head

        def block(r, c, to):
            shift = (to - c) % 256
            v = acc[r : r + head, :]
            return (pltpu.roll(v, shift, 1) if shift else v)[:, :LANES]

        for h in range(2):
            r = h * head
            q2 = jnp.sum(sq[r : r + head, :], axis=1, keepdims=True)
            k2 = jnp.sum(sq[own + r : own + r + head, :], axis=1, keepdims=True)
            v = jnp.where(valid, block(r, r, 0), block(own + r, own + r, head))
            v = jnp.where(lane == 2 * head, q2, v)
            sums[r : r + head, :] = jnp.where(lane == 2 * head + 1, k2, v)

        mine = pl.ds(pl.multiple_of(core * head, 8), head)
        theirs = pl.ds(pl.multiple_of((1 - core) * head, 8), head)
        first = remote(sums.at[theirs], pair, send_p.at[0], recv_p.at[0], other)
        first.start()
        for c in weight_copies():
            c.wait()
        first.wait()
        parts[chip] = sums[mine, :] + pair[...]
        copies = [
            remote(parts.at[chip], parts.at[chip], send_a.at[k], recv_a.at[k], chip_peers[k - 1]) for k in range(1, chips)
        ]
        for c in copies:
            c.start()
        big[...] = jnp.zeros_like(big)
        pieces = [(w_ref, w4_ref)] + [(wall.at[j, 0:3], wall.at[j, 3]) for j in range(1, tp)]
        for j, (piece, piece4) in enumerate(pieces):
            for e in range(3):
                wn_ref[:, e * d + j * own : e * d + (j + 1) * own] = piece[e].T
                if j:
                    wt_ref[e * rest + (j - 1) * own : e * rest + j * own, :] = piece[e]
            wot_ref[:, j * own : (j + 1) * own] = piece4[...].T
            if j:
                wo_ref[(j - 1) * own : j * own, :] = piece4[...]
        for c in copies:
            c.wait()
        total = parts[0]
        for k in range(1, chips):
            total = total + parts[k]
        state[0, core] = head_state(total, temp_ref[my_tp * 2 + core], head)

        copies = [remote(state.at[0, core], state.at[0, core], send_b.at[0, 0], recv_b.at[0, core], other)]
        for k in range(1, tp):
            for t in range(2):
                copies.append(
                    remote(state.at[0, core], state.at[tp - k, core], send_b.at[k, t], recv_b.at[k, core], tp_peers[k - 1][t])
                )
        for c in copies:
            c.start()
        lane1 = lax.broadcasted_iota(jnp.int32, dt_ref.shape, 1)
        dt = jnp.zeros(dt_ref.shape, F32)
        zero = jnp.zeros((head, d - LANES), F32)
        for j in (0, tp - 1, 1, *range(2, tp - 1)):
            k = tp - j
            if j == 0:
                remote(state.at[0, core], state.at[0, 1 - core], send_b.at[0, 0], recv_b.at[0, 1 - core], other).wait_recv()
            for h in range(2):
                if j:
                    remote(state.at[0, core], state.at[j, h], send_b.at[k, h], recv_b.at[k, h], tp_peers[k - 1][h]).wait_recv()
                t = state[j, h]
                pick = lambda i: t[:, i : i + 1]
                r = j * own + h * head
                att = jnp.concatenate([jnp.where(valid, t, 0.0), zero], axis=1)
                d_gram = jnp.concatenate([jnp.where(valid, pltpu.roll(t, LANES - head, 1), 0.0), zero], axis=1)
                big[0, r : r + head, :] = pltpu.roll(att, r, 1) if r else att
                big[1, r : r + head, :] = pltpu.roll(d_gram, r, 1) if r else d_gram
                cq_ref[r : r + head, :] = jnp.broadcast_to(pick(2 * head), (head, NT))
                ck_ref[r : r + head, :] = jnp.broadcast_to(pick(2 * head + 1), (head, NT))
                which = lax.rem(my_tp + j, tp) * 2 + h
                dt = jnp.where(lane1 == which, pick(2 * head + 2)[0:1, :], dt)
        for c in copies:
            c.wait_send()
        dt_ref[...] = dt
        low = m1_ref.shape[1]
        for i in range(2):
            m = big[i].astype(BF16)
            mt = m.T
            m1_ref[2 * i] = m[0:low, 0:256]
            m2_ref[2 * i] = m[low:, 128:]
            m1_ref[2 * i + 1] = mt[0:low, 0:256]
            m2_ref[2 * i + 1] = mt[low:, 128:]
        for c in save_copies(step - 1, 1 - slot) + save_copies(step, slot):
            c.wait()


def front_call(x, g, w, w4, gam, bet, temps, tp, sp, block=4096):
    rows, d = x.shape
    own = w4.shape[0]
    head = d // temps.shape[0]
    low = 256 // head * head
    steps = rows // block
    row = pl.BlockSpec((block, d), lambda i: (i, 0))
    full = lambda shape: pl.BlockSpec(shape, lambda i: (0,) * len(shape))
    smalls = [
        ((3 * (d - own), d), BF16),
        ((d, 3 * d), BF16),
        ((d - own, d), BF16),
        ((d, d), BF16),
        ((4, low, 256), BF16),
        ((4, d - low, 256), BF16),
        ((d, NT), F32),
        ((d, NT), F32),
        ((1, LANES), F32),
    ]
    dma = pltpu.SemaphoreType.DMA
    return pl.pallas_call(
        functools.partial(front_kernel, tp, sp, steps),
        grid=(steps,),
        in_specs=[row, row, full(w.shape), full(w4.shape), full(gam.shape), full(bet.shape), pl.BlockSpec(memory_space=pltpu.SMEM)],
        out_specs=[pl.BlockSpec(memory_space=pl.ANY)] * 2
        + [pl.BlockSpec((8, block), lambda i: (0, i))]
        + [full(s) for s, _ in smalls],
        out_shape=[jax.ShapeDtypeStruct((r, rows), t) for r, t in ((4 * own, BF16), (d, BF16), (8, F32))] + [jax.ShapeDtypeStruct(s, t) for s, t in smalls],
        scratch_shapes=[
            pltpu.VMEM((3 * own, d), BF16),
            pltpu.VMEM((d, NT), F32),
            pltpu.VMEM((d, NT), F32),
            pltpu.VMEM((d, block), BF16),
            pltpu.VMEM((d, block), BF16),
            pltpu.VMEM((d, block), BF16),
            pltpu.VMEM((2, 4 * own, block), BF16),
            pltpu.VMEM((2, d, block), BF16),
            pltpu.VMEM((2 * own, block), BF16),
            pltpu.VMEM((2 * own, block), BF16),
            pltpu.VMEM((2 * own, 256), F32),
            pltpu.VMEM((2 * own, LANES), F32),
            pltpu.VMEM((tp, 4, own, d), BF16),
            pltpu.VMEM((own, LANES), F32),
            pltpu.VMEM((head, LANES), F32),
            pltpu.VMEM((sp // 2, head, LANES), F32),
            pltpu.VMEM((tp, 2, head, LANES), F32),
            pltpu.VMEM((2, d, d), F32),
            dma((2, 2)),
            dma((tp, 2)),
            dma((tp, 2)),
            dma((1,)),
            dma((1,)),
            dma((sp // 2,)),
            dma((sp // 2,)),
            dma((tp, 2)),
            dma((tp, 2)),
        ],
        compiler_params=pltpu.CompilerParams(
            dimension_semantics=("arbitrary",), vmem_limit_bytes=60 * 2**20, collective_id=0, has_side_effects=True
        ),
        cost_estimate=pl.CostEstimate(flops=2 * rows * d * 4 * own, bytes_accessed=4 * rows * d, transcendentals=0),
        name="front",
    )(x, g, w, w4, gam, bet, temps)


def main_kernel(steps, x_ref, g_ref, save_ref, u_ref, st_ref, wt, wn, wo, wot, m1, m2, gam_ref, cq, ck, y_ref, dx_ref, dw_ref, gb_ref,
                gam, xt, gt, qkv, do, ot, rt, gx, acc_w, acc_o, acc_g):
    step = pl.program_id(0)
    rows, d = x_ref.shape
    rest = wo.shape[0]
    own = d - rest
    low = m1.shape[1]

    @pl.when(step == 0)
    def _():
        spread_columns(gam_ref, gam)
        acc_w[...] = jnp.zeros_like(acc_w)
        acc_o[...] = jnp.zeros_like(acc_o)
        acc_g[...] = jnp.zeros_like(acc_g)

    tiles = rows // NT
    at = lambda n: pl.ds(n * NT, NT)

    def project(n):
        for e in range(3):
            qkv[e * d : e * d + own, at(n)] = save_ref[e * own : (e + 1) * own, at(n)]
            qkv[e * d + own : (e + 1) * d, at(n)] = dot(wt[e * rest : (e + 1) * rest, :], u_ref[:, at(n)]).astype(BF16)
        do[0:own, at(n)] = save_ref[3 * own :, at(n)]
        do[own:, at(n)] = dot_nt(wo[...], g_ref[at(n), :]).astype(BF16)

    def mix(n):
        ot[0:low, at(n)] = dot(m1[0], qkv[2 * d : 2 * d + 256, at(n)]).astype(BF16)
        ot[low:d, at(n)] = dot(m2[0], qkv[2 * d + 128 : 3 * d, at(n)]).astype(BF16)
        rt[2 * d : 2 * d + low, at(n)] = dot(m1[1], do[0:256, at(n)]).astype(BF16)
        rt[2 * d + low : 3 * d, at(n)] = dot(m2[1], do[128:d, at(n)]).astype(BF16)
        for part, other, coef, i in ((0, d, cq, 2), (d, 0, ck, 3)):
            v = dot(m1[i], qkv[other : other + 256, at(n)])
            rt[part : part + low, at(n)] = (v + qkv[part : part + low, at(n)].astype(F32) * coef[0:low, :]).astype(BF16)
            v = dot(m2[i], qkv[other + 128 : other + d, at(n)])
            rt[part + low : part + d, at(n)] = (v + qkv[part + low : part + d, at(n)].astype(F32) * coef[low:d, :]).astype(BF16)

    def out(n):
        xt[:, at(n)] = x_ref[at(n), :].T
        for c, m in ((0, 128), (128, 256)):
            yt = dot(wot[c : c + m, :], ot[:, at(n)]) + xt[c : c + m, at(n)].astype(F32)
            y_ref[at(n), c : c + m] = yt.astype(BF16).T
        gx[:, at(n)] = dot(wn[...], rt[:, at(n)])

    def norm_bwd(*pair):
        mean = {n: st_ref[0:1, at(n)] for n in pair}
        inv = {n: st_ref[1:2, at(n)] for n in pair}
        s1 = {n: jnp.zeros((8, NT), F32) for n in pair}
        s2 = {n: jnp.zeros((8, NT), F32) for n in pair}
        for c in range(0, d, CH):
            gm = gam[c : c + CH, :]
            sum_h, sum_u = [], []
            for n in pair:
                du = gx[c : c + CH, at(n)]
                duh = du * ((xt[c : c + CH, at(n)].astype(F32) - mean[n]) * inv[n])
                s1[n] = s1[n] + fold8(du * gm)
                s2[n] = s2[n] + fold8(duh * gm)
                sum_h.append(duh)
                sum_u.append(du)
            v = sum(sum_h[1:], sum_h[0])
            acc_g[0, c : c + CH, :] += v[:, :LANES] + v[:, LANES:]
            v = sum(sum_u[1:], sum_u[0])
            acc_g[1, c : c + CH, :] += v[:, :LANES] + v[:, LANES:]
        for n in pair:
            m1_ = jnp.sum(s1[n], axis=0, keepdims=True) * (1.0 / d)
            m2_ = jnp.sum(s2[n], axis=0, keepdims=True) * (1.0 / d)
            slope = m2_ * inv[n] * inv[n]
            base = inv[n] * m1_
            gt[:, at(n)] = g_ref[at(n), :].T
            for c in range(0, d, CH):
                v = gx[c : c + CH, at(n)] * gam[c : c + CH, :] * inv[n] - base - (xt[c : c + CH, at(n)].astype(F32) - mean[n]) * slope
                gt[c : c + CH, at(n)] = (v + gt[c : c + CH, at(n)].astype(F32)).astype(BF16)
            dx_ref[at(n), :] = gt[:, at(n)].T

    for n in range(tiles + 3):
        if n >= 3:
            norm_bwd(n - 3)
        if n < tiles:
            project(n)
        if 2 <= n < tiles + 2:
            out(n - 2)
        if 1 <= n < tiles + 1:
            mix(n - 1)
    r_own = jnp.concatenate([rt[e * d : e * d + own, :] for e in range(3)], axis=0)
    acc_w[...] += dot_nt(r_own, u_ref[...])
    acc_o[...] += dot(ot[0:own, :], g_ref[...])

    @pl.when(step == steps - 1)
    def _():
        sp = dw_ref.shape[0]
        per = d // sp
        sub = own // sp
        wgrad = acc_w[...].T
        for s in range(sp):
            dw_ref[s, 0:per, 0 : 3 * own] = wgrad[s * per : (s + 1) * per, :]
            for q in range(d // own):
                dw_ref[s, q * sub : (q + 1) * sub, 3 * own :] = acc_o[s * sub : (s + 1) * sub, q * own : (q + 1) * own]
        for i in range(2):
            row = jnp.sum(acc_g[i].T, axis=0, keepdims=True)
            for q in range(d // own):
                gb_ref[i * (d // own) + q : i * (d // own) + q + 1, 0:own] = row[:, q * own : (q + 1) * own]


def main_call(x, g, save, u, st, wt, wn, wo, wot, m1, m2, gam, cq, ck, sp, block=2048):
    rows, d = x.shape
    own = d - wo.shape[0]
    steps = rows // block
    row = pl.BlockSpec((block, d), lambda i: (i, 0))
    col = lambda a: pl.BlockSpec((a.shape[0], block), lambda i: (0, i))
    full = lambda a: pl.BlockSpec(a.shape, lambda i: (0,) * a.ndim)
    slot = (sp, d // sp, d)
    sums = (2 * d // own, LANES)
    smalls = (wt, wn, wo, wot, m1, m2, gam, cq, ck)
    return pl.pallas_call(
        functools.partial(main_kernel, steps),
        grid=(steps,),
        in_specs=[row, row, col(save), col(u), col(st)] + [full(a) for a in smalls],
        out_specs=[row, row, pl.BlockSpec(slot, lambda i: (0, 0, 0)), pl.BlockSpec(sums, lambda i: (0, 0))],
        out_shape=[jax.ShapeDtypeStruct((rows, d), BF16), jax.ShapeDtypeStruct((rows, d), BF16), jax.ShapeDtypeStruct(slot, F32), jax.ShapeDtypeStruct(sums, F32)],
        scratch_shapes=[
            pltpu.VMEM((d, NT), F32),
            pltpu.VMEM((d, block), BF16),
            pltpu.VMEM((d, block), BF16),
            pltpu.VMEM((3 * d, block), BF16),
            pltpu.VMEM((d, block), BF16),
            pltpu.VMEM((d, block), BF16),
            pltpu.VMEM((3 * d, block), BF16),
            pltpu.VMEM((d, block), F32),
            pltpu.VMEM((3 * own, d), F32),
            pltpu.VMEM((own, d), F32),
            pltpu.VMEM((2, d, LANES), F32),
        ],
        compiler_params=pltpu.CompilerParams(dimension_semantics=("arbitrary",), vmem_limit_bytes=60 * 2**20),
        cost_estimate=pl.CostEstimate(flops=2 * rows * d * d * 9, bytes_accessed=8 * rows * d, transcendentals=0),
        name="main",
    )(x, g, save, u, st, *smalls)


def wgrad_kernel(sp, in_ref, gb_in, out_ref, gb_out, mine, pair, got, gb_mine, gb_pair, gb_got, sem, send_a, recv_a, send_b, recv_b):
    my = lax.axis_index("sp")
    chips = sp // 2
    core, chip = lax.rem(my, 2), my // 2
    other = {"sp": chip * 2 + 1 - core}
    there = [lax.rem(chip + k, chips) for k in range(chips)]
    peers = [{"sp": c * 2 + core} for c in there]
    barrier = pltpu.get_barrier_semaphore()
    for peer in [other] + peers[1:]:
        pl.semaphore_signal(barrier, inc=1, device_id=peer, device_id_type=MESH)
    loads = [pltpu.make_async_copy(in_ref, mine, sem.at[0]), pltpu.make_async_copy(gb_in, gb_mine, sem.at[1])]
    for c in loads:
        c.start()
    for c in loads:
        c.wait()
    pl.semaphore_wait(barrier, chips)
    order = sorted(range(1, chips), key=lambda k: -min(k, chips - k)) + [0]
    first = [remote(mine.at[2 * c + 1 - core], pair.at[c], send_a.at[k], recv_a.at[k], other) for k, c in enumerate(there)]
    gb_first = remote(gb_mine, gb_pair, send_a.at[chips], recv_a.at[chips], other)
    for k in order:
        first[k].start()
    gb_first.start()
    second = {
        k: remote(got.at[chips + there[k]], got.at[chip], send_b.at[k], recv_b.at[k], peers[k]) for k in range(1, chips)
    }
    for k in order:
        first[k].wait()
        v = mine[2 * there[k] + core] + pair[there[k]]
        if k:
            got[chips + there[k]] = v
            second[k].start()
        else:
            got[chip] = v
    gb_first.wait()
    gb_got[chips] = gb_mine[...] + gb_pair[...]
    gb_second = [
        remote(gb_got.at[chips], gb_got.at[chip], send_b.at[chips + k], recv_b.at[chips + k], peers[k]) for k in range(1, chips)
    ]
    for c in gb_second:
        c.start()
    gb_got[chip] = gb_mine[...] + gb_pair[...]
    for k in order[:-1]:
        second[k].wait()
    total = got[0]
    for c in range(1, chips):
        total = total + got[c]
    out_ref[...] = total
    for c in gb_second:
        c.wait()
    total = gb_got[0]
    for c in range(1, chips):
        total = total + gb_got[c]
    gb_out[...] = total


def wgrad_call(parts, gb):
    sp, slot = parts.shape[0], parts.shape[1:]
    chips = sp // 2
    dma = pltpu.SemaphoreType.DMA
    hbm, vmem = pl.BlockSpec(memory_space=pl.ANY), pl.BlockSpec(memory_space=pltpu.VMEM)
    return pl.pallas_call(
        functools.partial(wgrad_kernel, sp),
        in_specs=[hbm, hbm],
        out_specs=[vmem, vmem],
        out_shape=[jax.ShapeDtypeStruct(slot, F32), jax.ShapeDtypeStruct(gb.shape, F32)],
        scratch_shapes=[
            pltpu.VMEM((sp, *slot), F32),
            pltpu.VMEM((chips, *slot), F32),
            pltpu.VMEM((sp, *slot), F32),
            pltpu.VMEM(gb.shape, F32),
            pltpu.VMEM(gb.shape, F32),
            pltpu.VMEM((chips + 1, *gb.shape), F32),
            dma((2,)),
            dma((chips + 1,)),
            dma((chips + 1,)),
            dma((sp,)),
            dma((sp,)),
        ],
        compiler_params=pltpu.CompilerParams(collective_id=1, has_side_effects=True),
        name="wgrad",
    )(parts, gb)


def finish_kernel(sum_ref, gb_ref, dt_ref, w_ref, o_ref, gam_ref, bet_ref, tau_ref):
    own = w_ref.shape[2]
    sub = o_ref.shape[0]
    split = o_ref.shape[1] // own
    for e in range(3):
        w_ref[e] = sum_ref[:, e * own : (e + 1) * own]
    for q in range(split):
        o_ref[:, q * own : (q + 1) * own] = sum_ref[q * sub : (q + 1) * sub, 3 * own :]
    for i, ref in enumerate((gam_ref, bet_ref)):
        row = [gb_ref[i * split + q : i * split + q + 1, 0:own] for q in range(split)]
        ref[...] = jnp.concatenate(row, axis=1)[0]
    tau_ref[...] = dt_ref[0, 0 : tau_ref.shape[0]]


def finish_call(total, gb, dt, own, sp, heads):
    d = total.shape[1]
    vmem = pl.BlockSpec(memory_space=pltpu.VMEM)
    shapes = [(3, d // sp, own), (own // sp, d), (d,), (d,), (heads,)]
    return pl.pallas_call(
        finish_kernel,
        in_specs=[vmem] * 3,
        out_specs=[vmem] * 5,
        out_shape=[jax.ShapeDtypeStruct(s, F32) for s in shapes],
        name="finish",
    )(total, gb, dt)


def solution(mesh):
    tp, sp = mesh.shape["tp"], mesh.shape["sp"]
    row_spec = P(("dp", "sp"), None)

    def local_step(x, g, w_qkv, w_out, gamma, beta, temps):
        save, u, st, wt, wn, wo, wot, m1, m2, cq, ck, dt = front_call(
            x, g, w_qkv.transpose(1, 2, 0), w_out, gamma, beta, temps, tp, sp
        )
        y, dx, parts, gb = main_call(x, g, save, u, st, wt, wn, wo, wot, m1, m2, gamma, cq, ck, sp)
        grad_w, grad_o, grad_gamma, grad_beta, grad_temp = finish_call(
            *wgrad_call(parts, gb), dt, w_out.shape[0], sp, temps.shape[0]
        )
        return y, dx, grad_w.transpose(1, 0, 2), grad_o, grad_gamma, grad_beta, grad_temp

    in_specs = (row_spec, row_spec, P(None, None, "tp"), P("tp", None), P(None), P(None), P(None))
    out_specs = (row_spec, row_spec, P(("dp", "sp"), None, "tp"), P(("dp", "tp", "sp"), None), P("dp"), P("dp"), P("dp"))
    return jax.shard_map(local_step, mesh=mesh, in_specs=in_specs, out_specs=out_specs, check_vma=False)
```

```python
import functools

import jax
import jax.numpy as jnp
from jax import lax
from jax.experimental import pallas as pl
from jax.experimental.pallas import tpu as pltpu
from jax.sharding import PartitionSpec as P

F32, BF16 = jnp.float32, jnp.bfloat16
LN_EPS = 1e-6
NT = 256
CH = 64
LANES = 128
MESH = pl.DeviceIdType.MESH


def dot(a, b):
    return jnp.dot(a, b, preferred_element_type=F32)


def dot_nt(a, b):
    return lax.dot_general(a, b, (((1,), (1,)), ((), ())), preferred_element_type=F32)


def fold8(v):
    return jnp.sum(v.reshape(v.shape[0] // 8, 8, v.shape[1]), axis=0)


def ln_stats(xt, cols):
    d = xt.shape[0]
    acc = jnp.zeros((8, NT), F32)
    for c in range(0, d, CH):
        acc = acc + fold8(xt[c : c + CH, cols].astype(F32))
    mean = jnp.sum(acc, axis=0, keepdims=True) * (1.0 / d)
    acc = jnp.zeros((8, NT), F32)
    for c in range(0, d, CH):
        v = xt[c : c + CH, cols].astype(F32) - mean
        acc = acc + fold8(v * v)
    return mean, lax.rsqrt(jnp.sum(acc, axis=0, keepdims=True) * (1.0 / d) + LN_EPS)


def spread_columns(row_ref, out):
    d = row_ref.shape[0]
    out[...] = jnp.broadcast_to(row_ref[...].reshape(1, d), (NT, d)).T


def remote(src, dst, send_sem, recv_sem, device):
    return pltpu.make_async_remote_copy(
        src_ref=src, dst_ref=dst, send_sem=send_sem, recv_sem=recv_sem, device_id=device, device_id_type=MESH
    )


def head_state(t, tau, head):
    lane = lax.broadcasted_iota(jnp.int32, (head, LANES), 1)
    row = lax.broadcasted_iota(jnp.int32, (head, LANES), 0)
    valid = lane < head
    eye = lane == row
    pick = lambda i: t[:, i : i + 1]
    q2 = pick(2 * head)
    k2 = jnp.sum(jnp.where(eye, pick(2 * head + 1), 0.0), axis=0, keepdims=True)
    k2 = jnp.where(valid, k2, 1.0)
    norm = jnp.sqrt(q2) * jnp.sqrt(k2)
    gram_n = jnp.where(valid, t / norm, 0.0)
    datt = jnp.where(valid, pltpu.roll(t, LANES - head, 1), 0.0)
    logit = jnp.where(valid, tau * gram_n, -1e30)
    ex = jnp.exp(logit - jnp.max(logit, axis=1, keepdims=True))
    ex = jnp.where(valid, ex, 0.0)
    att = ex / jnp.sum(ex, axis=1, keepdims=True)
    d_logit = att * (datt - jnp.sum(att * datt, axis=1, keepdims=True))
    d_tau = jnp.sum(jnp.sum(d_logit * gram_n, axis=1, keepdims=True), axis=0, keepdims=True)
    e_mat = tau * d_logit
    d_gram = (e_mat / norm).astype(BF16).astype(F32)
    es = e_mat * gram_n
    q_coef = -jnp.sum(es, axis=1, keepdims=True) / q2
    k_coef = -jnp.sum(es, axis=0, keepdims=True) / k2
    k_coef = jnp.sum(jnp.where(eye, k_coef, 0.0), axis=1, keepdims=True)
    v = jnp.where(valid, att.astype(BF16).astype(F32), pltpu.roll(d_gram, head, 1))
    v = jnp.where(lane == 2 * head, q_coef, v)
    v = jnp.where(lane == 2 * head + 1, k_coef, v)
    return jnp.where(lane == 2 * head + 2, d_tau, v)


def front_kernel(tp, sp, steps, x_ref, g_ref, w_ref, w4_ref, gam_ref, bet_ref, temp_ref,
                 save_ref, u_ref, st_ref, wt_ref, wn_ref, wo_ref, wot_ref, m1_ref, m2_ref, cq_ref, ck_ref, dt_ref,
                 wq, gam, bet, xt, gt, ut, save_s, u_s, qd, kv, acc, sq, wall, sums, pair, parts, state, big,
                 out_sem, send_w, recv_w, send_p, recv_p, send_a, recv_a, send_b, recv_b):
    step = pl.program_id(0)
    my_sp, my_tp = lax.axis_index("sp"), lax.axis_index("tp")
    chips = sp // 2
    core, chip = lax.rem(my_sp, 2), my_sp // 2
    rows, d = x_ref.shape
    own = w4_ref.shape[0]
    head = own // 2
    rest = d - own
    other = {"sp": chip * 2 + 1 - core}
    chip_peers = [{"sp": lax.rem(chip + k, chips) * 2 + core} for k in range(1, chips)]
    tp_peers = [[{"tp": lax.rem(my_tp + k, tp), "sp": chip * 2 + t} for t in range(2)] for k in range(1, tp)]
    barrier = pltpu.get_barrier_semaphore()
    peers = [other] + chip_peers + [p for ps in tp_peers for p in ps]

    @pl.when(step == 0)
    def _():
        for peer in peers:
            pl.semaphore_signal(barrier, inc=1, device_id=peer, device_id_type=MESH)
        for e in range(3):
            wq[e * own : (e + 1) * own, :] = w_ref[e]
        spread_columns(gam_ref, gam)
        spread_columns(bet_ref, bet)
        acc[...] = jnp.zeros_like(acc)
        sq[...] = jnp.zeros_like(sq)

    def weight_copies():
        out = []
        for k in range(1, tp):
            for i, (src, dst) in enumerate(((w_ref, wall.at[tp - k, 0:3]), (w4_ref, wall.at[tp - k, 3]))):
                peer = {"tp": lax.rem(my_tp + k, tp), "sp": my_sp}
                out.append(remote(src, dst, send_w.at[k, i], recv_w.at[k, i], peer))
        return out

    @pl.when(step == 1)
    def _():
        pl.semaphore_wait(barrier, len(peers))
        for c in weight_copies():
            c.start()

    slot = lax.rem(step, 2)

    def save_copies(to, at_slot):
        cols = pl.ds(pl.multiple_of(to * rows, LANES), rows)
        return [
            pltpu.make_async_copy(save_s.at[at_slot], save_ref.at[:, cols], out_sem.at[at_slot, 0]),
            pltpu.make_async_copy(u_s.at[at_slot], u_ref.at[:, cols], out_sem.at[at_slot, 1]),
        ]

    @pl.when(step >= 2)
    def _():
        for c in save_copies(step - 2, slot):
            c.wait()

    tiles = rows // NT
    at = lambda n: pl.ds(n * NT, NT)

    def norm(n):
        xt[:, at(n)] = x_ref[at(n), :].T
        gt[:, at(n)] = g_ref[at(n), :].T
        mean, inv = ln_stats(xt, at(n))
        st_ref[0:1, at(n)] = mean
        st_ref[1:2, at(n)] = inv
        for c in range(0, d, CH):
            v = (xt[c : c + CH, at(n)].astype(F32) - mean) * inv
            v = (v * gam[c : c + CH, :] + bet[c : c + CH, :]).astype(BF16)
            ut[c : c + CH, at(n)] = v
            u_s[slot, c : c + CH, at(n)] = v

    def project(n):
        qkv = dot(wq[...], ut[:, at(n)])
        for e, (ref, r) in enumerate(((qd, 0), (kv, 0), (kv, own))):
            v = qkv[e * own : (e + 1) * own].astype(BF16)
            ref[r : r + own, at(n)] = v
            save_s[slot, e * own : (e + 1) * own, at(n)] = v
            if e < 2:
                v = v.astype(F32)
                v = v * v
                sq[e * own : (e + 1) * own] += v[:, :LANES] + v[:, LANES:]
        v = dot(w4_ref[...], gt[:, at(n)]).astype(BF16)
        qd[own:, at(n)] = v
        save_s[slot, 3 * own :, at(n)] = v

    def gram(n):
        cols = pl.ds(n * NT, 4 * NT)
        acc[:, 0 : 2 * own] += dot_nt(qd[:, cols], kv[:, cols])

    norm(0)
    for n in range(tiles):
        if n + 1 < tiles:
            norm(n + 1)
        if n >= 4 and n % 4 == 0:
            gram(n - 4)
        project(n)
    gram(tiles - 4)
    for c in save_copies(step, slot):
        c.start()

    @pl.when(step == steps - 1)
    def _():
        lane = lax.broadcasted_iota(jnp.int32, (head, LANES), 1)
        row = lax.broadcasted_iota(jnp.int32, (head, LANES), 0)
        valid = lane < head

        def block(r, c, to):
            shift = (to - c) % 256
            v = acc[r : r + head, :]
            return (pltpu.roll(v, shift, 1) if shift else v)[:, :LANES]

        for h in range(2):
            r = h * head
            q2 = jnp.sum(sq[r : r + head, :], axis=1, keepdims=True)
            k2 = jnp.sum(sq[own + r : own + r + head, :], axis=1, keepdims=True)
            v = jnp.where(valid, block(r, r, 0), block(own + r, own + r, head))
            v = jnp.where(lane == 2 * head, q2, v)
            sums[r : r + head, :] = jnp.where(lane == 2 * head + 1, k2, v)

        mine = pl.ds(pl.multiple_of(core * head, 8), head)
        theirs = pl.ds(pl.multiple_of((1 - core) * head, 8), head)
        first = remote(sums.at[theirs], pair, send_p.at[0], recv_p.at[0], other)
        first.start()
        for c in weight_copies():
            c.wait()
        first.wait()
        parts[chip] = sums[mine, :] + pair[...]
        copies = [
            remote(parts.at[chip], parts.at[chip], send_a.at[k], recv_a.at[k], chip_peers[k - 1]) for k in range(1, chips)
        ]
        for c in copies:
            c.start()
        big[...] = jnp.zeros_like(big)
        pieces = [(w_ref, w4_ref)] + [(wall.at[j, 0:3], wall.at[j, 3]) for j in range(1, tp)]
        for j, (piece, piece4) in enumerate(pieces):
            for e in range(3):
                wn_ref[:, e * d + j * own : e * d + (j + 1) * own] = piece[e].T
                if j:
                    wt_ref[e * rest + (j - 1) * own : e * rest + j * own, :] = piece[e]
            wot_ref[:, j * own : (j + 1) * own] = piece4[...].T
            if j:
                wo_ref[(j - 1) * own : j * own, :] = piece4[...]
        for c in copies:
            c.wait()
        total = parts[0]
        for k in range(1, chips):
            total = total + parts[k]
        state[0, core] = head_state(total, temp_ref[my_tp * 2 + core], head)

        copies = [remote(state.at[0, core], state.at[0, core], send_b.at[0, 0], recv_b.at[0, core], other)]
        for k in range(1, tp):
            for t in range(2):
                copies.append(
                    remote(state.at[0, core], state.at[tp - k, core], send_b.at[k, t], recv_b.at[k, core], tp_peers[k - 1][t])
                )
        for c in copies:
            c.start()
        lane1 = lax.broadcasted_iota(jnp.int32, dt_ref.shape, 1)
        dt = jnp.zeros(dt_ref.shape, F32)
        zero = jnp.zeros((head, d - LANES), F32)
        for j in (0, tp - 1, 1, *range(2, tp - 1)):
            k = tp - j
            if j == 0:
                remote(state.at[0, core], state.at[0, 1 - core], send_b.at[0, 0], recv_b.at[0, 1 - core], other).wait_recv()
            for h in range(2):
                if j:
                    remote(state.at[0, core], state.at[j, h], send_b.at[k, h], recv_b.at[k, h], tp_peers[k - 1][h]).wait_recv()
                t = state[j, h]
                pick = lambda i: t[:, i : i + 1]
                r = j * own + h * head
                att = jnp.concatenate([jnp.where(valid, t, 0.0), zero], axis=1)
                d_gram = jnp.concatenate([jnp.where(valid, pltpu.roll(t, LANES - head, 1), 0.0), zero], axis=1)
                big[0, r : r + head, :] = pltpu.roll(att, r, 1) if r else att
                big[1, r : r + head, :] = pltpu.roll(d_gram, r, 1) if r else d_gram
                cq_ref[r : r + head, :] = jnp.broadcast_to(pick(2 * head), (head, NT))
                ck_ref[r : r + head, :] = jnp.broadcast_to(pick(2 * head + 1), (head, NT))
                which = lax.rem(my_tp + j, tp) * 2 + h
                dt = jnp.where(lane1 == which, pick(2 * head + 2)[0:1, :], dt)
        for c in copies:
            c.wait_send()
        dt_ref[...] = dt
        low = m1_ref.shape[1]
        for i in range(2):
            m = big[i].astype(BF16)
            mt = m.T
            m1_ref[2 * i] = m[0:low, 0:256]
            m2_ref[2 * i] = m[low:, 128:]
            m1_ref[2 * i + 1] = mt[0:low, 0:256]
            m2_ref[2 * i + 1] = mt[low:, 128:]
        for c in save_copies(step - 1, 1 - slot) + save_copies(step, slot):
            c.wait()


def front_call(x, g, w, w4, gam, bet, temps, tp, sp, block=4096):
    rows, d = x.shape
    own = w4.shape[0]
    head = d // temps.shape[0]
    low = 256 // head * head
    steps = rows // block
    row = pl.BlockSpec((block, d), lambda i: (i, 0))
    full = lambda shape: pl.BlockSpec(shape, lambda i: (0,) * len(shape))
    smalls = [
        ((3 * (d - own), d), BF16),
        ((d, 3 * d), BF16),
        ((d - own, d), BF16),
        ((d, d), BF16),
        ((4, low, 256), BF16),
        ((4, d - low, 256), BF16),
        ((d, NT), F32),
        ((d, NT), F32),
        ((1, LANES), F32),
    ]
    dma = pltpu.SemaphoreType.DMA
    return pl.pallas_call(
        functools.partial(front_kernel, tp, sp, steps),
        grid=(steps,),
        in_specs=[row, row, full(w.shape), full(w4.shape), full(gam.shape), full(bet.shape), pl.BlockSpec(memory_space=pltpu.SMEM)],
        out_specs=[pl.BlockSpec(memory_space=pl.ANY)] * 2
        + [pl.BlockSpec((8, block), lambda i: (0, i))]
        + [full(s) for s, _ in smalls],
        out_shape=[jax.ShapeDtypeStruct((r, rows), t) for r, t in ((4 * own, BF16), (d, BF16), (8, F32))] + [jax.ShapeDtypeStruct(s, t) for s, t in smalls],
        scratch_shapes=[
            pltpu.VMEM((3 * own, d), BF16),
            pltpu.VMEM((d, NT), F32),
            pltpu.VMEM((d, NT), F32),
            pltpu.VMEM((d, block), BF16),
            pltpu.VMEM((d, block), BF16),
            pltpu.VMEM((d, block), BF16),
            pltpu.VMEM((2, 4 * own, block), BF16),
            pltpu.VMEM((2, d, block), BF16),
            pltpu.VMEM((2 * own, block), BF16),
            pltpu.VMEM((2 * own, block), BF16),
            pltpu.VMEM((2 * own, 256), F32),
            pltpu.VMEM((2 * own, LANES), F32),
            pltpu.VMEM((tp, 4, own, d), BF16),
            pltpu.VMEM((own, LANES), F32),
            pltpu.VMEM((head, LANES), F32),
            pltpu.VMEM((sp // 2, head, LANES), F32),
            pltpu.VMEM((tp, 2, head, LANES), F32),
            pltpu.VMEM((2, d, d), F32),
            dma((2, 2)),
            dma((tp, 2)),
            dma((tp, 2)),
            dma((1,)),
            dma((1,)),
            dma((sp // 2,)),
            dma((sp // 2,)),
            dma((tp, 2)),
            dma((tp, 2)),
        ],
        compiler_params=pltpu.CompilerParams(
            dimension_semantics=("arbitrary",), vmem_limit_bytes=60 * 2**20, collective_id=0, has_side_effects=True
        ),
        cost_estimate=pl.CostEstimate(flops=2 * rows * d * 4 * own, bytes_accessed=4 * rows * d, transcendentals=0),
        name="front",
    )(x, g, w, w4, gam, bet, temps)


def main_kernel(steps, x_ref, g_ref, save_ref, u_ref, st_ref, wt, wn, wo, wot, m1, m2, gam_ref, cq, ck, y_ref, dx_ref, dw_ref, gb_ref,
                gam, xt, gt, qkv, do, ot, rt, gx, acc_w, acc_o, acc_g):
    step = pl.program_id(0)
    rows, d = x_ref.shape
    rest = wo.shape[0]
    own = d - rest
    low = m1.shape[1]

    @pl.when(step == 0)
    def _():
        spread_columns(gam_ref, gam)
        acc_w[...] = jnp.zeros_like(acc_w)
        acc_o[...] = jnp.zeros_like(acc_o)
        acc_g[...] = jnp.zeros_like(acc_g)

    tiles = rows // NT
    at = lambda n: pl.ds(n * NT, NT)

    def project(n):
        for e in range(3):
            qkv[e * d : e * d + own, at(n)] = save_ref[e * own : (e + 1) * own, at(n)]
            qkv[e * d + own : (e + 1) * d, at(n)] = dot(wt[e * rest : (e + 1) * rest, :], u_ref[:, at(n)]).astype(BF16)
        do[0:own, at(n)] = save_ref[3 * own :, at(n)]
        do[own:, at(n)] = dot_nt(wo[...], g_ref[at(n), :]).astype(BF16)

    def mix(n):
        ot[0:low, at(n)] = dot(m1[0], qkv[2 * d : 2 * d + 256, at(n)]).astype(BF16)
        ot[low:d, at(n)] = dot(m2[0], qkv[2 * d + 128 : 3 * d, at(n)]).astype(BF16)
        rt[2 * d : 2 * d + low, at(n)] = dot(m1[1], do[0:256, at(n)]).astype(BF16)
        rt[2 * d + low : 3 * d, at(n)] = dot(m2[1], do[128:d, at(n)]).astype(BF16)
        for part, other, coef, i in ((0, d, cq, 2), (d, 0, ck, 3)):
            v = dot(m1[i], qkv[other : other + 256, at(n)])
            rt[part : part + low, at(n)] = (v + qkv[part : part + low, at(n)].astype(F32) * coef[0:low, :]).astype(BF16)
            v = dot(m2[i], qkv[other + 128 : other + d, at(n)])
            rt[part + low : part + d, at(n)] = (v + qkv[part + low : part + d, at(n)].astype(F32) * coef[low:d, :]).astype(BF16)

    def out(n):
        xt[:, at(n)] = x_ref[at(n), :].T
        for c, m in ((0, 128), (128, 256)):
            yt = dot(wot[c : c + m, :], ot[:, at(n)]) + xt[c : c + m, at(n)].astype(F32)
            y_ref[at(n), c : c + m] = yt.astype(BF16).T
        gx[:, at(n)] = dot(wn[...], rt[:, at(n)])

    def norm_bwd(*pair):
        mean = {n: st_ref[0:1, at(n)] for n in pair}
        inv = {n: st_ref[1:2, at(n)] for n in pair}
        s1 = {n: jnp.zeros((8, NT), F32) for n in pair}
        s2 = {n: jnp.zeros((8, NT), F32) for n in pair}
        for c in range(0, d, CH):
            gm = gam[c : c + CH, :]
            sum_h, sum_u = [], []
            for n in pair:
                du = gx[c : c + CH, at(n)]
                duh = du * ((xt[c : c + CH, at(n)].astype(F32) - mean[n]) * inv[n])
                s1[n] = s1[n] + fold8(du * gm)
                s2[n] = s2[n] + fold8(duh * gm)
                sum_h.append(duh)
                sum_u.append(du)
            v = sum(sum_h[1:], sum_h[0])
            acc_g[0, c : c + CH, :] += v[:, :LANES] + v[:, LANES:]
            v = sum(sum_u[1:], sum_u[0])
            acc_g[1, c : c + CH, :] += v[:, :LANES] + v[:, LANES:]
        for n in pair:
            m1_ = jnp.sum(s1[n], axis=0, keepdims=True) * (1.0 / d)
            m2_ = jnp.sum(s2[n], axis=0, keepdims=True) * (1.0 / d)
            slope = m2_ * inv[n] * inv[n]
            base = mean[n] * slope - inv[n] * m1_
            gt[:, at(n)] = g_ref[at(n), :].T
            for c in range(0, d, CH):
                v = gx[c : c + CH, at(n)] * gam[c : c + CH, :] * inv[n] + base - xt[c : c + CH, at(n)].astype(F32) * slope
                gt[c : c + CH, at(n)] = (v + gt[c : c + CH, at(n)].astype(F32)).astype(BF16)
            dx_ref[at(n), :] = gt[:, at(n)].T

    for n in range(tiles + 3):
        if n >= 3:
            norm_bwd(n - 3)
        if n < tiles:
            project(n)
        if 2 <= n < tiles + 2:
            out(n - 2)
        if 1 <= n < tiles + 1:
            mix(n - 1)
    r_own = jnp.concatenate([rt[e * d : e * d + own, :] for e in range(3)], axis=0)
    acc_w[...] += dot_nt(r_own, u_ref[...])
    acc_o[...] += dot(ot[0:own, :], g_ref[...])

    @pl.when(step == steps - 1)
    def _():
        sp = dw_ref.shape[0]
        per = d // sp
        sub = own // sp
        wgrad = acc_w[...].T
        for s in range(sp):
            dw_ref[s, 0:per, 0 : 3 * own] = wgrad[s * per : (s + 1) * per, :]
            for q in range(d // own):
                dw_ref[s, q * sub : (q + 1) * sub, 3 * own :] = acc_o[s * sub : (s + 1) * sub, q * own : (q + 1) * own]
        for i in range(2):
            row = jnp.sum(acc_g[i].T, axis=0, keepdims=True)
            for q in range(d // own):
                gb_ref[i * (d // own) + q : i * (d // own) + q + 1, 0:own] = row[:, q * own : (q + 1) * own]


def main_call(x, g, save, u, st, wt, wn, wo, wot, m1, m2, gam, cq, ck, sp, block=2048):
    rows, d = x.shape
    own = d - wo.shape[0]
    steps = rows // block
    row = pl.BlockSpec((block, d), lambda i: (i, 0))
    col = lambda a: pl.BlockSpec((a.shape[0], block), lambda i: (0, i))
    full = lambda a: pl.BlockSpec(a.shape, lambda i: (0,) * a.ndim)
    slot = (sp, d // sp, d)
    sums = (2 * d // own, LANES)
    smalls = (wt, wn, wo, wot, m1, m2, gam, cq, ck)
    return pl.pallas_call(
        functools.partial(main_kernel, steps),
        grid=(steps,),
        in_specs=[row, row, col(save), col(u), col(st)] + [full(a) for a in smalls],
        out_specs=[row, row, pl.BlockSpec(slot, lambda i: (0, 0, 0)), pl.BlockSpec(sums, lambda i: (0, 0))],
        out_shape=[jax.ShapeDtypeStruct((rows, d), BF16), jax.ShapeDtypeStruct((rows, d), BF16), jax.ShapeDtypeStruct(slot, F32), jax.ShapeDtypeStruct(sums, F32)],
        scratch_shapes=[
            pltpu.VMEM((d, NT), F32),
            pltpu.VMEM((d, block), BF16),
            pltpu.VMEM((d, block), BF16),
            pltpu.VMEM((3 * d, block), BF16),
            pltpu.VMEM((d, block), BF16),
            pltpu.VMEM((d, block), BF16),
            pltpu.VMEM((3 * d, block), BF16),
            pltpu.VMEM((d, block), F32),
            pltpu.VMEM((3 * own, d), F32),
            pltpu.VMEM((own, d), F32),
            pltpu.VMEM((2, d, LANES), F32),
        ],
        compiler_params=pltpu.CompilerParams(dimension_semantics=("arbitrary",), vmem_limit_bytes=60 * 2**20),
        cost_estimate=pl.CostEstimate(flops=2 * rows * d * d * 9, bytes_accessed=8 * rows * d, transcendentals=0),
        name="main",
    )(x, g, save, u, st, *smalls)


def wgrad_kernel(sp, in_ref, gb_in, out_ref, gb_out, mine, pair, got, gb_mine, gb_pair, gb_got, sem, send_a, recv_a, send_b, recv_b):
    my = lax.axis_index("sp")
    chips = sp // 2
    core, chip = lax.rem(my, 2), my // 2
    other = {"sp": chip * 2 + 1 - core}
    there = [lax.rem(chip + k, chips) for k in range(chips)]
    peers = [{"sp": c * 2 + core} for c in there]
    barrier = pltpu.get_barrier_semaphore()
    for peer in [other] + peers[1:]:
        pl.semaphore_signal(barrier, inc=1, device_id=peer, device_id_type=MESH)
    loads = [pltpu.make_async_copy(in_ref, mine, sem.at[0]), pltpu.make_async_copy(gb_in, gb_mine, sem.at[1])]
    for c in loads:
        c.start()
    for c in loads:
        c.wait()
    pl.semaphore_wait(barrier, chips)
    order = sorted(range(1, chips), key=lambda k: -min(k, chips - k)) + [0]
    first = [remote(mine.at[2 * c + 1 - core], pair.at[c], send_a.at[k], recv_a.at[k], other) for k, c in enumerate(there)]
    gb_first = remote(gb_mine, gb_pair, send_a.at[chips], recv_a.at[chips], other)
    for k in order:
        first[k].start()
    gb_first.start()
    second = {
        k: remote(got.at[chips + there[k]], got.at[chip], send_b.at[k], recv_b.at[k], peers[k]) for k in range(1, chips)
    }
    for k in order:
        first[k].wait()
        v = mine[2 * there[k] + core] + pair[there[k]]
        if k:
            got[chips + there[k]] = v
            second[k].start()
        else:
            got[chip] = v
    gb_first.wait()
    gb_got[chips] = gb_mine[...] + gb_pair[...]
    gb_second = [
        remote(gb_got.at[chips], gb_got.at[chip], send_b.at[chips + k], recv_b.at[chips + k], peers[k]) for k in range(1, chips)
    ]
    for c in gb_second:
        c.start()
    gb_got[chip] = gb_mine[...] + gb_pair[...]
    for k in order[:-1]:
        second[k].wait()
    total = got[0]
    for c in range(1, chips):
        total = total + got[c]
    out_ref[...] = total
    for c in gb_second:
        c.wait()
    total = gb_got[0]
    for c in range(1, chips):
        total = total + gb_got[c]
    gb_out[...] = total


def wgrad_call(parts, gb):
    sp, slot = parts.shape[0], parts.shape[1:]
    chips = sp // 2
    dma = pltpu.SemaphoreType.DMA
    hbm, vmem = pl.BlockSpec(memory_space=pl.ANY), pl.BlockSpec(memory_space=pltpu.VMEM)
    return pl.pallas_call(
        functools.partial(wgrad_kernel, sp),
        in_specs=[hbm, hbm],
        out_specs=[vmem, vmem],
        out_shape=[jax.ShapeDtypeStruct(slot, F32), jax.ShapeDtypeStruct(gb.shape, F32)],
        scratch_shapes=[
            pltpu.VMEM((sp, *slot), F32),
            pltpu.VMEM((chips, *slot), F32),
            pltpu.VMEM((sp, *slot), F32),
            pltpu.VMEM(gb.shape, F32),
            pltpu.VMEM(gb.shape, F32),
            pltpu.VMEM((chips + 1, *gb.shape), F32),
            dma((2,)),
            dma((chips + 1,)),
            dma((chips + 1,)),
            dma((sp,)),
            dma((sp,)),
        ],
        compiler_params=pltpu.CompilerParams(collective_id=1, has_side_effects=True),
        name="wgrad",
    )(parts, gb)


def finish_kernel(sum_ref, gb_ref, dt_ref, w_ref, o_ref, gam_ref, bet_ref, tau_ref):
    own = w_ref.shape[2]
    sub = o_ref.shape[0]
    split = o_ref.shape[1] // own
    for e in range(3):
        w_ref[e] = sum_ref[:, e * own : (e + 1) * own]
    for q in range(split):
        o_ref[:, q * own : (q + 1) * own] = sum_ref[q * sub : (q + 1) * sub, 3 * own :]
    for i, ref in enumerate((gam_ref, bet_ref)):
        row = [gb_ref[i * split + q : i * split + q + 1, 0:own] for q in range(split)]
        ref[...] = jnp.concatenate(row, axis=1)[0]
    tau_ref[...] = dt_ref[0, 0 : tau_ref.shape[0]]


def finish_call(total, gb, dt, own, sp, heads):
    d = total.shape[1]
    vmem = pl.BlockSpec(memory_space=pltpu.VMEM)
    shapes = [(3, d // sp, own), (own // sp, d), (d,), (d,), (heads,)]
    return pl.pallas_call(
        finish_kernel,
        in_specs=[vmem] * 3,
        out_specs=[vmem] * 5,
        out_shape=[jax.ShapeDtypeStruct(s, F32) for s in shapes],
        name="finish",
    )(total, gb, dt)


def solution(mesh):
    tp, sp = mesh.shape["tp"], mesh.shape["sp"]
    row_spec = P(("dp", "sp"), None)

    def local_step(x, g, w_qkv, w_out, gamma, beta, temps):
        save, u, st, wt, wn, wo, wot, m1, m2, cq, ck, dt = front_call(
            x, g, w_qkv.transpose(1, 2, 0), w_out, gamma, beta, temps, tp, sp
        )
        y, dx, parts, gb = main_call(x, g, save, u, st, wt, wn, wo, wot, m1, m2, gamma, cq, ck, sp)
        grad_w, grad_o, grad_gamma, grad_beta, grad_temp = finish_call(
            *wgrad_call(parts, gb), dt, w_out.shape[0], sp, temps.shape[0]
        )
        return y, dx, grad_w.transpose(1, 0, 2), grad_o, grad_gamma, grad_beta, grad_temp

    in_specs = (row_spec, row_spec, P(None, None, "tp"), P("tp", None), P(None), P(None), P(None))
    out_specs = (row_spec, row_spec, P(("dp", "sp"), None, "tp"), P(("dp", "tp", "sp"), None), P("dp"), P("dp"), P("dp"))
    return jax.shard_map(local_step, mesh=mesh, in_specs=in_specs, out_specs=out_specs, check_vma=False)
```
